32 devices in a mesh: dp: 4 (over z), seq: 8 (over y, x, core).
Axes of the slice: x: 2, y: 2, z: 4, core: 2. Of those that a mesh axis runs over, the one named last changes fastest.
Arguments:
- tokens: bfloat16 [4, 2048, 1536], P('dp', 'seq'), may hold values from -6 to 6
- cotangent: bfloat16 [4, 2048, 1536], P('dp', 'seq'), may hold values from -6 to 6
- in_weight: bfloat16 [1536, 6448], P(('dp', 'seq')), may hold values from -0.15625 to 0.15625
- out_weight: bfloat16 [3072, 1536], P(('dp', 'seq')), may hold values from -0.109375 to 0.109375
- conv_weight: bfloat16 [3328, 4], P(('dp', 'seq')), may hold values from -3 to 3
- conv_bias: bfloat16 [3328], P(('dp', 'seq')), may hold values from -0.5 to 0.5
- norm_gain: bfloat16 [1536], P(('dp', 'seq')), may hold values from 0.5 to 1.5
- gate_gain: bfloat16 [3072], P(('dp', 'seq')), may hold values from 0.5 to 1.5
- decay_rate: float32 [48], replicated, may hold values from 0.00012207031 to 0.08
- dt_bias: float32 [48], replicated, may hold values from -2 to 0.5
- d_skip: float32 [48], replicated, may hold values from 0.5 to 2
Outputs:
- block_out: bfloat16 [4, 2048, 1536], P('dp', 'seq')
- grad_input: float32 [4, 2048, 1536], P('dp', 'seq')
- grad_inproj: float32 [1536, 6448], P(('dp', 'seq'))
- grad_outproj: float32 [3072, 1536], P(('dp', 'seq'))
- grad_convw: float32 [3328, 4], P(('dp', 'seq'))
- grad_convb: float32 [3328], P(('dp', 'seq'))
- grad_normgain: float32 [1536], P(('dp', 'seq'))
- grad_gategain: float32 [3072], P(('dp', 'seq'))
- grad_rate: float32 [48], replicated
- grad_dtbias: float32 [48], replicated
- grad_skip: float32 [48], replicated
The draws below stay inside these ranges and needn't reach their ends.
All inputs are finite; a program needn't handle non-finite values.
Results may differ from the reference program's by a relative error of at most 0.0077.
Values may be sent and summed in bfloat16 or wider, within the bound.
A program may use at most 192 MiB of HBM per device.

```python
import math
from functools import partial
import jax
import jax.numpy as jnp
from jax import lax

D = 1536
DIN = 3072
HDIM = 64
NSTATE = 128
CONVK = 4
BLOCK = 256
HEADS = 48
CONVCH = 3328
DPROJ = 6448
LENGTH = 2048
SEQS = 4


def shard_levels(key, dims, split, smallest, largest):
    level, own = 1.0, jax.random.fold_in(key, 6)
    for axis_at, blocks in split:
        steps = jnp.exp(jax.random.uniform(jax.random.fold_in(own, axis_at), (blocks,), jnp.float32, smallest / len(split), largest / len(split)))
        level = level * jnp.repeat(steps, dims[axis_at] // blocks).reshape([-1 if axis == axis_at else 1 for axis in range(len(dims))])
    return level


def scatter_about(key, extent, scale, limit, cuts=(), kind=jnp.bfloat16):
    drawn = jax.random.normal(key, extent, jnp.float32) * scale
    if len(cuts) > 0:
        drawn = shard_levels(key, extent, cuts, -0.22, 0.18) * drawn
    return jnp.clip(drawn, min=-limit, max=limit).astype(kind)


def setup_inputs(seed: int = 0) -> dict:
    key_list = jax.random.split(jax.random.key(seed), 12)
    tokens = scatter_about(key_list[0], (SEQS, LENGTH, D), 1.0, 6.0, ((0, 4), (1, 8)))
    cotangent = scatter_about(key_list[1], (SEQS, LENGTH, D), 1.0, 6.0, ((0, 4), (1, 8)))
    in_weight = scatter_about(key_list[2], (D, DPROJ), D ** -0.5, 0.15625, ((0, 32),))
    out_weight = scatter_about(key_list[3], (DIN, D), DIN ** -0.5, 0.109375, ((0, 32),))
    conv_weight = scatter_about(key_list[4], (CONVCH, CONVK), CONVK ** -0.5, 3.0, ((0, 32),))
    conv_bias = jnp.clip(jax.random.uniform(key_list[5], (CONVCH,), jnp.float32, -0.5, 0.5) * shard_levels(key_list[5], (CONVCH,), ((0, 32),), -0.4, 0.0), -0.5, 0.5).astype(jnp.bfloat16)
    norm_gain = jnp.clip(1.0 + 0.1 * jax.random.normal(key_list[6], (D,), jnp.float32), 0.5, 1.5).astype(jnp.bfloat16)
    gate_gain = jnp.clip(1.0 + 0.1 * jax.random.normal(key_list[7], (DIN,), jnp.float32), 0.5, 1.5).astype(jnp.bfloat16)
    decay_rate = jnp.clip(jnp.exp(jax.random.uniform(key_list[8], (HEADS,), jnp.float32, math.log(0.00012207031), math.log(0.08))), 0.00012207031, 0.08)
    dt_bias = jnp.clip(jax.random.uniform(key_list[9], (HEADS,), jnp.float32, -2.0, 0.5), -2.0, 0.5)
    d_skip = jnp.clip(jax.random.uniform(key_list[10], (HEADS,), jnp.float32, 0.5, 2.0), 0.5, 2.0)
    return dict(tokens=tokens, cotangent=cotangent, in_weight=in_weight, out_weight=out_weight, conv_weight=conv_weight, conv_bias=conv_bias, norm_gain=norm_gain, gate_gain=gate_gain, decay_rate=decay_rate, dt_bias=dt_bias, d_skip=d_skip)


epsilon = 1e-05
highest = lax.Precision.HIGHEST

def rms_scale(values, gain):
    mean_sq = lax.optimization_barrier(jnp.mean(values * values, axis=-1, keepdims=True))
    return values * lax.rsqrt(mean_sq + epsilon) * gain

def gate_norm(gate_part, mixed, gain):
    return rms_scale(mixed * jax.nn.silu(gate_part), gain)

def block_step(rate_in, state_now, pieces):
    x_heads, b_proj, c_proj, step_dt = pieces
    width = x_heads.shape[0]
    cumul = jnp.cumsum(step_dt * -rate_in, axis=0)
    cumul_h = cumul.T
    log_gaps = cumul_h[:, :, None] - cumul_h[:, None, :]
    causal = jnp.arange(width)[:, None] >= jnp.arange(width)[None, :]
    decay = jnp.exp(jnp.where(causal[None], log_gaps, -1e+30))
    scores = jnp.einsum('tn,sn->ts', c_proj, b_proj, precision=highest)
    weighted = decay * scores[None] * step_dt.T[:, None, :]
    inner_part = jnp.einsum('hts,shp->thp', weighted, x_heads, precision=highest)
    carried = jnp.einsum('hpn,tn->thp', state_now, c_proj, precision=highest) * jnp.exp(cumul)[:, :, None]
    tail_weight = jnp.exp(cumul[-1][None, :] - cumul) * step_dt
    state_new = state_now * jnp.exp(cumul[-1])[:, None, None] + jnp.einsum('shp,sn->hpn', x_heads * tail_weight[:, :, None], b_proj, precision=highest)
    return (state_new, inner_part + carried)

def ssd_blocks(x_heads, b_proj, c_proj, step_dt, rate_in, start_state):
    length = x_heads.shape[0]
    blocks = length // BLOCK
    pieces = (x_heads.reshape(blocks, BLOCK, HEADS, HDIM), b_proj.reshape(blocks, BLOCK, NSTATE), c_proj.reshape(blocks, BLOCK, NSTATE), step_dt.reshape(blocks, BLOCK, HEADS))
    stepper = jax.checkpoint(partial(block_step, rate_in))
    end_state, results = lax.scan(stepper, start_state, pieces)
    return (results.reshape(length, HEADS, HDIM), end_state)

def prepare(padded, conv_w, conv_b, dt_raw, bias_in):
    length = dt_raw.shape[0]
    filtered = conv_b
    for offset in range(CONVK):
        filtered = filtered + padded[offset:offset + length] * conv_w[:, offset]
    activated = jax.nn.silu(filtered)
    x_heads = activated[:, :DIN].reshape(length, HEADS, HDIM)
    b_proj = activated[:, DIN:DIN + NSTATE]
    c_proj = activated[:, DIN + NSTATE:]
    step_dt = jax.nn.softplus(dt_raw + bias_in)
    return (x_heads, b_proj, c_proj, step_dt)

def mix_heads(padded, conv_w, conv_b, dt_raw, rate_in, bias_in, skip_in, start_state):
    x_heads, b_proj, c_proj, step_dt = prepare(padded, conv_w, conv_b, dt_raw, bias_in)
    results, end_state = ssd_blocks(x_heads, b_proj, c_proj, step_dt, rate_in, start_state)
    mixed = results + skip_in[:, None] * x_heads
    return (mixed.reshape(dt_raw.shape[0], DIN), end_state)

def reference(tokens, cotangent, in_weight, out_weight, conv_weight, conv_bias, norm_gain, gate_gain, decay_rate, dt_bias, d_skip):
    gain_norm = norm_gain.astype(jnp.float32)
    gain_gate = gate_gain.astype(jnp.float32)
    convw_f = conv_weight.astype(jnp.float32)
    convb_f = conv_bias.astype(jnp.float32)
    zero_state = jnp.zeros((HEADS, HDIM, NSTATE), jnp.float32)
    mixer_fn = partial(mix_heads, start_state=zero_state)

    def per_sequence(totals, inputs):
        seq_x, cot_rows = inputs
        x_float = seq_x.astype(jnp.float32)
        normed = rms_scale(x_float, gain_norm).astype(jnp.bfloat16)
        projected = jnp.dot(normed, in_weight, preferred_element_type=jnp.float32).astype(jnp.bfloat16)
        gate_part = projected[:, :DIN].astype(jnp.float32)
        conv_in = projected[:, DIN:DIN + CONVCH].astype(jnp.float32)
        dt_raw = projected[:, DIN + CONVCH:].astype(jnp.float32)
        padded = jnp.concatenate([jnp.zeros((CONVK - 1, CONVCH), jnp.float32), conv_in], axis=0)
        (mixed, end_state), mixer_back = jax.vjp(mixer_fn, padded, convw_f, convb_f, dt_raw, decay_rate, dt_bias, d_skip)
        gated_f, gated_back = jax.vjp(gate_norm, gate_part, mixed, gain_gate)
        gated = gated_f.astype(jnp.bfloat16)
        block_out = (x_float + jnp.dot(gated, out_weight, preferred_element_type=jnp.float32)).astype(jnp.bfloat16)
        d_w_out = jnp.dot(gated.T, cot_rows, preferred_element_type=jnp.float32)
        d_gated = jnp.dot(cot_rows, out_weight.T, preferred_element_type=jnp.float32)
        d_gate, d_mixed, d_g2 = gated_back(d_gated)
        d_pad, d_cw, d_cb, d_raw, d_rate, d_bias, d_skp = mixer_back((d_mixed, jnp.zeros_like(end_state)))
        d_proj = jnp.concatenate([d_gate, d_pad[CONVK - 1:], d_raw], axis=1).astype(jnp.bfloat16)
        d_w_in = jnp.dot(normed.T, d_proj, preferred_element_type=jnp.float32)
        d_normed = jnp.dot(d_proj, in_weight.T, preferred_element_type=jnp.float32)
        _, norm_back = jax.vjp(rms_scale, x_float, gain_norm)
        d_xn, d_g1 = norm_back(d_normed)
        grad_x = cot_rows.astype(jnp.float32) + d_xn
        grads = (d_w_in, d_w_out, d_cw, d_cb, d_g1, d_g2, d_rate, d_bias, d_skp)
        return (jax.tree.map(lambda left, right: left + right, totals, grads), (block_out, grad_x))
    zero_grads = (jnp.zeros((D, DPROJ), jnp.float32), jnp.zeros((DIN, D), jnp.float32), jnp.zeros((CONVCH, CONVK), jnp.float32), jnp.zeros((CONVCH,), jnp.float32), jnp.zeros((D,), jnp.float32), jnp.zeros((DIN,), jnp.float32), jnp.zeros((HEADS,), jnp.float32), jnp.zeros((HEADS,), jnp.float32), jnp.zeros((HEADS,), jnp.float32))
    totals, (outputs, grads_x) = lax.scan(per_sequence, zero_grads, (tokens, cotangent))
    return (outputs, grads_x, totals[0], totals[1], totals[2], totals[3], totals[4], totals[5], totals[6], totals[7], totals[8])
```

```python
from functools import partial

import jax
import jax.numpy as jnp
from jax import lax
from jax.experimental import pallas as pl
from jax.experimental.pallas import tpu as pltpu
from jax.sharding import PartitionSpec as P

HDIM = 64
NSTATE = 128
CONVK = 4
LANES = 128
SUB = 128
TOKENS = 256
EDGE = 8

epsilon = 1e-05
highest = lax.Precision.HIGHEST
bf16 = jnp.bfloat16
f32 = jnp.float32


def dot(a, b, dims, precision=None):
    return lax.dot_general(
        a, b, (dims, ((), ())), preferred_element_type=f32, precision=precision
    )


NN, NT, TN = ((1,), (0,)), ((1,), (1,)), ((0,), (0,))


def sigmoid(a):
    return 0.5 * jnp.tanh(0.5 * a) + 0.5


def iota(shape, axis):
    return lax.broadcasted_iota(jnp.int32, shape, axis)


def steps_of(raw, bias):
    shifted = raw + bias
    return jnp.maximum(shifted, 0.0) + jnp.log1p(jnp.exp(-jnp.abs(shifted)))


def convolve(pad, conv_ref, tile, count):
    total = conv_ref[CONVK : CONVK + 1, tile]
    for k in range(CONVK):
        total = total + pad[EDGE - CONVK + 1 + k : EDGE - CONVK + 1 + k + count, tile] * conv_ref[k : k + 1, tile]
    return total


class Chunk:
    def __init__(self, step, rate):
        n = SUB
        upper = jnp.where(iota((n, n), 0) <= iota((n, n), 1), 1.0, 0.0)
        self.step = step
        self.rows = dot(step * -rate, upper, NN, highest)
        self.cols = self.rows.T
        self.step_cols = step.T

    def col(self, h):
        return jnp.broadcast_to(self.cols[:, h : h + 1], (SUB, SUB))

    def decay(self, h, col, hide):
        return jnp.exp(col - self.rows[h : h + 1, :] + hide)

    def step_col(self, h):
        return jnp.broadcast_to(self.step_cols[:, h : h + 1], (SUB, SUB))


def fwd_kernel(
    proj_ref, raw_ref, cot_ref, wout_ref, conv_ref, lane_ref, head_ref,
    y_ref, dg_ref, out_ref, state_ref, sum_ref,
    pad, act, carry, gated,
):
    block = proj_ref.shape[0]
    din = y_ref.shape[1]
    conv = conv_ref.shape[1]

    @pl.when(pl.program_id(0) == 0)
    def _():
        carry[...] = jnp.zeros_like(carry)
        pad[0:EDGE, :] = jnp.zeros((EDGE, conv), f32)

    @pl.when(pl.program_id(0) > 0)
    def _():
        pad[0:EDGE, :] = pad[block : block + EDGE, :]

    for j in range(conv // LANES):
        tile = slice(j * LANES, (j + 1) * LANES)
        pad[EDGE:, tile] = proj_ref[:, din + j * LANES : din + (j + 1) * LANES].astype(f32)
        filtered = convolve(pad, conv_ref, tile, block)
        act[:, tile] = filtered * sigmoid(filtered)
    dg_ref[...] = dot(cot_ref[...], wout_ref[...], NT)

    low = iota((SUB, LANES), 1) < HDIM
    hide = jnp.where(iota((SUB, SUB), 0) >= iota((SUB, SUB), 1), 0.0, -1e30)
    for i in range(block // SUB):
        rows = slice(i * SUB, (i + 1) * SUB)
        b = act[rows, din : din + NSTATE].astype(bf16)
        c = act[rows, din + NSTATE :].astype(bf16)
        chunk = Chunk(steps_of(raw_ref[:, rows], head_ref[1]), head_ref[0])
        scores = dot(c, b, NT)
        sq = jnp.zeros((SUB, LANES), f32)
        cross = jnp.zeros((SUB, LANES), f32)
        for j in range(din // LANES):
            tile = slice(j * LANES, (j + 1) * LANES)
            x = act[rows, tile]
            col0, col1 = chunk.col(2 * j), chunk.col(2 * j + 1)
            m0 = (chunk.decay(2 * j, col0, hide) * scores).astype(bf16)
            m1 = (chunk.decay(2 * j + 1, col1, hide) * scores).astype(bf16)
            cexp = jnp.where(low, col0, col1)
            xs = x * jnp.where(low, chunk.step_col(2 * j), chunk.step_col(2 * j + 1))
            zero = jnp.zeros_like(xs)
            split = jnp.concatenate(
                [jnp.where(low, xs, zero).astype(bf16), jnp.where(low, zero, xs).astype(bf16)], axis=0
            )
            before = carry[:, tile]
            state_ref[i, :, tile] = before.astype(bf16)
            y = dot(jnp.concatenate([m0, m1], axis=1), split, NN)
            y = y + dot(c, before.astype(bf16), NN) * jnp.exp(cexp)
            y_ref[rows, tile] = y
            last = cexp[SUB - 1 :, :]
            weighted = (xs * jnp.exp(last - cexp)).astype(bf16)
            carry[:, tile] = before * jnp.exp(last) + dot(b, weighted, TN)
            z = proj_ref[rows, tile].astype(f32)
            v = (y + lane_ref[0:1, tile] * x) * (z * sigmoid(z))
            scaled = v * lane_ref[1:2, tile]
            gated[rows, tile] = scaled.astype(bf16)
            sq = sq + v * v
            cross = cross + scaled * dg_ref[rows, tile]
        ones = jnp.ones((4, LANES), f32)
        sum_ref[0:4, rows] = dot(ones, sq, NT, highest)
        sum_ref[4:8, rows] = dot(ones, cross, NT, highest)
    out_ref[...] = dot(gated[...], wout_ref[...], NN).astype(bf16)


def bwd_kernel(
    total_din,
    proj_ref, rim_ref, raw_ref, y_ref, dg_ref, sum_ref, state_ref, cot_ref, conv_ref, lane_ref, head_ref,
    dproj_ref, draw_ref, dwout_ref, dconv_ref, dlane_ref, dhead_ref,
    pad, act, slope, dpad, carry, edge, gated, dact,
):
    block = proj_ref.shape[0]
    din = y_ref.shape[1]
    conv = conv_ref.shape[1]
    step_id = pl.program_id(0)
    first = step_id == pl.num_programs(0) - 1

    @pl.when(step_id == 0)
    def _():
        carry[...] = jnp.zeros_like(carry)
        edge[...] = jnp.zeros_like(edge)
        dpad[0:EDGE, :] = jnp.zeros((EDGE, conv), f32)
        dwout_ref[...] = jnp.zeros_like(dwout_ref)
        dconv_ref[...] = jnp.zeros_like(dconv_ref)
        dlane_ref[...] = jnp.zeros_like(dlane_ref)
        dhead_ref[...] = jnp.zeros_like(dhead_ref)

    dpad[block : block + EDGE, :] = dpad[0:EDGE, :]
    keep = jnp.where(first, 0.0, 1.0)
    for j in range(conv // LANES):
        tile = slice(j * LANES, (j + 1) * LANES)
        src = slice(din + j * LANES, din + (j + 1) * LANES)
        pad[0:EDGE, tile] = rim_ref[rim_ref.shape[0] - EDGE :, src].astype(f32) * keep
        pad[EDGE:, tile] = proj_ref[:, src].astype(f32)
        filtered = convolve(pad, conv_ref, tile, block)
        s = sigmoid(filtered)
        act[:, tile] = filtered * s
        slope[:, tile] = s * (1.0 + filtered * (1.0 - s))

    low = iota((SUB, LANES), 1) < HDIM
    hide = jnp.where(iota((SUB, SUB), 0) >= iota((SUB, SUB), 1), 0.0, -1e30)
    lower = jnp.where(iota((SUB, SUB), 0) >= iota((SUB, SUB), 1), 1.0, 0.0)
    heads = draw_ref.shape[0]
    dgain = [jnp.zeros((1, LANES), f32) for _ in range(din // LANES)]
    dskip = [jnp.zeros((1, LANES), f32) for _ in range(din // LANES)]
    for i in reversed(range(block // SUB)):
        rows = slice(i * SUB, (i + 1) * SUB)
        b = act[rows, din : din + NSTATE].astype(bf16)
        c = act[rows, din + NSTATE :].astype(bf16)
        chunk = Chunk(steps_of(raw_ref[:, rows], head_ref[1]), head_ref[0])
        scores = dot(c, b, NT)
        sums = sum_ref[:, rows].T
        scale = lax.rsqrt(jnp.broadcast_to(sums[:, 0:1], (SUB, LANES)) * (1.0 / total_din) + epsilon)
        mean = jnp.broadcast_to(sums[:, 4:5], (SUB, LANES)) * (1.0 / total_din) * (scale * scale * scale)
        dscores = jnp.zeros((SUB, SUB), f32)
        d_b = jnp.zeros((SUB, NSTATE), f32)
        d_c = jnp.zeros((SUB, NSTATE), f32)
        d_cum = jnp.zeros((heads, SUB), f32)
        d_step = jnp.zeros((heads, SUB), f32)
        reach = jnp.zeros((heads, 8), f32)
        for j in range(din // LANES):
            tile = slice(j * LANES, (j + 1) * LANES)
            x = act[rows, tile]
            y = y_ref[rows, tile]
            skip, gain = lane_ref[0:1, tile], lane_ref[1:2, tile]
            z = proj_ref[rows, tile].astype(f32)
            sz = sigmoid(z)
            mixed = y + skip * x
            silu = z * sz
            v = mixed * silu
            dg = dg_ref[rows, tile]
            vs = v * scale
            dgain[j] = dgain[j] + jnp.sum(dg * vs, axis=0, keepdims=True)
            gated[rows, tile] = (vs * gain).astype(bf16)
            dv = scale * (gain * dg) - v * mean
            dy = dv * silu
            dproj_ref[rows, tile] = (dv * mixed * (sz * (1.0 + z * (1.0 - sz)))).astype(bf16)
            dskip[j] = dskip[j] + jnp.sum(dy * x, axis=0, keepdims=True)

            col0, col1 = chunk.col(2 * j), chunk.col(2 * j + 1)
            l0, l1 = chunk.decay(2 * j, col0, hide), chunk.decay(2 * j + 1, col1, hide)
            m = jnp.concatenate([(l0 * scores).astype(bf16), (l1 * scores).astype(bf16)], axis=0)
            cexp = jnp.where(low, col0, col1)
            step = jnp.where(low, chunk.step_col(2 * j), chunk.step_col(2 * j + 1))
            last = cexp[SUB - 1 :, :]
            grow, tail = jnp.exp(cexp), jnp.exp(last - cexp)
            xs = x * step
            zero = jnp.zeros_like(dy)
            dsplit = jnp.concatenate(
                [jnp.where(low, dy, zero).astype(bf16), jnp.where(low, zero, dy).astype(bf16)], axis=0
            )
            xs16 = xs.astype(bf16)
            dm = dot(dsplit, xs16, NT)
            dscores = dscores + dm[:SUB] * l0 + dm[SUB:] * l1
            dend = carry[:, tile]
            dend16 = dend.astype(bf16)
            before = state_ref[i, :, tile]
            dxs = dot(m, dsplit, TN) + dot(b, dend16, NN) * tail
            grown = (dy * grow).astype(bf16)
            d_c = d_c + dot(grown, before, NT)
            d_b = d_b + dot((xs * tail).astype(bf16), dend16, NT)
            dprev = dend * jnp.exp(last) + dot(c, grown, TN)
            carry[:, tile] = dprev
            pick = jnp.where(lax.shift_right_logical(iota((heads, LANES), 1), 6) + 2 * j == iota((heads, LANES), 0), 1.0, 0.0)
            balance = dy.astype(bf16).astype(f32) * y - xs16.astype(f32) * dxs
            d_cum = d_cum + dot(pick, balance, NT, highest)
            d_step = d_step + dot(pick, x * dxs, NT, highest)
            crossing = jnp.sum(dprev * before.astype(f32), axis=0, keepdims=True)
            reach = reach + dot(pick, jnp.broadcast_to(crossing, (8, LANES)), NT, highest)
            dact[rows, tile] = dxs * step + skip * dy
        ds16 = dscores.astype(bf16)
        dact[rows, din : din + NSTATE] = d_b + dot(ds16, c, TN)
        dact[rows, din + NSTATE :] = d_c + dot(ds16, b, NN)
        d_log = dot(d_cum, lower, NN, highest) + edge[...]
        edge[...] = jnp.broadcast_to(reach[:, 0:1], edge.shape)
        raw = raw_ref[:, rows] + head_ref[1]
        draw = (d_step - head_ref[0] * d_log) * sigmoid(raw)
        draw_ref[:, rows] = draw
        dhead_ref[0] += -chunk.step * d_log
        dhead_ref[1] += draw
    for j in range(din // LANES):
        tile = slice(j * LANES, (j + 1) * LANES)
        dlane_ref[0:1, tile] += dskip[j]
        dlane_ref[1:2, tile] += dgain[j]
    dwout_ref[...] += dot(gated[...], cot_ref[...], TN)
    for j in range(conv // LANES):
        tile = slice(j * LANES, (j + 1) * LANES)
        df = dact[:, tile] * slope[:, tile]
        dpad[0:block, tile] = df
        dconv_ref[CONVK : CONVK + 1, tile] += jnp.sum(df, axis=0, keepdims=True)
        back = jnp.zeros((block, LANES), f32)
        for k in range(CONVK):
            shift = CONVK - 1 - k
            dconv_ref[k : k + 1, tile] += jnp.sum(
                df * pad[EDGE - shift : EDGE - shift + block, tile], axis=0, keepdims=True
            )
            back = back + conv_ref[k : k + 1, tile] * dpad[shift : shift + block, tile]
        dproj_ref[:, din + j * LANES : din + (j + 1) * LANES] = back.astype(bf16)


def rows_spec(block, width):
    return pl.BlockSpec((block, width), lambda t: (t, 0))


def whole(shape):
    return pl.BlockSpec(shape, lambda t: (0,) * len(shape))


def mixer_forward(proj, raw, cot, w_out, conv, lanes, heads):
    length, width = proj.shape
    din, d = w_out.shape
    cc = conv.shape[1]
    block = min(TOKENS, length)
    n = block // SUB
    cols = pl.BlockSpec((8, block), lambda t: (0, t))
    return pl.pallas_call(
        fwd_kernel,
        grid=(length // block,),
        in_specs=[
            rows_spec(block, width), cols, rows_spec(block, d), whole(w_out.shape),
            whole(conv.shape), whole(lanes.shape), whole(heads.shape),
        ],
        out_specs=[
            rows_spec(block, din), rows_spec(block, din), rows_spec(block, d),
            pl.BlockSpec((n, NSTATE, din), lambda t: (t, 0, 0)), cols,
        ],
        out_shape=[
            jax.ShapeDtypeStruct((length, din), f32),
            jax.ShapeDtypeStruct((length, din), f32),
            jax.ShapeDtypeStruct((length, d), bf16),
            jax.ShapeDtypeStruct((length // SUB, NSTATE, din), bf16),
            jax.ShapeDtypeStruct((8, length), f32),
        ],
        scratch_shapes=[
            pltpu.VMEM((block + EDGE, cc), f32),
            pltpu.VMEM((block, cc), f32),
            pltpu.VMEM((NSTATE, din), f32),
            pltpu.VMEM((block, din), bf16),
        ],
        name="mix_forward",
    )(proj, raw, cot, w_out, conv, lanes, heads)


def mixer_backward(total_din, proj, raw, y, dg, sums, states, cot, conv, lanes, heads):
    length, width = proj.shape
    din, d = y.shape[1], cot.shape[1]
    cc = conv.shape[1]
    block = min(TOKENS, length)
    n = block // SUB
    last = length // block - 1
    rim = 16

    def back(block, width):
        return pl.BlockSpec((block, width), lambda t: (last - t, 0))

    cols = pl.BlockSpec((8, block), lambda t: (0, last - t))
    return pl.pallas_call(
        partial(bwd_kernel, total_din),
        grid=(length // block,),
        in_specs=[
            back(block, width),
            pl.BlockSpec((rim, width), lambda t: (jnp.maximum((last - t) * (block // rim) - 1, 0), 0)),
            cols, back(block, din), back(block, din), cols,
            pl.BlockSpec((n, NSTATE, din), lambda t: (last - t, 0, 0)),
            back(block, d), whole(conv.shape), whole(lanes.shape), whole(heads.shape),
        ],
        out_specs=[
            back(block, width), cols, whole((din, d)), whole((8, cc)), whole((8, din)), whole((2, 8, SUB)),
        ],
        out_shape=[
            jax.ShapeDtypeStruct((length, width), bf16),
            jax.ShapeDtypeStruct((8, length), f32),
            jax.ShapeDtypeStruct((din, d), f32),
            jax.ShapeDtypeStruct((8, cc), f32),
            jax.ShapeDtypeStruct((8, din), f32),
            jax.ShapeDtypeStruct((2, 8, SUB), f32),
        ],
        scratch_shapes=[
            pltpu.VMEM((block + EDGE, cc), f32),
            pltpu.VMEM((block, cc), f32),
            pltpu.VMEM((block, cc), f32),
            pltpu.VMEM((block + EDGE, cc), f32),
            pltpu.VMEM((NSTATE, din), f32),
            pltpu.VMEM((8, SUB), f32),
            pltpu.VMEM((block, din), bf16),
            pltpu.VMEM((block, cc), f32),
        ],
        name="mix_backward",
    )(proj, proj, raw, y, dg, sums, states, cot, conv, lanes, heads)


def rms_scale(values, gain):
    mean_sq = jnp.mean(values * values, axis=-1, keepdims=True)
    return values * lax.rsqrt(mean_sq + epsilon) * gain


def widen(array, size, axis):
    pads = [(0, 0)] * array.ndim
    pads[axis] = (0, size - array.shape[axis])
    return jnp.pad(array, pads)


def per_device(
    tokens,
    cotangent,
    in_weight,
    out_weight,
    conv_weight,
    conv_bias,
    norm_gain,
    gate_gain,
    decay_rate,
    dt_bias,
    d_skip,
):
    ranks = lax.axis_size("seq")
    me = lax.axis_index("seq")
    both = ("dp", "seq")
    heads = decay_rate.shape[0] // ranks
    din = heads * HDIM
    padded = -(-din // LANES) * LANES
    din_all = din * ranks
    rows, width = in_weight.shape
    conv_all = din_all + 2 * NSTATE
    main = 2 * padded + 2 * NSTATE

    def mine(array, size, axis=0):
        return lax.dynamic_slice_in_dim(array, me * size, size, axis)

    x_own = tokens[0].astype(f32)
    tok = lax.all_gather(tokens[0], "seq", axis=0, tiled=True)
    cot = lax.all_gather(cotangent[0], "seq", axis=0, tiled=True)
    send = jnp.concatenate(
        [
            widen(in_weight[:, :din_all].reshape(rows, ranks, din), padded, 2),
            widen(in_weight[:, din_all : 2 * din_all].reshape(rows, ranks, din), padded, 2),
            jnp.broadcast_to(
                in_weight[:, None, 2 * din_all : 2 * din_all + 2 * NSTATE], (rows, ranks, 2 * NSTATE)
            ),
            widen(in_weight[:, din_all + conv_all :].reshape(rows, ranks, heads), 8, 2),
        ],
        axis=2,
    ).transpose(1, 0, 2)
    cols = send.shape[2]
    got = lax.all_to_all(send, "seq", 0, 0)
    w_all = lax.all_gather(got.reshape(ranks * rows, cols), "dp", axis=0, tiled=True)
    w_in, w_dt = w_all[:, :main], w_all[:, main:].T
    w_out = widen(mine(lax.all_gather(out_weight, both, axis=0, tiled=True), din), padded, 0)
    conv_w, conv_b, gain_norm, gain_gate = (
        lax.all_gather(a, both, axis=0, tiled=True).astype(f32)
        for a in (conv_weight, conv_bias, norm_gain, gate_gain)
    )
    taps = jnp.concatenate([conv_w.T, conv_b[None], jnp.zeros((8 - CONVK - 1, conv_all), f32)], axis=0)
    conv = jnp.concatenate([widen(mine(taps, din, 1), padded, 1), taps[:, din_all:]], axis=1)
    rate, bias, skip = (mine(a, heads) for a in (decay_rate, dt_bias, d_skip))
    lanes = jnp.stack([jnp.repeat(skip, HDIM), mine(gain_gate, din)])
    lanes = widen(widen(lanes, padded, 1), 8, 0)
    head_rows = jnp.broadcast_to(widen(jnp.stack([rate, bias]), 8, 1)[:, :, None], (2, 8, SUB))

    normed = rms_scale(tok.astype(f32), gain_norm).astype(bf16)
    proj = dot(normed, w_in, NN).astype(bf16)
    raw = dot(w_dt, normed, NT).astype(bf16).astype(f32)
    y, dg, out_part, states, sums = mixer_forward(proj, raw, cot, w_out, conv, lanes, head_rows)
    sums = lax.psum(sums, "seq")
    out_sum = lax.psum_scatter(out_part, "seq", scatter_dimension=0, tiled=True)
    d_proj, d_raw, d_w_out, d_conv, d_lane, d_head = mixer_backward(
        din_all, proj, raw, y, dg, sums, states, cot, conv, lanes, head_rows
    )
    own = mine(sums[0], x_own.shape[0])[:, None]
    block_out = (x_own + lax.rsqrt(own / din_all + epsilon) * out_sum.astype(f32)).astype(bf16)
    d_raw16 = d_raw.astype(bf16)
    d_normed_part = (dot(d_proj, w_in, NT) + dot(d_raw16, w_dt, TN)).astype(bf16)
    d_normed = lax.psum_scatter(d_normed_part, "seq", scatter_dimension=0, tiled=True).astype(f32)
    d_w_in = jnp.concatenate([dot(normed, d_proj, TN), dot(normed, d_raw16, ((0,), (1,)))], axis=1).astype(bf16)

    _, norm_back = jax.vjp(rms_scale, x_own, gain_norm)
    d_xn, d_g1 = norm_back(d_normed)
    grad_x = cotangent[0].astype(f32) + d_xn

    d_w_in = lax.psum_scatter(d_w_in, "dp", scatter_dimension=0, tiled=True)
    d_w_in = lax.all_to_all(d_w_in.reshape(ranks, rows, cols), "seq", 0, 0).astype(f32)
    spread = d_w_in.transpose(1, 0, 2)
    grad_in = jnp.concatenate(
        [
            spread[:, :, :din].reshape(rows, din_all),
            spread[:, :, padded : padded + din].reshape(rows, din_all),
            jnp.sum(spread[:, :, 2 * padded : main], axis=1),
            spread[:, :, main : main + heads].reshape(rows, heads * ranks),
        ],
        axis=1,
    )
    full_out = lax.dynamic_update_slice_in_dim(
        jnp.zeros((din_all, w_out.shape[1]), bf16), d_w_out[:din].astype(bf16), me * din, 0
    )
    grad_out = lax.psum_scatter(full_out, both, scatter_dimension=0, tiled=True).astype(f32)

    def place(own, size):
        return lax.dynamic_update_slice_in_dim(
            jnp.zeros((size * ranks,) + own.shape[1:], f32), own, me * size, 0
        )

    d_cw, d_cb = d_conv[:CONVK].T, d_conv[CONVK]
    full_cw = jnp.concatenate([place(d_cw[:din], din), d_cw[padded:]], axis=0)
    full_cb = jnp.concatenate([place(d_cb[:din], din), d_cb[padded:]], axis=0)
    d_skp = jnp.sum(d_lane[0, :din].reshape(heads, HDIM), axis=1)
    d_rate, d_bias = jnp.sum(d_head, axis=2)[:, :heads]
    g_cw, g_cb, g_gain, g_gate = (
        lax.psum_scatter(a, both, scatter_dimension=0, tiled=True)
        for a in (full_cw, full_cb, d_g1, place(d_lane[1, :din], din))
    )
    head_sums = lax.psum([place(a, heads) for a in (d_rate, d_bias, d_skp)], both)
    return (
        block_out[None],
        grad_x[None],
        grad_in,
        grad_out,
        g_cw,
        g_cb,
        g_gain,
        g_gate,
        head_sums[0],
        head_sums[1],
        head_sums[2],
    )


def solution(mesh):
    rows = P(("dp", "seq"), None)
    flat = P(("dp", "seq"))
    act = P("dp", "seq", None)
    return jax.shard_map(
        per_device,
        mesh=mesh,
        in_specs=(act, act, rows, rows, rows, flat, flat, flat, P(), P(), P()),
        out_specs=(act, act, rows, rows, rows, flat, flat, flat, P(), P(), P()),
        check_vma=False,
    )
```

```python
from functools import partial

import jax
import jax.numpy as jnp
from jax import lax
from jax.experimental import pallas as pl
from jax.experimental.pallas import tpu as pltpu
from jax.sharding import PartitionSpec as P

HDIM = 64
NSTATE = 128
CONVK = 4
LANES = 128
SUB = 128
TOKENS = 256
EDGE = 8

epsilon = 1e-05
highest = lax.Precision.HIGHEST
bf16 = jnp.bfloat16
f32 = jnp.float32


def dot(a, b, dims, precision=None):
    return lax.dot_general(
        a, b, (dims, ((), ())), preferred_element_type=f32, precision=precision
    )


NN, NT, TN = ((1,), (0,)), ((1,), (1,)), ((0,), (0,))


def sigmoid(a):
    return 0.5 * jnp.tanh(0.5 * a) + 0.5


def iota(shape, axis):
    return lax.broadcasted_iota(jnp.int32, shape, axis)


def parts(a):
    high = a.astype(bf16)
    return high, (a - high.astype(f32)).astype(bf16)


def fine(a, b, dims):
    left = jnp.concatenate([a[0], a[0], a[1]], axis=dims[0][0])
    right = jnp.concatenate([b[0], b[1], b[0]], axis=dims[1][0])
    return dot(left, right, dims)


def steps_of(raw, bias):
    shifted = raw + bias
    return jnp.maximum(shifted, 0.0) + jnp.log1p(jnp.exp(-jnp.abs(shifted)))


def convolve(pad, conv_ref, tile, count):
    total = conv_ref[CONVK : CONVK + 1, tile]
    for k in range(CONVK):
        total = total + pad[EDGE - CONVK + 1 + k : EDGE - CONVK + 1 + k + count, tile] * conv_ref[k : k + 1, tile]
    return total


class Chunk:
    def __init__(self, step, rate):
        n = SUB
        upper = jnp.where(iota((n, n), 0) <= iota((n, n), 1), 1.0, 0.0)
        self.step = step
        self.rows = dot(step * -rate, upper, NN, highest)
        self.cols = self.rows.T
        self.step_cols = step.T

    def col(self, h):
        return jnp.broadcast_to(self.cols[:, h : h + 1], (SUB, SUB))

    def decay(self, h, col, hide):
        return jnp.exp(col - self.rows[h : h + 1, :] + hide)

    def step_col(self, h):
        return jnp.broadcast_to(self.step_cols[:, h : h + 1], (SUB, SUB))


def fwd_kernel(
    proj_ref, raw_ref, cot_ref, wout_ref, conv_ref, lane_ref, head_ref,
    y_ref, dg_ref, out_ref, state_ref, sum_ref,
    pad, act, carry, gated,
):
    block = proj_ref.shape[0]
    din = y_ref.shape[1]
    conv = conv_ref.shape[1]

    @pl.when(pl.program_id(0) == 0)
    def _():
        carry[...] = jnp.zeros_like(carry)
        pad[0:EDGE, :] = jnp.zeros((EDGE, conv), f32)

    @pl.when(pl.program_id(0) > 0)
    def _():
        pad[0:EDGE, :] = pad[block : block + EDGE, :]

    for j in range(conv // LANES):
        tile = slice(j * LANES, (j + 1) * LANES)
        pad[EDGE:, tile] = proj_ref[:, din + j * LANES : din + (j + 1) * LANES].astype(f32)
        filtered = convolve(pad, conv_ref, tile, block)
        act[:, tile] = filtered * sigmoid(filtered)
    dg_ref[...] = dot(cot_ref[...], wout_ref[...], NT)

    low = iota((SUB, LANES), 1) < HDIM
    hide = jnp.where(iota((SUB, SUB), 0) >= iota((SUB, SUB), 1), 0.0, -1e30)
    for i in range(block // SUB):
        rows = slice(i * SUB, (i + 1) * SUB)
        b, c = parts(act[rows, din : din + NSTATE]), parts(act[rows, din + NSTATE :])
        chunk = Chunk(steps_of(raw_ref[:, rows], head_ref[1]), head_ref[0])
        scores = fine(c, b, NT)
        sq = jnp.zeros((SUB, LANES), f32)
        cross = jnp.zeros((SUB, LANES), f32)
        for j in range(din // LANES):
            tile = slice(j * LANES, (j + 1) * LANES)
            x = act[rows, tile]
            col0, col1 = chunk.col(2 * j), chunk.col(2 * j + 1)
            m0 = chunk.decay(2 * j, col0, hide) * scores
            m1 = chunk.decay(2 * j + 1, col1, hide) * scores
            cexp = jnp.where(low, col0, col1)
            xs = x * jnp.where(low, chunk.step_col(2 * j), chunk.step_col(2 * j + 1))
            zero = jnp.zeros_like(xs)
            split = jnp.concatenate([jnp.where(low, xs, zero), jnp.where(low, zero, xs)], axis=0)
            before = carry[:, tile]
            state_ref[i, :, tile] = before
            y = fine(parts(jnp.concatenate([m0, m1], axis=1)), parts(split), NN)
            y = y + fine(c, parts(before), NN) * jnp.exp(cexp)
            y_ref[rows, tile] = y
            last = cexp[SUB - 1 :, :]
            carry[:, tile] = before * jnp.exp(last) + fine(b, parts(xs * jnp.exp(last - cexp)), TN)
            z = proj_ref[rows, tile].astype(f32)
            v = (y + lane_ref[0:1, tile] * x) * (z * sigmoid(z))
            scaled = v * lane_ref[1:2, tile]
            gated[rows, tile] = scaled.astype(bf16)
            sq = sq + v * v
            cross = cross + scaled * dg_ref[rows, tile]
        ones = jnp.ones((4, LANES), f32)
        sum_ref[0:4, rows] = dot(ones, sq, NT, highest)
        sum_ref[4:8, rows] = dot(ones, cross, NT, highest)
    out_ref[...] = dot(gated[...], wout_ref[...], NN).astype(bf16)


def bwd_kernel(
    total_din,
    proj_ref, rim_ref, raw_ref, y_ref, dg_ref, sum_ref, state_ref, cot_ref, conv_ref, lane_ref, head_ref,
    dproj_ref, draw_ref, dwout_ref, dconv_ref, dlane_ref, dhead_ref,
    pad, act, slope, dpad, carry, edge, gated, dact,
):
    block = proj_ref.shape[0]
    din = y_ref.shape[1]
    conv = conv_ref.shape[1]
    step_id = pl.program_id(0)
    first = step_id == pl.num_programs(0) - 1

    @pl.when(step_id == 0)
    def _():
        carry[...] = jnp.zeros_like(carry)
        edge[...] = jnp.zeros_like(edge)
        dpad[0:EDGE, :] = jnp.zeros((EDGE, conv), f32)
        dwout_ref[...] = jnp.zeros_like(dwout_ref)
        dconv_ref[...] = jnp.zeros_like(dconv_ref)
        dlane_ref[...] = jnp.zeros_like(dlane_ref)
        dhead_ref[...] = jnp.zeros_like(dhead_ref)

    dpad[block : block + EDGE, :] = dpad[0:EDGE, :]
    keep = jnp.where(first, 0.0, 1.0)
    for j in range(conv // LANES):
        tile = slice(j * LANES, (j + 1) * LANES)
        src = slice(din + j * LANES, din + (j + 1) * LANES)
        pad[0:EDGE, tile] = rim_ref[rim_ref.shape[0] - EDGE :, src].astype(f32) * keep
        pad[EDGE:, tile] = proj_ref[:, src].astype(f32)
        filtered = convolve(pad, conv_ref, tile, block)
        s = sigmoid(filtered)
        act[:, tile] = filtered * s
        slope[:, tile] = s * (1.0 + filtered * (1.0 - s))

    low = iota((SUB, LANES), 1) < HDIM
    hide = jnp.where(iota((SUB, SUB), 0) >= iota((SUB, SUB), 1), 0.0, -1e30)
    lower = jnp.where(iota((SUB, SUB), 0) >= iota((SUB, SUB), 1), 1.0, 0.0)
    heads = draw_ref.shape[0]
    dgain = [jnp.zeros((1, LANES), f32) for _ in range(din // LANES)]
    dskip = [jnp.zeros((1, LANES), f32) for _ in range(din // LANES)]
    for i in reversed(range(block // SUB)):
        rows = slice(i * SUB, (i + 1) * SUB)
        b_parts, c_parts = parts(act[rows, din : din + NSTATE]), parts(act[rows, din + NSTATE :])
        chunk = Chunk(steps_of(raw_ref[:, rows], head_ref[1]), head_ref[0])
        scores = fine(c_parts, b_parts, NT)
        sums = sum_ref[:, rows].T
        scale = lax.rsqrt(jnp.broadcast_to(sums[:, 0:1], (SUB, LANES)) * (1.0 / total_din) + epsilon)
        mean = jnp.broadcast_to(sums[:, 4:5], (SUB, LANES)) * (1.0 / total_din) * (scale * scale * scale)
        dscores = jnp.zeros((SUB, SUB), f32)
        d_b = jnp.zeros((SUB, NSTATE), f32)
        d_c = jnp.zeros((SUB, NSTATE), f32)
        d_cum = jnp.zeros((heads, SUB), f32)
        d_step = jnp.zeros((heads, SUB), f32)
        reach = jnp.zeros((heads, 8), f32)
        for j in range(din // LANES):
            tile = slice(j * LANES, (j + 1) * LANES)
            x = act[rows, tile]
            y = y_ref[rows, tile]
            skip, gain = lane_ref[0:1, tile], lane_ref[1:2, tile]
            z = proj_ref[rows, tile].astype(f32)
            sz = sigmoid(z)
            mixed = y + skip * x
            silu = z * sz
            v = mixed * silu
            dg = dg_ref[rows, tile]
            vs = v * scale
            dgain[j] = dgain[j] + jnp.sum(dg * vs, axis=0, keepdims=True)
            gated[rows, tile] = (vs * gain).astype(bf16)
            dv = scale * (gain * dg) - v * mean
            dy = dv * silu
            dproj_ref[rows, tile] = (dv * mixed * (sz * (1.0 + z * (1.0 - sz)))).astype(bf16)
            dskip[j] = dskip[j] + jnp.sum(dy * x, axis=0, keepdims=True)

            col0, col1 = chunk.col(2 * j), chunk.col(2 * j + 1)
            l0, l1 = chunk.decay(2 * j, col0, hide), chunk.decay(2 * j + 1, col1, hide)
            m = parts(jnp.concatenate([l0 * scores, l1 * scores], axis=0))
            cexp = jnp.where(low, col0, col1)
            step = jnp.where(low, chunk.step_col(2 * j), chunk.step_col(2 * j + 1))
            last = cexp[SUB - 1 :, :]
            grow, tail = jnp.exp(cexp), jnp.exp(last - cexp)
            xs = x * step
            zero = jnp.zeros_like(dy)
            dsplit = parts(jnp.concatenate([jnp.where(low, dy, zero), jnp.where(low, zero, dy)], axis=0))
            xs_parts = parts(xs)
            dm = fine(dsplit, xs_parts, NT)
            dscores = dscores + dm[:SUB] * l0 + dm[SUB:] * l1
            dend = carry[:, tile]
            dend_parts = parts(dend)
            before = state_ref[i, :, tile]
            dxs = fine(m, dsplit, TN) + fine(b_parts, dend_parts, NN) * tail
            grown = parts(dy * grow)
            d_c = d_c + fine(grown, parts(before), NT)
            d_b = d_b + fine(parts(xs * tail), dend_parts, NT)
            dprev = dend * jnp.exp(last) + fine(c_parts, grown, TN)
            carry[:, tile] = dprev
            pick = jnp.where(lax.shift_right_logical(iota((heads, LANES), 1), 6) + 2 * j == iota((heads, LANES), 0), 1.0, 0.0)
            balance = dy * y - xs * dxs
            d_cum = d_cum + dot(pick, balance, NT, highest)
            d_step = d_step + dot(pick, x * dxs, NT, highest)
            crossing = jnp.sum(dprev * before, axis=0, keepdims=True)
            reach = reach + dot(pick, jnp.broadcast_to(crossing, (8, LANES)), NT, highest)
            dact[rows, tile] = dxs * step + skip * dy
        ds_parts = parts(dscores)
        dact[rows, din : din + NSTATE] = d_b + fine(ds_parts, c_parts, TN)
        dact[rows, din + NSTATE :] = d_c + fine(ds_parts, b_parts, NN)
        d_log = dot(d_cum, lower, NN, highest) + edge[...]
        edge[...] = jnp.broadcast_to(reach[:, 0:1], edge.shape)
        raw = raw_ref[:, rows] + head_ref[1]
        draw = (d_step - head_ref[0] * d_log) * sigmoid(raw)
        draw_ref[:, rows] = draw
        dhead_ref[0] += -chunk.step * d_log
        dhead_ref[1] += draw
    for j in range(din // LANES):
        tile = slice(j * LANES, (j + 1) * LANES)
        dlane_ref[0:1, tile] += dskip[j]
        dlane_ref[1:2, tile] += dgain[j]
    dwout_ref[...] += dot(gated[...], cot_ref[...], TN)
    for j in range(conv // LANES):
        tile = slice(j * LANES, (j + 1) * LANES)
        df = dact[:, tile] * slope[:, tile]
        dpad[0:block, tile] = df
        dconv_ref[CONVK : CONVK + 1, tile] += jnp.sum(df, axis=0, keepdims=True)
        back = jnp.zeros((block, LANES), f32)
        for k in range(CONVK):
            shift = CONVK - 1 - k
            dconv_ref[k : k + 1, tile] += jnp.sum(
                df * pad[EDGE - shift : EDGE - shift + block, tile], axis=0, keepdims=True
            )
            back = back + conv_ref[k : k + 1, tile] * dpad[shift : shift + block, tile]
        dproj_ref[:, din + j * LANES : din + (j + 1) * LANES] = back.astype(bf16)


def rows_spec(block, width):
    return pl.BlockSpec((block, width), lambda t: (t, 0))


def whole(shape):
    return pl.BlockSpec(shape, lambda t: (0,) * len(shape))


def mixer_forward(proj, raw, cot, w_out, conv, lanes, heads):
    length, width = proj.shape
    din, d = w_out.shape
    cc = conv.shape[1]
    block = min(TOKENS, length)
    n = block // SUB
    cols = pl.BlockSpec((8, block), lambda t: (0, t))
    return pl.pallas_call(
        fwd_kernel,
        grid=(length // block,),
        in_specs=[
            rows_spec(block, width), cols, rows_spec(block, d), whole(w_out.shape),
            whole(conv.shape), whole(lanes.shape), whole(heads.shape),
        ],
        out_specs=[
            rows_spec(block, din), rows_spec(block, din), rows_spec(block, d),
            pl.BlockSpec((n, NSTATE, din), lambda t: (t, 0, 0)), cols,
        ],
        out_shape=[
            jax.ShapeDtypeStruct((length, din), f32),
            jax.ShapeDtypeStruct((length, din), f32),
            jax.ShapeDtypeStruct((length, d), bf16),
            jax.ShapeDtypeStruct((length // SUB, NSTATE, din), f32),
            jax.ShapeDtypeStruct((8, length), f32),
        ],
        scratch_shapes=[
            pltpu.VMEM((block + EDGE, cc), f32),
            pltpu.VMEM((block, cc), f32),
            pltpu.VMEM((NSTATE, din), f32),
            pltpu.VMEM((block, din), bf16),
        ],
        name="mix_forward",
    )(proj, raw, cot, w_out, conv, lanes, heads)


def mixer_backward(total_din, proj, raw, y, dg, sums, states, cot, conv, lanes, heads):
    length, width = proj.shape
    din, d = y.shape[1], cot.shape[1]
    cc = conv.shape[1]
    block = min(TOKENS, length)
    n = block // SUB
    last = length // block - 1
    rim = 16

    def back(block, width):
        return pl.BlockSpec((block, width), lambda t: (last - t, 0))

    cols = pl.BlockSpec((8, block), lambda t: (0, last - t))
    return pl.pallas_call(
        partial(bwd_kernel, total_din),
        grid=(length // block,),
        in_specs=[
            back(block, width),
            pl.BlockSpec((rim, width), lambda t: (jnp.maximum((last - t) * (block // rim) - 1, 0), 0)),
            cols, back(block, din), back(block, din), cols,
            pl.BlockSpec((n, NSTATE, din), lambda t: (last - t, 0, 0)),
            back(block, d), whole(conv.shape), whole(lanes.shape), whole(heads.shape),
        ],
        out_specs=[
            back(block, width), cols, whole((din, d)), whole((8, cc)), whole((8, din)), whole((2, 8, SUB)),
        ],
        out_shape=[
            jax.ShapeDtypeStruct((length, width), bf16),
            jax.ShapeDtypeStruct((8, length), f32),
            jax.ShapeDtypeStruct((din, d), f32),
            jax.ShapeDtypeStruct((8, cc), f32),
            jax.ShapeDtypeStruct((8, din), f32),
            jax.ShapeDtypeStruct((2, 8, SUB), f32),
        ],
        scratch_shapes=[
            pltpu.VMEM((block + EDGE, cc), f32),
            pltpu.VMEM((block, cc), f32),
            pltpu.VMEM((block, cc), f32),
            pltpu.VMEM((block + EDGE, cc), f32),
            pltpu.VMEM((NSTATE, din), f32),
            pltpu.VMEM((8, SUB), f32),
            pltpu.VMEM((block, din), bf16),
            pltpu.VMEM((block, cc), f32),
        ],
        name="mix_backward",
    )(proj, proj, raw, y, dg, sums, states, cot, conv, lanes, heads)


MESH = pl.DeviceIdType.MESH


def flip(index, bit):
    return index + bit * (1 - 2 * (lax.div(index, bit) % 2))


def flip_mask(index, mask, bits):
    for bit in bits:
        if mask & bit:
            index = flip(index, bit)
    return index


def bits_of(size):
    return [1 << k for k in range(size.bit_length() - 1)]


def both_orders(size):
    bits = bits_of(size)
    slow = bits[1:]
    return [slow + bits[:1], slow[::-1] + bits[:1]]


def remote(src, dst, send, recv, to):
    return pltpu.make_async_remote_copy(
        src_ref=src, dst_ref=dst, send_sem=send, recv_sem=recv, device_id=to, device_id_type=MESH
    )


class Spread:
    def __init__(self, buf, send, recv, own=None):
        self.size = buf.shape[0]
        self.bits = bits_of(self.size)
        self.orders = both_orders(self.size)
        self.buf, self.send, self.recv = buf, send, recv
        self.me, self.dp = lax.axis_index("seq"), lax.axis_index("dp")
        self.own = own

    def masks(self, half):
        order = self.orders[half]
        got = [0]
        for bit in order:
            got = got + [m | bit for m in got]
        return got

    def copy(self, half, mask, bit):
        origin = flip_mask(self.me, mask, self.bits)
        dst = self.buf.at[origin, half]
        src = self.own.at[half] if (mask == 0 and self.own is not None) else dst
        slot = half * self.size + (mask | bit)
        return remote(src, dst, self.send.at[slot], self.recv.at[slot], (self.dp, flip(self.me, bit)))

    def start(self, half, mask):
        order = self.orders[half]
        after = max((order.index(b) for b in self.bits if mask & b), default=-1) + 1
        for bit in order[after:]:
            self.copy(half, mask, bit).start()

    def arrive(self, half, mask):
        order = self.orders[half]
        top = order[max(order.index(b) for b in self.bits if mask & b)]
        self.copy(half, mask & ~top, top).wait_recv()

    def forward(self, group):
        for k in range(1 << group, 2 << group):
            for half in range(2):
                mask = self.masks(half)[k]
                self.arrive(half, mask)
                self.start(half, mask)

    def finish(self):
        for half in range(2):
            for mask in range(1, self.size):
                order = self.orders[half]
                top = order[max(order.index(b) for b in self.bits if mask & b)]
                self.copy(half, mask & ~top, top).wait_send()

    @property
    def groups(self):
        return len(self.bits)


class Line:
    def __init__(self, at, size, send, recv):
        self.at, self.size, self.send, self.recv = at, size, send, recv
        self.me, self.seq = lax.axis_index("dp"), lax.axis_index("seq")

    def copy(self, way, hop):
        block = self.me - way * (hop - 1)
        slot = (self.size if way > 0 else 0) + hop
        ref = self.at(block)
        return remote(ref, ref, self.send.at[slot], self.recv.at[slot], (self.me + way, self.seq))

    def sends(self, way, hop):
        block = self.me - way * (hop - 1)
        to = self.me + way
        return (block >= 0) & (block < self.size) & (to >= 0) & (to < self.size)

    def start(self, hop):
        for way in (1, -1):
            @pl.when(self.sends(way, hop))
            def _():
                self.copy(way, hop).start()

    def arrive(self, hop):
        for way in (1, -1):
            source = self.me - way * hop
            @pl.when((source >= 0) & (source < self.size))
            def _():
                ref = self.at(source)
                slot = (self.size if way > 0 else 0) + hop
                pltpu.make_async_copy(ref, ref, self.recv.at[slot]).wait()

    def forward(self, hop):
        self.arrive(hop)
        if hop + 1 < self.size:
            self.start(hop + 1)

    def finish(self):
        for hop in range(1, self.size):
            for way in (1, -1):
                @pl.when(self.sends(way, hop))
                def _():
                    self.copy(way, hop).wait_send()


def greet(ranks, planes):
    me, dp = lax.axis_index("seq"), lax.axis_index("dp")
    barrier = pltpu.get_barrier_semaphore()
    for mask in range(1, ranks):
        pl.semaphore_signal(
            barrier, inc=1, device_id=(dp, flip_mask(me, mask, bits_of(ranks))), device_id_type=MESH
        )
    for way in (1, -1):
        @pl.when((dp + way >= 0) & (dp + way < planes))
        def _():
            pl.semaphore_signal(barrier, inc=1, device_id=(dp + way, me), device_id_type=MESH)
    near = jnp.where(dp > 0, 1, 0) + jnp.where(dp < planes - 1, 1, 0)
    pl.semaphore_wait(barrier, ranks - 1 + near)


def gather_kernel(
    tok_in, cot_in, w_in, wout_in, common_in,
    tok, cot, w, wout, common,
    stage, tok_s, tok_r, cot_s, cot_r, com_s, com_r, wz_s, wz_r, oz_s, oz_r, cz_s, cz_r,
    a2a_s, a2a_r, mix_s, mix_r, local,
):
    ranks, planes = tok.shape[0], w.shape[0]
    me, dp = lax.axis_index("seq"), lax.axis_index("dp")
    bits = bits_of(ranks)
    greet(ranks, planes)
    half = planes // 2
    tokens = Spread(tok, tok_s, tok_r, tok_in)
    cots = Spread(cot, cot_s, cot_r, cot_in)
    commons = Spread(common, com_s, com_r)
    w_line = Line(lambda d: w.at[d], planes, wz_s, wz_r)
    o_line = Line(lambda d: stage.at[d], planes, oz_s, oz_r)
    c_line = Line(lambda d: common.at[me, lax.div(d, half), d % half], planes, cz_s, cz_r)

    def exchange(mask):
        peer = flip_mask(me, mask, bits)
        return remote(w_in.at[peer], w.at[dp, me], a2a_s.at[mask], a2a_r.at[mask], (dp, peer))

    def arrived(mask):
        ref = w.at[dp, flip_mask(me, mask, bits)]
        return pltpu.make_async_copy(ref, ref, a2a_r.at[mask])

    for mask in range(1, ranks):
        exchange(mask).start()
    places = [
        pltpu.make_async_copy(w_in.at[me], w.at[dp, me], local.at[0]),
        pltpu.make_async_copy(common_in, common.at[me, lax.div(dp, half), dp % half], local.at[1]),
        pltpu.make_async_copy(wout_in, stage.at[dp], local.at[2]),
        pltpu.make_async_copy(tok_in, tok.at[me], local.at[3]),
        pltpu.make_async_copy(cot_in, cot.at[me], local.at[4]),
    ]
    for place in places:
        place.start()
    for h in range(2):
        tokens.start(h, 0)
    for place in places:
        place.wait()
    c_line.start(1)
    o_line.start(1)
    for mask in range(1, ranks):
        arrived(mask).wait()
    w_line.start(1)
    for hop in range(1, planes):
        c_line.forward(hop)
    tokens.forward(0)
    for h in range(2):
        commons.start(h, 0)
    w_line.forward(1)
    for group in range(1, tokens.groups - 1):
        tokens.forward(group)
    for hop in range(2, planes - 1):
        w_line.forward(hop)
    commons.forward(0)
    for h in range(2):
        cots.start(h, 0)
    tokens.forward(tokens.groups - 1)
    for group in range(1, commons.groups):
        commons.forward(group)
    o_line.forward(1)
    w_line.forward(planes - 1)
    cots.forward(0)
    for hop in range(2, planes):
        o_line.forward(hop)

    def moved(d):
        index = d * ranks + me
        return lax.div(index, planes), index % planes

    for d in range(planes):
        to, place = moved(d)

        @pl.when(to == me)
        def _():
            pltpu.make_async_copy(stage.at[d], wout.at[place], mix_r.at[place]).start()

        @pl.when(to != me)
        def _():
            remote(stage.at[d], wout.at[place], mix_s.at[d], mix_r.at[place], (dp, to)).start()

    for group in range(1, cots.groups):
        cots.forward(group)
    for place in range(planes):
        pltpu.make_async_copy(wout.at[place], wout.at[place], mix_r.at[place]).wait()
    for d in range(planes):
        to, place = moved(d)

        @pl.when(to != me)
        def _():
            remote(stage.at[d], wout.at[place], mix_s.at[d], mix_r.at[place], (dp, to)).wait_send()

    for mask in range(1, ranks):
        exchange(mask).wait_send()
    for ring in (tokens, cots, commons, w_line, o_line, c_line):
        ring.finish()


def gather_all(ranks, planes, tok, cot, w, w_out, common):
    length, d = tok.shape
    halves = (2, length // 2, d)
    dma = pltpu.SemaphoreType.DMA
    vmem = pl.BlockSpec(memory_space=pltpu.VMEM)
    ring, line = 2 * ranks, 2 * planes
    out = [
        (ranks,) + halves, (ranks,) + halves, (planes,) + w.shape, (planes,) + w_out.shape,
        (ranks, 2, planes // 2) + common.shape,
    ]
    tok_all, cot_all, w_all, out_all, common_all = pl.pallas_call(
        gather_kernel,
        in_specs=[pl.BlockSpec(memory_space=pl.ANY)] * 5,
        out_specs=[vmem] * 5,
        out_shape=[jax.ShapeDtypeStruct(s, bf16) for s in out],
        scratch_shapes=[pltpu.VMEM((planes,) + w_out.shape, bf16)]
        + [dma((ring,))] * 6
        + [dma((line,))] * 6
        + [dma((ranks,)), dma((ranks,)), dma((planes,)), dma((planes,)), dma((5,))],
        compiler_params=pltpu.CompilerParams(collective_id=0, has_side_effects=True),
        name="gather_all",
    )(tok.reshape(halves), cot.reshape(halves), w, w_out, common)
    rows = common.shape[0]
    return (
        tok_all.reshape(ranks * length, d),
        cot_all.reshape(ranks * length, d),
        w_all.reshape(planes * ranks * w.shape[1], w.shape[2]),
        out_all.reshape(planes * w_out.shape[0], d),
        common_all.reshape(ranks, planes, rows, common.shape[1]).transpose(1, 0, 2, 3),
    )


def add_into(dst, pieces, rows):
    count = dst.shape[-2]

    def body(i, _):
        at = pl.ds(pl.multiple_of(i * rows, rows), rows)
        total = pieces[0][at, :].astype(f32)
        for piece in pieces[1:]:
            total = total + piece[at, :].astype(f32)
        dst[at, :] = total.astype(dst.dtype)
        return 0

    lax.fori_loop(0, count // rows, body, 0)


def flat_views(ref):
    if len(ref.shape) == 2:
        return [ref]
    return [view for k in range(ref.shape[0]) for view in flat_views(ref.at[k])]


def add_all(dst, pieces, rows):
    for views in zip(flat_views(dst), *(flat_views(p) for p in pieces)):
        add_into(views[0], views[1:], rows)


class Collect:
    def __init__(self, acc, land, send, recv, rows):
        self.size = acc.shape[0]
        self.bits = bits_of(self.size)
        self.orders = both_orders(self.size)
        self.acc, self.land, self.send, self.recv, self.rows = acc, land, send, recv, rows
        self.me, self.dp = lax.axis_index("seq"), lax.axis_index("dp")

    def copy(self, half, mask, bit):
        slot = half * (self.size - 1) + (mask | bit) - 1
        owner = flip_mask(self.me, mask | bit, self.bits)
        return remote(
            self.acc.at[owner, half], self.land.at[slot], self.send.at[slot], self.recv.at[slot],
            (self.dp, flip(self.me, bit)),
        )

    def subsets(self, bits):
        got = [0]
        for bit in bits:
            got = got + [m | bit for m in got]
        return got

    def arrivals(self, half, mask, after):
        pieces = []
        for bit in self.orders[half][after:]:
            slot = half * (self.size - 1) + (mask | bit) - 1
            pltpu.make_async_copy(self.land.at[slot], self.land.at[slot], self.recv.at[slot]).wait()
            pieces.append(self.land.at[slot])
        return pieces

    def push(self, k):
        for half in range(2):
            order = self.orders[half]
            for mask in self.subsets(order[:k]):
                full = mask | order[k]
                pieces = self.arrivals(half, full, k + 1)
                if pieces:
                    ref = self.acc.at[flip_mask(self.me, full, self.bits), half]
                    add_all(ref, [ref] + pieces, self.rows)
                self.copy(half, mask, order[k]).start()

    def total(self, dst):
        for half in range(2):
            pieces = self.arrivals(half, 0, 0)
            add_all(dst.at[half], [self.acc.at[self.me, half]] + pieces, self.rows)

    def finish(self):
        for half in range(2):
            order = self.orders[half]
            for k in range(len(order)):
                for mask in self.subsets(order[:k]):
                    self.copy(half, mask, order[k]).wait_send()


class Fold:
    def __init__(self, at, land, size, send, recv, rows):
        self.at, self.land, self.size, self.send, self.recv, self.rows = at, land, size, send, recv, rows
        self.me, self.seq = lax.axis_index("dp"), lax.axis_index("seq")

    def copy(self, way, block):
        slot = (self.size if way > 0 else 0) + block
        return remote(
            self.at(block), self.land.at[slot], self.send.at[slot], self.recv.at[slot], (self.me + way, self.seq)
        )

    def landed(self, way, block):
        slot = (self.size if way > 0 else 0) + block
        ref = self.land.at[slot]
        pltpu.make_async_copy(ref, ref, self.recv.at[slot]).wait()
        return ref

    def sends(self, way, block):
        return block > self.me if way > 0 else block < self.me

    def push(self, t):
        for way, block in ((1, self.size - 1 - t), (-1, t)):
            @pl.when(self.sends(way, block))
            def _():
                behind = self.me - way

                @pl.when((behind >= 0) & (behind < self.size))
                def _():
                    add_all(self.at(block), [self.at(block), self.landed(way, block)], self.rows)

                self.copy(way, block).start()

    def total(self, dst):
        me = self.me
        add_all(dst, [self.at(me)], self.rows)
        for way in (1, -1):
            behind = me - way

            @pl.when((behind >= 0) & (behind < self.size))
            def _():
                add_all(dst, [dst, self.landed(way, me)], self.rows)

    def finish(self):
        for t in range(self.size):
            for way in (1, -1):
                @pl.when(self.sends(way, t))
                def _():
                    self.copy(way, t).wait_send()


def reduce_kernel(
    out_in, dn_in, w_in, o_in, c_in, s_in,
    out_sum, dn_sum, w_sum, o_sum, c_sum, s_sum,
    out_acc, dn_acc, w_acc, c_acc, s_acc, stage, own,
    out_land, dn_land, w_land, o_land, c_land, s_land, cz_land, sz_land,
    out_s, out_r, dn_s, dn_r, cr_s, cr_r, sr_s, sr_r,
    wz_s, wz_r, oz_s, oz_r, cz_s, cz_r, sz_s, sz_r,
    a2a_s, a2a_r, mix_s, mix_r, local,
):
    ranks, planes = out_in.shape[0], w_in.shape[0]
    me, dp = lax.axis_index("seq"), lax.axis_index("dp")
    bits = bits_of(ranks)
    half = planes // 2
    greet(ranks, planes)
    loads = [
        pltpu.make_async_copy(src, dst, local.at[k])
        for k, (src, dst) in enumerate(
            [(w_in, w_acc), (out_in, out_acc), (c_in, c_acc), (s_in, s_acc), (dn_in, dn_acc)]
        )
    ]
    for load in loads:
        load.start()
    outs = Collect(out_acc, out_land, out_s, out_r, 16)
    dns = Collect(dn_acc, dn_land, dn_s, dn_r, 16)
    cs = Collect(c_acc, c_land, cr_s, cr_r, c_acc.shape[-2])
    ss = Collect(s_acc, s_land, sr_s, sr_r, 8)
    w_fold = Fold(lambda d: w_acc.at[d], w_land, planes, wz_s, wz_r, w_acc.shape[-2])
    o_fold = Fold(lambda d: stage.at[d], o_land, planes, oz_s, oz_r, o_in.shape[1])
    c_fold = Fold(lambda d: own_c(d), cz_land, planes, cz_s, cz_r, c_acc.shape[-2])
    s_fold = Fold(lambda d: own_s(d), sz_land, planes, sz_s, sz_r, 8)

    def own_c(d):
        return c_acc.at[me, lax.div(d, half), d % half]

    def own_s(d):
        return s_acc.at[me, lax.div(d, half), d % half]

    def moved(k):
        index = me * planes + k
        return lax.div(index, ranks), index % ranks

    loads[0].wait()
    w_fold.push(0)
    for load in loads[1:]:
        load.wait()
    top = len(bits) - 1
    outs.push(top)
    dns.push(top)
    cs.push(top)
    ss.push(top)
    for k in range(planes):
        to_plane, to = moved(k)

        @pl.when(to == me)
        def _():
            pltpu.make_async_copy(o_in.at[k], stage.at[to_plane], mix_r.at[to_plane]).start()

        @pl.when(to != me)
        def _():
            remote(o_in.at[k], stage.at[to_plane], mix_s.at[k], mix_r.at[to_plane], (dp, to)).start()

    for k in reversed(range(top)):
        cs.push(k)
        ss.push(k)
    for k in reversed(range(1, top)):
        dns.push(k)
    c_rows = [c_acc.at[me, k] for k in range(2)]
    for h in range(2):
        for ring in (cs, ss):
            pieces = ring.arrivals(h, 0, 0)
            ref = ring.acc.at[me, h]
            add_all(ref, [ref] + pieces, ring.rows)
    for t in range(planes - 1):
        c_fold.push(t)
        s_fold.push(t)
    dns.push(0)
    for k in reversed(range(1, top)):
        outs.push(k)
    w_fold.push(1)
    for d in range(planes):
        pltpu.make_async_copy(stage.at[d], stage.at[d], mix_r.at[d]).wait()
    o_fold.push(0)
    for t in range(2, planes - 1):
        w_fold.push(t)
    outs.push(0)
    for t in range(1, planes - 1):
        o_fold.push(t)
    w_fold.total(own)

    def exchange(mask):
        peer = flip_mask(me, mask, bits)
        return remote(own.at[peer], w_sum.at[me], a2a_s.at[mask], a2a_r.at[mask], (dp, peer))

    for mask in range(1, ranks):
        exchange(mask).start()
    keep = pltpu.make_async_copy(own.at[me], w_sum.at[me], local.at[0])
    keep.start()
    dns.total(dn_sum)
    c_fold.total(c_sum)
    s_fold.total(s_sum)
    outs.total(out_sum)
    o_fold.total(o_sum)
    keep.wait()
    for mask in range(1, ranks):
        ref = w_sum.at[flip_mask(me, mask, bits)]
        pltpu.make_async_copy(ref, ref, a2a_r.at[mask]).wait()
    for mask in range(1, ranks):
        exchange(mask).wait_send()
    for k in range(planes):
        to_plane, to = moved(k)

        @pl.when(to != me)
        def _():
            remote(o_in.at[k], stage.at[to_plane], mix_s.at[k], mix_r.at[to_plane], (dp, to)).wait_send()

    for ring in (outs, dns, cs, ss, w_fold, o_fold, c_fold, s_fold):
        ring.finish()


def reduce_all(ranks, planes, out_part, dn_part, w, w_out, common, small):
    length, d = out_part.shape[0] // ranks, out_part.shape[1]
    part = (2, length // 2, d)
    rows, cols = w.shape[2:]
    dma = pltpu.SemaphoreType.DMA
    vmem = pl.BlockSpec(memory_space=pltpu.VMEM)
    cpart, spart = common.shape[1:], small.shape[1:]
    ring, line = 2 * (ranks - 1), 2 * planes
    results = pl.pallas_call(
        reduce_kernel,
        in_specs=[pl.BlockSpec(memory_space=pl.ANY)] * 6,
        out_specs=[vmem] * 6,
        out_shape=[
            jax.ShapeDtypeStruct(part, f32),
            jax.ShapeDtypeStruct(part, f32),
            jax.ShapeDtypeStruct((ranks, rows, cols), bf16),
            jax.ShapeDtypeStruct(w_out.shape[1:], f32),
            jax.ShapeDtypeStruct(cpart[2:], f32),
            jax.ShapeDtypeStruct(spart[2:], f32),
        ],
        scratch_shapes=[
            pltpu.VMEM((ranks,) + part, bf16),
            pltpu.VMEM((ranks,) + part, bf16),
            pltpu.VMEM(w.shape, bf16),
            pltpu.VMEM(common.shape, bf16),
            pltpu.VMEM(small.shape, f32),
            pltpu.VMEM(w_out.shape, bf16),
            pltpu.VMEM(w.shape[1:], bf16),
            pltpu.VMEM((ring,) + part[1:], bf16),
            pltpu.VMEM((ring,) + part[1:], bf16),
            pltpu.VMEM((line,) + w.shape[1:], bf16),
            pltpu.VMEM((line,) + w_out.shape[1:], bf16),
            pltpu.VMEM((ring,) + cpart[1:], bf16),
            pltpu.VMEM((ring,) + spart[1:], f32),
            pltpu.VMEM((line,) + cpart[2:], bf16),
            pltpu.VMEM((line,) + spart[2:], f32),
        ]
        + [dma((ring,))] * 8
        + [dma((line,))] * 8
        + [dma((ranks,)), dma((ranks,)), dma((planes,)), dma((planes,)), dma((5,))],
        compiler_params=pltpu.CompilerParams(
            collective_id=1, has_side_effects=True, vmem_limit_bytes=67043328
        ),
        name="reduce_all",
    )(out_part.reshape((ranks,) + part), dn_part.reshape((ranks,) + part), w, w_out, common, small)
    out_sum, dn_sum, w_sum, o_sum, c_sum, s_sum = results
    return out_sum.reshape(length, d), dn_sum.reshape(length, d), w_sum, o_sum, c_sum, s_sum


def rms_scale(values, gain):
    mean_sq = jnp.mean(values * values, axis=-1, keepdims=True)
    return values * lax.rsqrt(mean_sq + epsilon) * gain


def widen(array, size, axis):
    pads = [(0, 0)] * array.ndim
    pads[axis] = (0, size - array.shape[axis])
    return jnp.pad(array, pads)


def per_device(
    tokens,
    cotangent,
    in_weight,
    out_weight,
    conv_weight,
    conv_bias,
    norm_gain,
    gate_gain,
    decay_rate,
    dt_bias,
    d_skip,
):
    ranks = lax.axis_size("seq")
    me = lax.axis_index("seq")
    both = ("dp", "seq")
    heads = decay_rate.shape[0] // ranks
    din = heads * HDIM
    padded = -(-din // LANES) * LANES
    din_all = din * ranks
    rows, width = in_weight.shape
    conv_all = din_all + 2 * NSTATE
    main = 2 * padded + 2 * NSTATE

    def mine(array, size, axis=0):
        return lax.dynamic_slice_in_dim(array, me * size, size, axis)

    planes = lax.axis_size("dp")
    x_own = tokens[0].astype(f32)
    send = jnp.concatenate(
        [
            widen(in_weight[:, :din_all].reshape(rows, ranks, din), padded, 2),
            widen(in_weight[:, din_all : 2 * din_all].reshape(rows, ranks, din), padded, 2),
            widen(in_weight[:, din_all + conv_all :].reshape(rows, ranks, heads), 8, 2),
        ],
        axis=2,
    ).transpose(1, 0, 2)
    small = [norm_gain, gate_gain, conv_weight.reshape(-1), conv_bias]
    sizes = [a.shape[0] for a in small]
    packed = widen(jnp.concatenate(small), rows * LANES, 0).reshape(rows, LANES)
    shared = in_weight[:, 2 * din_all : 2 * din_all + 2 * NSTATE]
    common = jnp.concatenate([shared, packed], axis=1)
    tok, cot, w_all, w_out, common = gather_all(
        ranks, planes, tokens[0], cotangent[0], send, out_weight, common
    )
    shared = common[..., : 2 * NSTATE].reshape(-1, 2 * NSTATE)
    w_in = jnp.concatenate([w_all[:, : 2 * padded], shared], axis=1)
    w_dt = w_all[:, 2 * padded :].T
    w_out = widen(w_out, padded, 0)
    packed = common[..., 2 * NSTATE :].reshape(ranks * planes, rows * LANES).astype(f32)
    gain_norm, gain_gate, conv_w, conv_b = (
        packed[:, sum(sizes[:k]) : sum(sizes[: k + 1])].reshape(-1) for k in range(4)
    )
    conv_w = conv_w.reshape(-1, CONVK)
    taps = jnp.concatenate([conv_w.T, conv_b[None], jnp.zeros((8 - CONVK - 1, conv_all), f32)], axis=0)
    conv = jnp.concatenate([widen(mine(taps, din, 1), padded, 1), taps[:, din_all:]], axis=1)
    rate, bias, skip = (mine(a, heads) for a in (decay_rate, dt_bias, d_skip))
    lanes = jnp.stack([jnp.repeat(skip, HDIM), mine(gain_gate, din)])
    lanes = widen(widen(lanes, padded, 1), 8, 0)
    head_rows = jnp.broadcast_to(widen(jnp.stack([rate, bias]), 8, 1)[:, :, None], (2, 8, SUB))

    normed = rms_scale(tok.astype(f32), gain_norm).astype(bf16)
    proj = dot(normed, w_in, NN).astype(bf16)
    raw = dot(w_dt, normed, NT).astype(bf16).astype(f32)
    y, dg, out_part, states, sums = mixer_forward(proj, raw, cot, w_out, conv, lanes, head_rows)
    sums = lax.psum(sums, "seq")
    d_proj, d_raw, d_w_out, d_conv, d_lane, d_head = mixer_backward(
        din_all, proj, raw, y, dg, sums, states, cot, conv, lanes, head_rows
    )
    d_raw16 = d_raw.astype(bf16)
    d_normed_part = dot(d_proj, w_in, NT) + dot(d_raw16, w_dt, TN)
    x_hat = tok.astype(f32)
    x_hat = x_hat * lax.rsqrt(jnp.mean(x_hat * x_hat, axis=1, keepdims=True) + epsilon)
    d_g1 = jnp.sum(d_normed_part * x_hat, axis=0)
    d_w = dot(normed, d_proj, TN).astype(bf16)
    d_wdt = dot(normed, d_raw16, ((0,), (1,))).astype(bf16)
    d_w_main = jnp.concatenate([d_w[:, : 2 * padded], d_wdt], axis=1).reshape(planes, ranks, rows, -1)

    def by_owner(array):
        split = array.reshape((2, planes // 2, ranks) + array.shape[1:])
        return split.transpose((2, 0, 1) + tuple(range(3, split.ndim)))

    def place(own, size):
        return lax.dynamic_update_slice_in_dim(
            jnp.zeros((size * ranks,) + own.shape[1:], f32), own, me * size, 0
        )

    d_bc = d_w[:, 2 * padded :].reshape(planes * ranks, rows, 2 * NSTATE)
    d_cw, d_cb = d_conv[:CONVK].T, d_conv[CONVK]
    full_cw = jnp.concatenate([place(d_cw[:din], din), d_cw[padded:]], axis=0)
    full_cb = jnp.concatenate([place(d_cb[:din], din), d_cb[padded:]], axis=0)
    d_skp = jnp.sum(d_lane[0, :din].reshape(heads, HDIM), axis=1)
    d_rate, d_bias = jnp.sum(d_head, axis=2)[:, :heads]
    devices = planes * ranks
    head_part = jnp.concatenate([place(a, heads) for a in (d_rate, d_bias, d_skp)])
    fields = [
        a.reshape(devices, -1) for a in (full_cw, full_cb, d_g1, place(d_lane[1, :din], din))
    ] + [jnp.broadcast_to(head_part, (devices,) + head_part.shape)]
    ends = [0]
    for a in fields:
        ends.append(ends[-1] + a.shape[1])
    small = widen(jnp.concatenate(fields, axis=1), 8 * LANES, 1).reshape(devices, 8, LANES)
    out_sum, d_normed, w_sum, grad_out, bc_sum, small_sum = reduce_all(
        ranks, planes, out_part, d_normed_part.astype(bf16), d_w_main,
        d_w_out[:din].astype(bf16).reshape(planes, -1, d_w_out.shape[1]), by_owner(d_bc), by_owner(small),
    )
    own = mine(sums[0], x_own.shape[0])[:, None]
    block_out = (x_own + lax.rsqrt(own / din_all + epsilon) * out_sum).astype(bf16)
    gain = gain_norm * d_normed
    inv = lax.rsqrt(jnp.mean(x_own * x_own, axis=1, keepdims=True) + epsilon)
    d_xn = inv * (gain - x_own * (inv * inv * jnp.mean(gain * x_own, axis=1, keepdims=True)))
    grad_x = cotangent[0].astype(f32) + d_xn
    spread = w_sum.astype(f32).transpose(1, 0, 2)
    grad_in = jnp.concatenate(
        [
            spread[:, :, :din].reshape(rows, din_all),
            spread[:, :, padded : padded + din].reshape(rows, din_all),
            bc_sum,
            spread[:, :, 2 * padded : 2 * padded + heads].reshape(rows, heads * ranks),
        ],
        axis=1,
    )
    small_sum = small_sum.reshape(-1)
    g_cw, g_cb, g_gain, g_gate, head_sums = (small_sum[a:b] for a, b in zip(ends[:-1], ends[1:]))
    g_cw = g_cw.reshape(-1, CONVK)
    head_sums = head_sums.reshape(3, -1)
    return (
        block_out[None],
        grad_x[None],
        grad_in,
        grad_out,
        g_cw,
        g_cb,
        g_gain,
        g_gate,
        head_sums[0],
        head_sums[1],
        head_sums[2],
    )


def solution(mesh):
    rows = P(("dp", "seq"), None)
    flat = P(("dp", "seq"))
    act = P("dp", "seq", None)
    return jax.shard_map(
        per_device,
        mesh=mesh,
        in_specs=(act, act, rows, rows, rows, flat, flat, flat, P(), P(), P()),
        out_specs=(act, act, rows, rows, rows, flat, flat, flat, P(), P(), P()),
        check_vma=False,
    )
```

```python
from functools import partial

import jax
import jax.numpy as jnp
from jax import lax
from jax.experimental import pallas as pl
from jax.experimental.pallas import tpu as pltpu
from jax.sharding import PartitionSpec as P

HDIM = 64
NSTATE = 128
CONVK = 4
LANES = 128
SUB = 128
TOKENS = 256
EDGE = 8

epsilon = 1e-05
highest = lax.Precision.HIGHEST
bf16 = jnp.bfloat16
f32 = jnp.float32


def dot(a, b, dims, precision=None):
    return lax.dot_general(
        a, b, (dims, ((), ())), preferred_element_type=f32, precision=precision
    )


NN, NT, TN = ((1,), (0,)), ((1,), (1,)), ((0,), (0,))


def sigmoid(a):
    return 0.5 * jnp.tanh(0.5 * a) + 0.5


def iota(shape, axis):
    return lax.broadcasted_iota(jnp.int32, shape, axis)


def parts(a):
    high = a.astype(bf16)
    return high, (a - high.astype(f32)).astype(bf16)


def fine(a, b, dims):
    left = jnp.concatenate([a[0], a[0], a[1]], axis=dims[0][0])
    right = jnp.concatenate([b[0], b[1], b[0]], axis=dims[1][0])
    return dot(left, right, dims)


def steps_of(raw, bias):
    shifted = raw + bias
    return jnp.maximum(shifted, 0.0) + jnp.log1p(jnp.exp(-jnp.abs(shifted)))


def convolve(pad, conv_ref, tile, count):
    total = conv_ref[CONVK : CONVK + 1, tile]
    for k in range(CONVK):
        total = total + pad[EDGE - CONVK + 1 + k : EDGE - CONVK + 1 + k + count, tile] * conv_ref[k : k + 1, tile]
    return total


class Chunk:
    def __init__(self, step, rate):
        n = SUB
        upper = jnp.where(iota((n, n), 0) <= iota((n, n), 1), 1.0, 0.0)
        self.step = step
        self.rows = dot(step * -rate, upper, NN, highest)
        self.cols = self.rows.T
        self.step_cols = step.T

    def col(self, h):
        return jnp.broadcast_to(self.cols[:, h : h + 1], (SUB, SUB))

    def decay(self, h, col, hide):
        return jnp.exp(col - self.rows[h : h + 1, :] + hide)

    def step_col(self, h):
        return jnp.broadcast_to(self.step_cols[:, h : h + 1], (SUB, SUB))


def fwd_kernel(
    proj_ref, raw_ref, cot_ref, wout_ref, conv_ref, lane_ref, head_ref,
    y_ref, dg_ref, out_ref, state_ref, sum_ref,
    pad, act, carry, gated,
):
    block = proj_ref.shape[0]
    din = y_ref.shape[1]
    conv = conv_ref.shape[1]

    @pl.when(pl.program_id(0) == 0)
    def _():
        carry[...] = jnp.zeros_like(carry)
        pad[0:EDGE, :] = jnp.zeros((EDGE, conv), f32)

    @pl.when(pl.program_id(0) > 0)
    def _():
        pad[0:EDGE, :] = pad[block : block + EDGE, :]

    for j in range(conv // LANES):
        tile = slice(j * LANES, (j + 1) * LANES)
        pad[EDGE:, tile] = proj_ref[:, din + j * LANES : din + (j + 1) * LANES].astype(f32)
        filtered = convolve(pad, conv_ref, tile, block)
        act[:, tile] = filtered * sigmoid(filtered)
    dg_ref[...] = dot(cot_ref[...], wout_ref[...], NT)

    low = iota((SUB, LANES), 1) < HDIM
    hide = jnp.where(iota((SUB, SUB), 0) >= iota((SUB, SUB), 1), 0.0, -1e30)
    for i in range(block // SUB):
        rows = slice(i * SUB, (i + 1) * SUB)
        b, c = parts(act[rows, din : din + NSTATE]), parts(act[rows, din + NSTATE :])
        chunk = Chunk(steps_of(raw_ref[:, rows], head_ref[1]), head_ref[0])
        scores = fine(c, b, NT)
        sq = jnp.zeros((SUB, LANES), f32)
        cross = jnp.zeros((SUB, LANES), f32)
        for j in range(din // LANES):
            tile = slice(j * LANES, (j + 1) * LANES)
            x = act[rows, tile]
            col0, col1 = chunk.col(2 * j), chunk.col(2 * j + 1)
            m0 = chunk.decay(2 * j, col0, hide) * scores
            m1 = chunk.decay(2 * j + 1, col1, hide) * scores
            cexp = jnp.where(low, col0, col1)
            xs = x * jnp.where(low, chunk.step_col(2 * j), chunk.step_col(2 * j + 1))
            zero = jnp.zeros_like(xs)
            split = jnp.concatenate([jnp.where(low, xs, zero), jnp.where(low, zero, xs)], axis=0)
            before = carry[:, tile]
            state_ref[i, :, tile] = before
            y = fine(parts(jnp.concatenate([m0, m1], axis=1)), parts(split), NN)
            y = y + fine(c, parts(before), NN) * jnp.exp(cexp)
            y_ref[rows, tile] = y
            last = cexp[SUB - 1 :, :]
            carry[:, tile] = before * jnp.exp(last) + fine(b, parts(xs * jnp.exp(last - cexp)), TN)
            z = proj_ref[rows, tile].astype(f32)
            v = (y + lane_ref[0:1, tile] * x) * (z * sigmoid(z))
            scaled = v * lane_ref[1:2, tile]
            gated[rows, tile] = scaled.astype(bf16)
            sq = sq + v * v
            cross = cross + scaled * dg_ref[rows, tile]
        ones = jnp.ones((4, LANES), f32)
        sum_ref[0:4, rows] = dot(ones, sq, NT, highest)
        sum_ref[4:8, rows] = dot(ones, cross, NT, highest)
    out_ref[...] = dot(gated[...], wout_ref[...], NN).astype(bf16)


def bwd_kernel(
    total_din,
    proj_ref, rim_ref, raw_ref, y_ref, dg_ref, sum_ref, state_ref, cot_ref, conv_ref, lane_ref, head_ref,
    dproj_ref, draw_ref, dwout_ref, dconv_ref, dlane_ref, dhead_ref,
    pad, act, slope, dpad, carry, edge, gated, dact,
):
    block = proj_ref.shape[0]
    din = y_ref.shape[1]
    conv = conv_ref.shape[1]
    step_id = pl.program_id(0)
    first = step_id == pl.num_programs(0) - 1

    @pl.when(step_id == 0)
    def _():
        carry[...] = jnp.zeros_like(carry)
        edge[...] = jnp.zeros_like(edge)
        dpad[0:EDGE, :] = jnp.zeros((EDGE, conv), f32)
        dwout_ref[...] = jnp.zeros_like(dwout_ref)
        dconv_ref[...] = jnp.zeros_like(dconv_ref)
        dlane_ref[...] = jnp.zeros_like(dlane_ref)
        dhead_ref[...] = jnp.zeros_like(dhead_ref)

    dpad[block : block + EDGE, :] = dpad[0:EDGE, :]
    keep = jnp.where(first, 0.0, 1.0)
    for j in range(conv // LANES):
        tile = slice(j * LANES, (j + 1) * LANES)
        src = slice(din + j * LANES, din + (j + 1) * LANES)
        pad[0:EDGE, tile] = rim_ref[rim_ref.shape[0] - EDGE :, src].astype(f32) * keep
        pad[EDGE:, tile] = proj_ref[:, src].astype(f32)
        filtered = convolve(pad, conv_ref, tile, block)
        s = sigmoid(filtered)
        act[:, tile] = filtered * s
        slope[:, tile] = s * (1.0 + filtered * (1.0 - s))

    low = iota((SUB, LANES), 1) < HDIM
    hide = jnp.where(iota((SUB, SUB), 0) >= iota((SUB, SUB), 1), 0.0, -1e30)
    lower = jnp.where(iota((SUB, SUB), 0) >= iota((SUB, SUB), 1), 1.0, 0.0)
    heads = draw_ref.shape[0]
    dgain = [jnp.zeros((1, LANES), f32) for _ in range(din // LANES)]
    dskip = [jnp.zeros((1, LANES), f32) for _ in range(din // LANES)]
    for i in reversed(range(block // SUB)):
        rows = slice(i * SUB, (i + 1) * SUB)
        b_parts, c_parts = parts(act[rows, din : din + NSTATE]), parts(act[rows, din + NSTATE :])
        chunk = Chunk(steps_of(raw_ref[:, rows], head_ref[1]), head_ref[0])
        scores = fine(c_parts, b_parts, NT)
        sums = sum_ref[:, rows].T
        scale = lax.rsqrt(jnp.broadcast_to(sums[:, 0:1], (SUB, LANES)) * (1.0 / total_din) + epsilon)
        mean = jnp.broadcast_to(sums[:, 4:5], (SUB, LANES)) * (1.0 / total_din) * (scale * scale * scale)
        dscores = jnp.zeros((SUB, SUB), f32)
        d_b = jnp.zeros((SUB, NSTATE), f32)
        d_c = jnp.zeros((SUB, NSTATE), f32)
        d_cum = jnp.zeros((heads, SUB), f32)
        d_step = jnp.zeros((heads, SUB), f32)
        reach = jnp.zeros((heads, 8), f32)
        for j in range(din // LANES):
            tile = slice(j * LANES, (j + 1) * LANES)
            x = act[rows, tile]
            y = y_ref[rows, tile]
            skip, gain = lane_ref[0:1, tile], lane_ref[1:2, tile]
            z = proj_ref[rows, tile].astype(f32)
            sz = sigmoid(z)
            mixed = y + skip * x
            silu = z * sz
            v = mixed * silu
            dg = dg_ref[rows, tile]
            vs = v * scale
            dgain[j] = dgain[j] + jnp.sum(dg * vs, axis=0, keepdims=True)
            gated[rows, tile] = (vs * gain).astype(bf16)
            dv = scale * (gain * dg) - v * mean
            dy = dv * silu
            dproj_ref[rows, tile] = (dv * mixed * (sz * (1.0 + z * (1.0 - sz)))).astype(bf16)
            dskip[j] = dskip[j] + jnp.sum(dy * x, axis=0, keepdims=True)

            col0, col1 = chunk.col(2 * j), chunk.col(2 * j + 1)
            l0, l1 = chunk.decay(2 * j, col0, hide), chunk.decay(2 * j + 1, col1, hide)
            m = parts(jnp.concatenate([l0 * scores, l1 * scores], axis=0))
            cexp = jnp.where(low, col0, col1)
            step = jnp.where(low, chunk.step_col(2 * j), chunk.step_col(2 * j + 1))
            last = cexp[SUB - 1 :, :]
            grow, tail = jnp.exp(cexp), jnp.exp(last - cexp)
            xs = x * step
            zero = jnp.zeros_like(dy)
            dsplit = parts(jnp.concatenate([jnp.where(low, dy, zero), jnp.where(low, zero, dy)], axis=0))
            xs_parts = parts(xs)
            dm = fine(dsplit, xs_parts, NT)
            dscores = dscores + dm[:SUB] * l0 + dm[SUB:] * l1
            dend = carry[:, tile]
            dend_parts = parts(dend)
            before = state_ref[i, :, tile]
            dxs = fine(m, dsplit, TN) + fine(b_parts, dend_parts, NN) * tail
            grown = parts(dy * grow)
            d_c = d_c + fine(grown, parts(before), NT)
            d_b = d_b + fine(parts(xs * tail), dend_parts, NT)
            dprev = dend * jnp.exp(last) + fine(c_parts, grown, TN)
            carry[:, tile] = dprev
            pick = jnp.where(lax.shift_right_logical(iota((heads, LANES), 1), 6) + 2 * j == iota((heads, LANES), 0), 1.0, 0.0)
            balance = dy * y - xs * dxs
            d_cum = d_cum + dot(pick, balance, NT, highest)
            d_step = d_step + dot(pick, x * dxs, NT, highest)
            crossing = jnp.sum(dprev * before, axis=0, keepdims=True)
            reach = reach + dot(pick, jnp.broadcast_to(crossing, (8, LANES)), NT, highest)
            dact[rows, tile] = dxs * step + skip * dy
        ds_parts = parts(dscores)
        dact[rows, din : din + NSTATE] = d_b + fine(ds_parts, c_parts, TN)
        dact[rows, din + NSTATE :] = d_c + fine(ds_parts, b_parts, NN)
        d_log = dot(d_cum, lower, NN, highest) + edge[...]
        edge[...] = jnp.broadcast_to(reach[:, 0:1], edge.shape)
        raw = raw_ref[:, rows] + head_ref[1]
        draw = (d_step - head_ref[0] * d_log) * sigmoid(raw)
        draw_ref[:, rows] = draw
        dhead_ref[0] += -chunk.step * d_log
        dhead_ref[1] += draw
    for j in range(din // LANES):
        tile = slice(j * LANES, (j + 1) * LANES)
        dlane_ref[0:1, tile] += dskip[j]
        dlane_ref[1:2, tile] += dgain[j]
    dwout_ref[...] += dot(gated[...], cot_ref[...], TN)
    for j in range(conv // LANES):
        tile = slice(j * LANES, (j + 1) * LANES)
        df = dact[:, tile] * slope[:, tile]
        dpad[0:block, tile] = df
        dconv_ref[CONVK : CONVK + 1, tile] += jnp.sum(df, axis=0, keepdims=True)
        back = jnp.zeros((block, LANES), f32)
        for k in range(CONVK):
            shift = CONVK - 1 - k
            dconv_ref[k : k + 1, tile] += jnp.sum(
                df * pad[EDGE - shift : EDGE - shift + block, tile], axis=0, keepdims=True
            )
            back = back + conv_ref[k : k + 1, tile] * dpad[shift : shift + block, tile]
        dproj_ref[:, din + j * LANES : din + (j + 1) * LANES] = back.astype(bf16)


def rows_spec(block, width):
    return pl.BlockSpec((block, width), lambda t: (t, 0))


def whole(shape):
    return pl.BlockSpec(shape, lambda t: (0,) * len(shape))


def mixer_forward(proj, raw, cot, w_out, conv, lanes, heads):
    length, width = proj.shape
    din, d = w_out.shape
    cc = conv.shape[1]
    block = min(TOKENS, length)
    n = block // SUB
    cols = pl.BlockSpec((8, block), lambda t: (0, t))
    return pl.pallas_call(
        fwd_kernel,
        grid=(length // block,),
        in_specs=[
            rows_spec(block, width), cols, rows_spec(block, d), whole(w_out.shape),
            whole(conv.shape), whole(lanes.shape), whole(heads.shape),
        ],
        out_specs=[
            rows_spec(block, din), rows_spec(block, din), rows_spec(block, d),
            pl.BlockSpec((n, NSTATE, din), lambda t: (t, 0, 0)), cols,
        ],
        out_shape=[
            jax.ShapeDtypeStruct((length, din), f32),
            jax.ShapeDtypeStruct((length, din), f32),
            jax.ShapeDtypeStruct((length, d), bf16),
            jax.ShapeDtypeStruct((length // SUB, NSTATE, din), f32),
            jax.ShapeDtypeStruct((8, length), f32),
        ],
        scratch_shapes=[
            pltpu.VMEM((block + EDGE, cc), f32),
            pltpu.VMEM((block, cc), f32),
            pltpu.VMEM((NSTATE, din), f32),
            pltpu.VMEM((block, din), bf16),
        ],
        name="mix_forward",
    )(proj, raw, cot, w_out, conv, lanes, heads)


def mixer_backward(total_din, proj, raw, y, dg, sums, states, cot, conv, lanes, heads):
    length, width = proj.shape
    din, d = y.shape[1], cot.shape[1]
    cc = conv.shape[1]
    block = min(TOKENS, length)
    n = block // SUB
    last = length // block - 1
    rim = 16

    def back(block, width):
        return pl.BlockSpec((block, width), lambda t: (last - t, 0))

    cols = pl.BlockSpec((8, block), lambda t: (0, last - t))
    return pl.pallas_call(
        partial(bwd_kernel, total_din),
        grid=(length // block,),
        in_specs=[
            back(block, width),
            pl.BlockSpec((rim, width), lambda t: (jnp.maximum((last - t) * (block // rim) - 1, 0), 0)),
            cols, back(block, din), back(block, din), cols,
            pl.BlockSpec((n, NSTATE, din), lambda t: (last - t, 0, 0)),
            back(block, d), whole(conv.shape), whole(lanes.shape), whole(heads.shape),
        ],
        out_specs=[
            back(block, width), cols, whole((din, d)), whole((8, cc)), whole((8, din)), whole((2, 8, SUB)),
        ],
        out_shape=[
            jax.ShapeDtypeStruct((length, width), bf16),
            jax.ShapeDtypeStruct((8, length), f32),
            jax.ShapeDtypeStruct((din, d), f32),
            jax.ShapeDtypeStruct((8, cc), f32),
            jax.ShapeDtypeStruct((8, din), f32),
            jax.ShapeDtypeStruct((2, 8, SUB), f32),
        ],
        scratch_shapes=[
            pltpu.VMEM((block + EDGE, cc), f32),
            pltpu.VMEM((block, cc), f32),
            pltpu.VMEM((block, cc), f32),
            pltpu.VMEM((block + EDGE, cc), f32),
            pltpu.VMEM((NSTATE, din), f32),
            pltpu.VMEM((8, SUB), f32),
            pltpu.VMEM((block, din), bf16),
            pltpu.VMEM((block, cc), f32),
        ],
        name="mix_backward",
    )(proj, proj, raw, y, dg, sums, states, cot, conv, lanes, heads)


MESH = pl.DeviceIdType.MESH


def flip(index, bit):
    return index + bit * (1 - 2 * (lax.div(index, bit) % 2))


def flip_mask(index, mask, bits):
    for bit in bits:
        if mask & bit:
            index = flip(index, bit)
    return index


def bits_of(size):
    return [1 << k for k in range(size.bit_length() - 1)]


def both_orders(size):
    bits = bits_of(size)
    slow = bits[1:]
    return [slow + bits[:1], slow[::-1] + bits[:1]]


def remote(src, dst, send, recv, to):
    return pltpu.make_async_remote_copy(
        src_ref=src, dst_ref=dst, send_sem=send, recv_sem=recv, device_id=to, device_id_type=MESH
    )


class Spread:
    def __init__(self, buf, send, recv, own=None):
        self.size = buf.shape[0]
        self.bits = bits_of(self.size)
        self.orders = both_orders(self.size)
        self.buf, self.send, self.recv = buf, send, recv
        self.me, self.dp = lax.axis_index("seq"), lax.axis_index("dp")
        self.own = own

    def masks(self, half):
        order = self.orders[half]
        got = [0]
        for bit in order:
            got = got + [m | bit for m in got]
        return got

    def copy(self, half, mask, bit):
        origin = flip_mask(self.me, mask, self.bits)
        dst = self.buf.at[origin, half]
        src = self.own.at[half] if (mask == 0 and self.own is not None) else dst
        slot = half * self.size + (mask | bit)
        return remote(src, dst, self.send.at[slot], self.recv.at[slot], (self.dp, flip(self.me, bit)))

    def start(self, half, mask):
        order = self.orders[half]
        after = max((order.index(b) for b in self.bits if mask & b), default=-1) + 1
        for bit in order[after:]:
            self.copy(half, mask, bit).start()

    def arrive(self, half, mask):
        order = self.orders[half]
        top = order[max(order.index(b) for b in self.bits if mask & b)]
        self.copy(half, mask & ~top, top).wait_recv()

    def forward(self, group):
        for k in range(1 << group, 2 << group):
            for half in range(2):
                mask = self.masks(half)[k]
                self.arrive(half, mask)
                self.start(half, mask)

    def finish(self):
        for half in range(2):
            for mask in range(1, self.size):
                order = self.orders[half]
                top = order[max(order.index(b) for b in self.bits if mask & b)]
                self.copy(half, mask & ~top, top).wait_send()

    @property
    def groups(self):
        return len(self.bits)


class Line:
    def __init__(self, at, size, send, recv):
        self.at, self.size, self.send, self.recv = at, size, send, recv
        self.me, self.seq = lax.axis_index("dp"), lax.axis_index("seq")

    def copy(self, way, hop):
        block = self.me - way * (hop - 1)
        slot = (self.size if way > 0 else 0) + hop
        ref = self.at(block)
        return remote(ref, ref, self.send.at[slot], self.recv.at[slot], (self.me + way, self.seq))

    def sends(self, way, hop):
        block = self.me - way * (hop - 1)
        to = self.me + way
        return (block >= 0) & (block < self.size) & (to >= 0) & (to < self.size)

    def start(self, hop):
        for way in (1, -1):
            @pl.when(self.sends(way, hop))
            def _():
                self.copy(way, hop).start()

    def arrive(self, hop):
        for way in (1, -1):
            source = self.me - way * hop
            @pl.when((source >= 0) & (source < self.size))
            def _():
                ref = self.at(source)
                slot = (self.size if way > 0 else 0) + hop
                pltpu.make_async_copy(ref, ref, self.recv.at[slot]).wait()

    def forward(self, hop):
        self.arrive(hop)
        if hop + 1 < self.size:
            self.start(hop + 1)

    def finish(self):
        for hop in range(1, self.size):
            for way in (1, -1):
                @pl.when(self.sends(way, hop))
                def _():
                    self.copy(way, hop).wait_send()


def greet(ranks, planes):
    me, dp = lax.axis_index("seq"), lax.axis_index("dp")
    barrier = pltpu.get_barrier_semaphore()
    for mask in range(1, ranks):
        pl.semaphore_signal(
            barrier, inc=1, device_id=(dp, flip_mask(me, mask, bits_of(ranks))), device_id_type=MESH
        )
    for way in (1, -1):
        @pl.when((dp + way >= 0) & (dp + way < planes))
        def _():
            pl.semaphore_signal(barrier, inc=1, device_id=(dp + way, me), device_id_type=MESH)
    near = jnp.where(dp > 0, 1, 0) + jnp.where(dp < planes - 1, 1, 0)
    pl.semaphore_wait(barrier, ranks - 1 + near)


def project(tok, w, common, normed, proj, raw, w_full):
    ranks, planes = tok.shape[0], w.shape[0]
    rows, width = w.shape[2:]
    strip, tile = 32, tok.shape[2]
    d = tok.shape[3]
    half = planes // 2

    def lay(i, gains):
        at = pl.ds(pl.multiple_of(i * rows, 16), rows)
        plane, rank = lax.div(i, ranks), i % ranks
        shared = common[rank, lax.div(plane, half), plane % half]
        w_full[at, :width] = w[plane, rank]
        w_full[at, width:] = shared
        return gains + shared[: d // HDIM, 2 * NSTATE :].astype(f32)

    gains = lax.fori_loop(0, planes * ranks, lay, jnp.zeros((d // HDIM, LANES), f32))
    moved = pltpu.roll(gains, HDIM, 1)
    low = iota((1, LANES), 1) < HDIM
    gain = [jnp.where(low, moved[2 * j : 2 * j + 1], gains[2 * j + 1 : 2 * j + 2]) for j in range(d // LANES)]

    def norm(i, _):
        per = tile // strip
        part = lax.div(i, per)
        at = pl.ds(pl.multiple_of((i % per) * strip, strip), strip)
        x = tok.at[lax.div(part, 2), part % 2][at, :].astype(f32)
        scale = lax.rsqrt(jnp.sum(x * x, axis=1, keepdims=True) * (1.0 / d) + epsilon)
        to = pl.ds(pl.multiple_of(i * strip, strip), strip)
        for j in range(d // LANES):
            cut = slice(j * LANES, (j + 1) * LANES)
            normed[to, cut] = (x[:, cut] * scale * gain[j]).astype(bf16)
        return 0

    lax.fori_loop(0, ranks * 2 * tile // strip, norm, 0)
    main = width + 2 * NSTATE

    def multiply(i, _):
        at = pl.ds(pl.multiple_of(i * 256, 256), 256)
        for start in range(0, main, 512):
            cut = slice(start, min(start + 512, main))
            proj[at, cut] = dot(normed[at, :], w_full[:, cut], NN).astype(bf16)
        steps = dot(normed[at, :], w_full[:, main:], NN).astype(bf16).astype(f32)
        for k in range(2):
            to = pl.ds(pl.multiple_of(i * 256 + k * LANES, LANES), LANES)
            raw[:, to] = steps[k * LANES : (k + 1) * LANES].T[: raw.shape[0]]
        return 0

    lax.fori_loop(0, ranks * 2 * tile // 256, multiply, 0)


def gather_kernel(
    fused, tok_in, cot_in, w_in, wout_in, common_in,
    cot, wout, common, *rest,
):
    if fused:
        normed, proj, raw, w_full, tok, w, *rest = rest
    else:
        tok, w, *rest = rest
    (stage, tok_s, tok_r, cot_s, cot_r, com_s, com_r, wz_s, wz_r, oz_s, oz_r, cz_s, cz_r,
    a2a_s, a2a_r, mix_s, mix_r, local) = rest
    ranks, planes = tok.shape[0], w.shape[0]
    me, dp = lax.axis_index("seq"), lax.axis_index("dp")
    bits = bits_of(ranks)
    greet(ranks, planes)
    half = planes // 2
    tokens = Spread(tok, tok_s, tok_r, tok_in)
    cots = Spread(cot, cot_s, cot_r, cot_in)
    commons = Spread(common, com_s, com_r)
    w_line = Line(lambda d: w.at[d], planes, wz_s, wz_r)
    o_line = Line(lambda d: stage.at[d], planes, oz_s, oz_r)
    c_line = Line(lambda d: common.at[me, lax.div(d, half), d % half], planes, cz_s, cz_r)

    def exchange(mask):
        peer = flip_mask(me, mask, bits)
        return remote(w_in.at[peer], w.at[dp, me], a2a_s.at[mask], a2a_r.at[mask], (dp, peer))

    def arrived(mask):
        ref = w.at[dp, flip_mask(me, mask, bits)]
        return pltpu.make_async_copy(ref, ref, a2a_r.at[mask])

    for mask in range(1, ranks):
        exchange(mask).start()
    places = [
        pltpu.make_async_copy(w_in.at[me], w.at[dp, me], local.at[0]),
        pltpu.make_async_copy(common_in, common.at[me, lax.div(dp, half), dp % half], local.at[1]),
        pltpu.make_async_copy(wout_in, stage.at[dp], local.at[2]),
        pltpu.make_async_copy(tok_in, tok.at[me], local.at[3]),
        pltpu.make_async_copy(cot_in, cot.at[me], local.at[4]),
    ]
    for place in places:
        place.start()
    for h in range(2):
        tokens.start(h, 0)
    for place in places:
        place.wait()
    c_line.start(1)
    o_line.start(1)
    for mask in range(1, ranks):
        arrived(mask).wait()
    w_line.start(1)
    for hop in range(1, planes):
        c_line.forward(hop)
    tokens.forward(0)
    for h in range(2):
        commons.start(h, 0)
    w_line.forward(1)
    for group in range(1, tokens.groups - 1):
        tokens.forward(group)
    for hop in range(2, planes - 1):
        w_line.forward(hop)
    commons.forward(0)
    for h in range(2):
        cots.start(h, 0)
    tokens.forward(tokens.groups - 1)
    for group in range(1, commons.groups):
        commons.forward(group)
    o_line.forward(1)
    w_line.forward(planes - 1)
    cots.forward(0)
    for hop in range(2, planes):
        o_line.forward(hop)

    def moved(d):
        index = d * ranks + me
        return lax.div(index, planes), index % planes

    for d in range(planes):
        to, place = moved(d)

        @pl.when(to == me)
        def _():
            pltpu.make_async_copy(stage.at[d], wout.at[place], mix_r.at[place]).start()

        @pl.when(to != me)
        def _():
            remote(stage.at[d], wout.at[place], mix_s.at[d], mix_r.at[place], (dp, to)).start()

    if fused:
        project(tok, w, common, normed, proj, raw, w_full)
    for group in range(1, cots.groups):
        cots.forward(group)
    for place in range(planes):
        pltpu.make_async_copy(wout.at[place], wout.at[place], mix_r.at[place]).wait()
    for d in range(planes):
        to, place = moved(d)

        @pl.when(to != me)
        def _():
            remote(stage.at[d], wout.at[place], mix_s.at[d], mix_r.at[place], (dp, to)).wait_send()

    for mask in range(1, ranks):
        exchange(mask).wait_send()
    for ring in (tokens, cots, commons, w_line, o_line, c_line):
        ring.finish()


def gather_all(ranks, planes, tok, cot, w, w_out, common):
    length, d = tok.shape
    halves = (2, length // 2, d)
    total = ranks * length
    rows, cols = w.shape[1:]
    fused = rows % 16 == 0 and rows * HDIM >= 2 * d and length % 256 == 0
    dma = pltpu.SemaphoreType.DMA
    vmem = pl.BlockSpec(memory_space=pltpu.VMEM)
    ring, line = 2 * ranks, 2 * planes
    buffers = [((ranks,) + halves, bf16), ((planes,) + w.shape, bf16)]
    out = [
        ((ranks,) + halves, bf16), ((planes,) + w_out.shape, bf16), ((ranks, 2, planes // 2) + common.shape, bf16)
    ]
    if fused:
        out += [
            ((total, d), bf16), ((total, cols + 2 * NSTATE), bf16), ((HDIM, total), f32),
            ((d, cols + common.shape[1]), bf16),
        ]
    else:
        out += buffers
    cot_all, out_all, common_all, *rest = pl.pallas_call(
        partial(gather_kernel, fused),
        in_specs=[pl.BlockSpec(memory_space=pl.ANY)] * 5,
        out_specs=[vmem] * len(out),
        out_shape=[jax.ShapeDtypeStruct(*s) for s in out],
        scratch_shapes=([pltpu.VMEM(*s) for s in buffers] if fused else [])
        + [pltpu.VMEM((planes,) + w_out.shape, bf16)]
        + [dma((ring,))] * 6
        + [dma((line,))] * 6
        + [dma((ranks,)), dma((ranks,)), dma((planes,)), dma((planes,)), dma((5,))],
        compiler_params=pltpu.CompilerParams(
            collective_id=0, has_side_effects=True, vmem_limit_bytes=67043328
        ),
        name="gather_all",
    )(tok.reshape(halves), cot.reshape(halves), w, w_out, common)
    common_all = common_all.reshape((ranks, planes) + common.shape).transpose(1, 0, 2, 3)
    cot_all, out_all = cot_all.reshape(total, d), out_all.reshape(planes * w_out.shape[0], d)
    if fused:
        return (cot_all, out_all, common_all, True) + tuple(rest)
    tok_all, w_all = rest
    return cot_all, out_all, common_all, False, tok_all.reshape(total, d), w_all.reshape(-1, cols)


def plane_sum_kernel(x_in, total, land, send, recv):
    ranks = land.shape[0]
    me, dp = lax.axis_index("seq"), lax.axis_index("dp")
    bits = bits_of(ranks)
    barrier = pltpu.get_barrier_semaphore()
    for mask in range(1, ranks):
        pl.semaphore_signal(barrier, inc=1, device_id=(dp, flip_mask(me, mask, bits)), device_id_type=MESH)
    pl.semaphore_wait(barrier, ranks - 1)

    def copy(mask):
        return remote(x_in, land.at[mask], send.at[mask], recv.at[mask], (dp, flip_mask(me, mask, bits)))

    for mask in range(1, ranks):
        copy(mask).start()
    value = x_in[...]
    for mask in range(1, ranks):
        copy(mask).wait_recv()
        value = value + land[mask]
    total[...] = value
    for mask in range(1, ranks):
        copy(mask).wait_send()


def plane_sum(ranks, x):
    vmem = pl.BlockSpec(memory_space=pltpu.VMEM)
    return pl.pallas_call(
        plane_sum_kernel,
        in_specs=[vmem],
        out_specs=vmem,
        out_shape=jax.ShapeDtypeStruct(x.shape, f32),
        scratch_shapes=[pltpu.VMEM((ranks,) + x.shape, f32)] + [pltpu.SemaphoreType.DMA((ranks,))] * 2,
        compiler_params=pltpu.CompilerParams(collective_id=2, has_side_effects=True),
        name="plane_sum",
    )(x)


def add_into(dst, pieces, rows):
    count = dst.shape[-2]

    def body(i, _):
        at = pl.ds(pl.multiple_of(i * rows, rows), rows)
        total = pieces[0][at, :].astype(f32)
        for piece in pieces[1:]:
            total = total + piece[at, :].astype(f32)
        dst[at, :] = total.astype(dst.dtype)
        return 0

    lax.fori_loop(0, count // rows, body, 0)


def flat_views(ref):
    if len(ref.shape) == 2:
        return [ref]
    return [view for k in range(ref.shape[0]) for view in flat_views(ref.at[k])]


def add_all(dst, pieces, rows):
    for views in zip(flat_views(dst), *(flat_views(p) for p in pieces)):
        add_into(views[0], views[1:], rows)


class Collect:
    def __init__(self, acc, land, send, recv, rows):
        self.size = acc.shape[0]
        self.bits = bits_of(self.size)
        self.orders = both_orders(self.size)
        self.acc, self.land, self.send, self.recv, self.rows = acc, land, send, recv, rows
        self.me, self.dp = lax.axis_index("seq"), lax.axis_index("dp")

    def copy(self, half, mask, bit):
        slot = half * (self.size - 1) + (mask | bit) - 1
        owner = flip_mask(self.me, mask | bit, self.bits)
        return remote(
            self.acc.at[owner, half], self.land.at[slot], self.send.at[slot], self.recv.at[slot],
            (self.dp, flip(self.me, bit)),
        )

    def subsets(self, bits):
        got = [0]
        for bit in bits:
            got = got + [m | bit for m in got]
        return got

    def arrivals(self, half, mask, after):
        pieces = []
        for bit in self.orders[half][after:]:
            slot = half * (self.size - 1) + (mask | bit) - 1
            pltpu.make_async_copy(self.land.at[slot], self.land.at[slot], self.recv.at[slot]).wait()
            pieces.append(self.land.at[slot])
        return pieces

    def push(self, k):
        for half in range(2):
            order = self.orders[half]
            for mask in self.subsets(order[:k]):
                full = mask | order[k]
                pieces = self.arrivals(half, full, k + 1)
                if pieces:
                    ref = self.acc.at[flip_mask(self.me, full, self.bits), half]
                    add_all(ref, [ref] + pieces, self.rows)
                self.copy(half, mask, order[k]).start()

    def total(self, dst):
        for half in range(2):
            pieces = self.arrivals(half, 0, 0)
            add_all(dst.at[half], [self.acc.at[self.me, half]] + pieces, self.rows)

    def finish(self):
        for half in range(2):
            order = self.orders[half]
            for k in range(len(order)):
                for mask in self.subsets(order[:k]):
                    self.copy(half, mask, order[k]).wait_send()


class Fold:
    def __init__(self, at, land, size, send, recv, rows):
        self.at, self.land, self.size, self.send, self.recv, self.rows = at, land, size, send, recv, rows
        self.me, self.seq = lax.axis_index("dp"), lax.axis_index("seq")

    def copy(self, way, block):
        slot = (self.size if way > 0 else 0) + block
        return remote(
            self.at(block), self.land.at[slot], self.send.at[slot], self.recv.at[slot], (self.me + way, self.seq)
        )

    def landed(self, way, block):
        slot = (self.size if way > 0 else 0) + block
        ref = self.land.at[slot]
        pltpu.make_async_copy(ref, ref, self.recv.at[slot]).wait()
        return ref

    def sends(self, way, block):
        return block > self.me if way > 0 else block < self.me

    def push(self, t):
        for way, block in ((1, self.size - 1 - t), (-1, t)):
            @pl.when(self.sends(way, block))
            def _():
                behind = self.me - way

                @pl.when((behind >= 0) & (behind < self.size))
                def _():
                    add_all(self.at(block), [self.at(block), self.landed(way, block)], self.rows)

                self.copy(way, block).start()

    def total(self, dst):
        me = self.me
        add_all(dst, [self.at(me)], self.rows)
        for way in (1, -1):
            behind = me - way

            @pl.when((behind >= 0) & (behind < self.size))
            def _():
                add_all(dst, [dst, self.landed(way, me)], self.rows)

    def finish(self):
        for t in range(self.size):
            for way in (1, -1):
                @pl.when(self.sends(way, t))
                def _():
                    self.copy(way, t).wait_send()


def reduce_kernel(
    out_in, dn_in, w_in, o_in, c_in, s_in,
    out_sum, dn_sum, w_sum, o_sum, c_sum, s_sum,
    out_acc, dn_acc, w_acc, c_acc, s_acc, stage, own,
    out_land, dn_land, w_land, o_land, c_land, s_land, cz_land, sz_land,
    out_s, out_r, dn_s, dn_r, cr_s, cr_r, sr_s, sr_r,
    wz_s, wz_r, oz_s, oz_r, cz_s, cz_r, sz_s, sz_r,
    a2a_s, a2a_r, mix_s, mix_r, local,
):
    ranks, planes = out_in.shape[0], w_in.shape[0]
    me, dp = lax.axis_index("seq"), lax.axis_index("dp")
    bits = bits_of(ranks)
    half = planes // 2
    greet(ranks, planes)
    loads = [
        pltpu.make_async_copy(src, dst, local.at[k])
        for k, (src, dst) in enumerate(
            [(w_in, w_acc), (out_in, out_acc), (c_in, c_acc), (s_in, s_acc), (dn_in, dn_acc)]
        )
    ]
    for load in loads:
        load.start()
    outs = Collect(out_acc, out_land, out_s, out_r, 16)
    dns = Collect(dn_acc, dn_land, dn_s, dn_r, 16)
    cs = Collect(c_acc, c_land, cr_s, cr_r, c_acc.shape[-2])
    ss = Collect(s_acc, s_land, sr_s, sr_r, 8)
    w_fold = Fold(lambda d: w_acc.at[d], w_land, planes, wz_s, wz_r, w_acc.shape[-2])
    o_fold = Fold(lambda d: stage.at[d], o_land, planes, oz_s, oz_r, o_in.shape[1])
    c_fold = Fold(lambda d: own_c(d), cz_land, planes, cz_s, cz_r, c_acc.shape[-2])
    s_fold = Fold(lambda d: own_s(d), sz_land, planes, sz_s, sz_r, 8)

    def own_c(d):
        return c_acc.at[me, lax.div(d, half), d % half]

    def own_s(d):
        return s_acc.at[me, lax.div(d, half), d % half]

    def moved(k):
        index = me * planes + k
        return lax.div(index, ranks), index % ranks

    loads[0].wait()
    w_fold.push(0)
    for load in loads[1:]:
        load.wait()
    top = len(bits) - 1
    outs.push(top)
    dns.push(top)
    cs.push(top)
    ss.push(top)
    for k in range(planes):
        to_plane, to = moved(k)

        @pl.when(to == me)
        def _():
            pltpu.make_async_copy(o_in.at[k], stage.at[to_plane], mix_r.at[to_plane]).start()

        @pl.when(to != me)
        def _():
            remote(o_in.at[k], stage.at[to_plane], mix_s.at[k], mix_r.at[to_plane], (dp, to)).start()

    for k in reversed(range(top)):
        cs.push(k)
        ss.push(k)
    for k in reversed(range(1, top)):
        dns.push(k)
    c_rows = [c_acc.at[me, k] for k in range(2)]
    for h in range(2):
        for ring in (cs, ss):
            pieces = ring.arrivals(h, 0, 0)
            ref = ring.acc.at[me, h]
            add_all(ref, [ref] + pieces, ring.rows)
    for t in range(planes - 1):
        c_fold.push(t)
        s_fold.push(t)
    dns.push(0)
    for k in reversed(range(1, top)):
        outs.push(k)
    w_fold.push(1)
    for d in range(planes):
        pltpu.make_async_copy(stage.at[d], stage.at[d], mix_r.at[d]).wait()
    o_fold.push(0)
    for t in range(2, planes - 1):
        w_fold.push(t)
    outs.push(0)
    for t in range(1, planes - 1):
        o_fold.push(t)
    w_fold.total(own)

    def exchange(mask):
        peer = flip_mask(me, mask, bits)
        return remote(own.at[peer], w_sum.at[me], a2a_s.at[mask], a2a_r.at[mask], (dp, peer))

    for mask in range(1, ranks):
        exchange(mask).start()
    keep = pltpu.make_async_copy(own.at[me], w_sum.at[me], local.at[0])
    keep.start()
    dns.total(dn_sum)
    c_fold.total(c_sum)
    s_fold.total(s_sum)
    outs.total(out_sum)
    o_fold.total(o_sum)
    keep.wait()
    for mask in range(1, ranks):
        ref = w_sum.at[flip_mask(me, mask, bits)]
        pltpu.make_async_copy(ref, ref, a2a_r.at[mask]).wait()
    for mask in range(1, ranks):
        exchange(mask).wait_send()
    for k in range(planes):
        to_plane, to = moved(k)

        @pl.when(to != me)
        def _():
            remote(o_in.at[k], stage.at[to_plane], mix_s.at[k], mix_r.at[to_plane], (dp, to)).wait_send()

    for ring in (outs, dns, cs, ss, w_fold, o_fold, c_fold, s_fold):
        ring.finish()


def reduce_all(ranks, planes, out_part, dn_part, w, w_out, common, small):
    length, d = out_part.shape[0] // ranks, out_part.shape[1]
    part = (2, length // 2, d)
    rows, cols = w.shape[2:]
    dma = pltpu.SemaphoreType.DMA
    vmem = pl.BlockSpec(memory_space=pltpu.VMEM)
    cpart, spart = common.shape[1:], small.shape[1:]
    ring, line = 2 * (ranks - 1), 2 * planes
    results = pl.pallas_call(
        reduce_kernel,
        in_specs=[pl.BlockSpec(memory_space=pl.ANY)] * 6,
        out_specs=[vmem] * 6,
        out_shape=[
            jax.ShapeDtypeStruct(part, f32),
            jax.ShapeDtypeStruct(part, f32),
            jax.ShapeDtypeStruct((ranks, rows, cols), bf16),
            jax.ShapeDtypeStruct(w_out.shape[1:], f32),
            jax.ShapeDtypeStruct(cpart[2:], f32),
            jax.ShapeDtypeStruct(spart[2:], f32),
        ],
        scratch_shapes=[
            pltpu.VMEM((ranks,) + part, bf16),
            pltpu.VMEM((ranks,) + part, bf16),
            pltpu.VMEM(w.shape, bf16),
            pltpu.VMEM(common.shape, bf16),
            pltpu.VMEM(small.shape, f32),
            pltpu.VMEM(w_out.shape, bf16),
            pltpu.VMEM(w.shape[1:], bf16),
            pltpu.VMEM((ring,) + part[1:], bf16),
            pltpu.VMEM((ring,) + part[1:], bf16),
            pltpu.VMEM((line,) + w.shape[1:], bf16),
            pltpu.VMEM((line,) + w_out.shape[1:], bf16),
            pltpu.VMEM((ring,) + cpart[1:], bf16),
            pltpu.VMEM((ring,) + spart[1:], f32),
            pltpu.VMEM((line,) + cpart[2:], bf16),
            pltpu.VMEM((line,) + spart[2:], f32),
        ]
        + [dma((ring,))] * 8
        + [dma((line,))] * 8
        + [dma((ranks,)), dma((ranks,)), dma((planes,)), dma((planes,)), dma((5,))],
        compiler_params=pltpu.CompilerParams(
            collective_id=1, has_side_effects=True, vmem_limit_bytes=67043328
        ),
        name="reduce_all",
    )(out_part.reshape((ranks,) + part), dn_part.reshape((ranks,) + part), w, w_out, common, small)
    out_sum, dn_sum, w_sum, o_sum, c_sum, s_sum = results
    return out_sum.reshape(length, d), dn_sum.reshape(length, d), w_sum, o_sum, c_sum, s_sum


def rms_scale(values, gain):
    mean_sq = jnp.mean(values * values, axis=-1, keepdims=True)
    return values * lax.rsqrt(mean_sq + epsilon) * gain


def widen(array, size, axis):
    pads = [(0, 0)] * array.ndim
    pads[axis] = (0, size - array.shape[axis])
    return jnp.pad(array, pads)


def per_device(
    tokens,
    cotangent,
    in_weight,
    out_weight,
    conv_weight,
    conv_bias,
    norm_gain,
    gate_gain,
    decay_rate,
    dt_bias,
    d_skip,
):
    ranks = lax.axis_size("seq")
    me = lax.axis_index("seq")
    both = ("dp", "seq")
    heads = decay_rate.shape[0] // ranks
    din = heads * HDIM
    padded = -(-din // LANES) * LANES
    din_all = din * ranks
    rows, width = in_weight.shape
    conv_all = din_all + 2 * NSTATE
    main = 2 * padded + 2 * NSTATE

    def mine(array, size, axis=0):
        return lax.dynamic_slice_in_dim(array, me * size, size, axis)

    planes = lax.axis_size("dp")
    x_own = tokens[0].astype(f32)
    send = jnp.concatenate(
        [
            widen(in_weight[:, :din_all].reshape(rows, ranks, din), padded, 2),
            widen(in_weight[:, din_all : 2 * din_all].reshape(rows, ranks, din), padded, 2),
        ],
        axis=2,
    ).transpose(1, 0, 2)
    d = in_weight.shape[0] * ranks * planes
    rank_id = lax.axis_index("dp") * ranks + me
    small = [norm_gain, gate_gain, conv_weight.reshape(-1), conv_bias]
    sizes = [a.shape[0] for a in small]
    room = rows * HDIM - d
    if room >= sum(sizes):
        placed = lax.dynamic_update_slice_in_dim(jnp.zeros((d,), bf16), norm_gain, rank_id * rows, 0)
        packed = jnp.concatenate([placed, widen(jnp.concatenate(small), room, 0)])
    else:
        packed = widen(jnp.concatenate(small), rows * HDIM, 0)
    common = jnp.concatenate(
        [
            in_weight[:, 2 * din_all : 2 * din_all + 2 * NSTATE],
            widen(in_weight[:, din_all + conv_all :], HDIM, 1),
            packed.reshape(rows, HDIM),
        ],
        axis=1,
    )
    cot, w_out, common, fused, *rest = gather_all(
        ranks, planes, tokens[0], cotangent[0], send, out_weight, common
    )
    w_out = widen(w_out, padded, 0)
    packed = common[..., 2 * NSTATE + HDIM :].reshape(ranks * planes, rows * HDIM).astype(f32)
    if room >= sum(sizes):
        packed = packed[:, d:]
    gain_norm, gain_gate, conv_w, conv_b = (
        packed[:, sum(sizes[:k]) : sum(sizes[: k + 1])].reshape(-1) for k in range(4)
    )
    conv_w = conv_w.reshape(-1, CONVK)
    taps = jnp.concatenate([conv_w.T, conv_b[None], jnp.zeros((8 - CONVK - 1, conv_all), f32)], axis=0)
    conv = jnp.concatenate([widen(mine(taps, din, 1), padded, 1), taps[:, din_all:]], axis=1)
    if fused:
        normed, proj, raw, w_full = rest
    else:
        tok, w_all = rest
        w_full = jnp.concatenate([w_all, common.reshape(-1, common.shape[-1])], axis=1)
        normed = rms_scale(tok.astype(f32), gain_norm).astype(bf16)
        proj = dot(normed, w_full[:, :main], NN).astype(bf16)
        raw = dot(w_full[:, main : main + HDIM].T, normed, NT).astype(bf16).astype(f32)
    raw = widen(mine(raw, heads), 8, 0)
    rate, bias, skip = (mine(a, heads) for a in (decay_rate, dt_bias, d_skip))
    lanes = jnp.stack([jnp.repeat(skip, HDIM), mine(gain_gate, din)])
    lanes = widen(widen(lanes, padded, 1), 8, 0)
    head_rows = jnp.broadcast_to(widen(jnp.stack([rate, bias]), 8, 1)[:, :, None], (2, 8, SUB))

    y, dg, out_part, states, sums = mixer_forward(proj, raw, cot, w_out, conv, lanes, head_rows)
    sums = plane_sum(ranks, sums[::4].reshape(8, -1)).reshape(2, -1)
    sums = jnp.repeat(sums, 4, axis=0)
    d_proj, d_raw, d_w_out, d_conv, d_lane, d_head = mixer_backward(
        din_all, proj, raw, y, dg, sums, states, cot, conv, lanes, head_rows
    )
    d_steps = lax.dynamic_update_slice_in_dim(
        jnp.zeros((proj.shape[0], w_full.shape[1] - main), bf16), d_raw[:heads].T.astype(bf16), me * heads, 1
    )
    d_proj = jnp.concatenate([d_proj, d_steps], axis=1)
    w_live = jnp.where(jnp.arange(w_full.shape[1]) < main + HDIM, w_full, 0)
    d_normed_part = dot(d_proj, w_live, NT)
    d_g1 = jnp.sum(d_normed_part * normed.astype(f32), axis=0) / gain_norm
    d_w = dot(normed, d_proj, TN).astype(bf16)
    d_w_main = d_w[:, : 2 * padded].reshape(planes, ranks, rows, -1)

    def by_owner(array):
        split = array.reshape((2, planes // 2, ranks) + array.shape[1:])
        return split.transpose((2, 0, 1) + tuple(range(3, split.ndim)))

    def place(own, size):
        return lax.dynamic_update_slice_in_dim(
            jnp.zeros((size * ranks,) + own.shape[1:], f32), own, me * size, 0
        )

    d_bc = d_w[:, 2 * padded :].reshape(planes * ranks, rows, -1)
    d_cw, d_cb = d_conv[:CONVK].T, d_conv[CONVK]
    full_cw = jnp.concatenate([place(d_cw[:din], din), d_cw[padded:]], axis=0)
    full_cb = jnp.concatenate([place(d_cb[:din], din), d_cb[padded:]], axis=0)
    d_skp = jnp.sum(d_lane[0, :din].reshape(heads, HDIM), axis=1)
    d_rate, d_bias = jnp.sum(d_head, axis=2)[:, :heads]
    devices = planes * ranks
    head_part = jnp.concatenate([place(a, heads) for a in (d_rate, d_bias, d_skp)])
    fields = [
        a.reshape(devices, -1) for a in (full_cw, full_cb, d_g1, place(d_lane[1, :din], din))
    ] + [jnp.broadcast_to(head_part, (devices,) + head_part.shape)]
    ends = [0]
    for a in fields:
        ends.append(ends[-1] + a.shape[1])
    small = widen(jnp.concatenate(fields, axis=1), 8 * LANES, 1).reshape(devices, 8, LANES)
    out_sum, d_normed, w_sum, grad_out, bc_sum, small_sum = reduce_all(
        ranks, planes, out_part, d_normed_part.astype(bf16), d_w_main,
        d_w_out[:din].astype(bf16).reshape(planes, -1, d_w_out.shape[1]), by_owner(d_bc), by_owner(small),
    )
    own = mine(sums[0], x_own.shape[0])[:, None]
    block_out = (x_own + lax.rsqrt(own / din_all + epsilon) * out_sum).astype(bf16)
    gain = gain_norm * d_normed
    inv = lax.rsqrt(jnp.mean(x_own * x_own, axis=1, keepdims=True) + epsilon)
    d_xn = inv * (gain - x_own * (inv * inv * jnp.mean(gain * x_own, axis=1, keepdims=True)))
    grad_x = cotangent[0].astype(f32) + d_xn
    spread = w_sum.astype(f32).transpose(1, 0, 2)
    grad_in = jnp.concatenate(
        [
            spread[:, :, :din].reshape(rows, din_all),
            spread[:, :, padded : padded + din].reshape(rows, din_all),
            bc_sum[:, : 2 * NSTATE + heads * ranks],
        ],
        axis=1,
    )
    small_sum = small_sum.reshape(-1)
    g_cw, g_cb, g_gain, g_gate, head_sums = (small_sum[a:b] for a, b in zip(ends[:-1], ends[1:]))
    g_cw = g_cw.reshape(-1, CONVK)
    head_sums = head_sums.reshape(3, -1)
    return (
        block_out[None],
        grad_x[None],
        grad_in,
        grad_out,
        g_cw,
        g_cb,
        g_gain,
        g_gate,
        head_sums[0],
        head_sums[1],
        head_sums[2],
    )


def solution(mesh):
    rows = P(("dp", "seq"), None)
    flat = P(("dp", "seq"))
    act = P("dp", "seq", None)
    return jax.shard_map(
        per_device,
        mesh=mesh,
        in_specs=(act, act, rows, rows, rows, flat, flat, flat, P(), P(), P()),
        out_specs=(act, act, rows, rows, rows, flat, flat, flat, P(), P(), P()),
        check_vma=False,
    )
```

```python
from functools import partial

import jax
import jax.numpy as jnp
from jax import lax
from jax.experimental import pallas as pl
from jax.experimental.pallas import tpu as pltpu
from jax.sharding import PartitionSpec as P

HDIM = 64
NSTATE = 128
CONVK = 4
LANES = 128
SUB = 128
TOKENS = 256
EDGE = 8

epsilon = 1e-05
highest = lax.Precision.HIGHEST
bf16 = jnp.bfloat16
f32 = jnp.float32


MESH = pl.DeviceIdType.MESH


def flip(index, bit):
    return index + bit * (1 - 2 * (lax.div(index, bit) % 2))


def flip_mask(index, mask, bits):
    for bit in bits:
        if mask & bit:
            index = flip(index, bit)
    return index


def bits_of(size):
    return [1 << k for k in range(size.bit_length() - 1)]


def both_orders(size):
    bits = bits_of(size)
    slow = bits[1:]
    return [slow + bits[:1], slow[::-1] + bits[:1]]


def remote(src, dst, send, recv, to):
    return pltpu.make_async_remote_copy(
        src_ref=src, dst_ref=dst, send_sem=send, recv_sem=recv, device_id=to, device_id_type=MESH
    )


class Spread:
    def __init__(self, buf, send, recv, own=None):
        self.size = buf.shape[0]
        self.bits = bits_of(self.size)
        self.orders = both_orders(self.size)
        self.buf, self.send, self.recv = buf, send, recv
        self.me, self.dp = lax.axis_index("seq"), lax.axis_index("dp")
        self.own = own

    def masks(self, half):
        order = self.orders[half]
        got = [0]
        for bit in order:
            got = got + [m | bit for m in got]
        return got

    def copy(self, half, mask, bit):
        origin = flip_mask(self.me, mask, self.bits)
        dst = self.buf.at[origin, half]
        src = self.own.at[half] if (mask == 0 and self.own is not None) else dst
        slot = half * self.size + (mask | bit)
        return remote(src, dst, self.send.at[slot], self.recv.at[slot], (self.dp, flip(self.me, bit)))

    def start(self, half, mask):
        order = self.orders[half]
        after = max((order.index(b) for b in self.bits if mask & b), default=-1) + 1
        for bit in order[after:]:
            self.copy(half, mask, bit).start()

    def arrive(self, half, mask):
        order = self.orders[half]
        top = order[max(order.index(b) for b in self.bits if mask & b)]
        self.copy(half, mask & ~top, top).wait_recv()

    def forward(self, group):
        for k in range(1 << group, 2 << group):
            for half in range(2):
                mask = self.masks(half)[k]
                self.arrive(half, mask)
                self.start(half, mask)

    def finish(self):
        for half in range(2):
            for mask in range(1, self.size):
                order = self.orders[half]
                top = order[max(order.index(b) for b in self.bits if mask & b)]
                self.copy(half, mask & ~top, top).wait_send()

    @property
    def groups(self):
        return len(self.bits)


class Line:
    def __init__(self, at, size, send, recv):
        self.at, self.size, self.send, self.recv = at, size, send, recv
        self.me, self.seq = lax.axis_index("dp"), lax.axis_index("seq")

    def copy(self, way, hop):
        block = self.me - way * (hop - 1)
        slot = (self.size if way > 0 else 0) + hop
        ref = self.at(block)
        return remote(ref, ref, self.send.at[slot], self.recv.at[slot], (self.me + way, self.seq))

    def sends(self, way, hop):
        block = self.me - way * (hop - 1)
        to = self.me + way
        return (block >= 0) & (block < self.size) & (to >= 0) & (to < self.size)

    def start(self, hop):
        for way in (1, -1):
            @pl.when(self.sends(way, hop))
            def _():
                self.copy(way, hop).start()

    def arrive(self, hop):
        for way in (1, -1):
            source = self.me - way * hop
            @pl.when((source >= 0) & (source < self.size))
            def _():
                ref = self.at(source)
                slot = (self.size if way > 0 else 0) + hop
                pltpu.make_async_copy(ref, ref, self.recv.at[slot]).wait()

    def forward(self, hop):
        self.arrive(hop)
        if hop + 1 < self.size:
            self.start(hop + 1)

    def finish(self):
        for hop in range(1, self.size):
            for way in (1, -1):
                @pl.when(self.sends(way, hop))
                def _():
                    self.copy(way, hop).wait_send()


def greet(ranks, planes):
    me, dp = lax.axis_index("seq"), lax.axis_index("dp")
    barrier = pltpu.get_barrier_semaphore()
    for mask in range(1, ranks):
        pl.semaphore_signal(
            barrier, inc=1, device_id=(dp, flip_mask(me, mask, bits_of(ranks))), device_id_type=MESH
        )
    for way in (1, -1):
        @pl.when((dp + way >= 0) & (dp + way < planes))
        def _():
            pl.semaphore_signal(barrier, inc=1, device_id=(dp + way, me), device_id_type=MESH)
    near = jnp.where(dp > 0, 1, 0) + jnp.where(dp < planes - 1, 1, 0)
    pl.semaphore_wait(barrier, ranks - 1 + near)


def norm_tokens(tok, common, normed, rows, w_full):
    ranks, planes = tok.shape[0], 2 * common.shape[2]
    width = w_full.shape[1] - common.shape[-1]
    strip, tile = 32, tok.shape[2]
    d = tok.shape[3]
    half = planes // 2

    def lay(i, gains):
        at = pl.ds(pl.multiple_of(i * rows, 16), rows)
        plane, rank = lax.div(i, ranks), i % ranks
        shared = common[rank, lax.div(plane, half), plane % half]
        w_full[at, width:] = shared
        return gains + shared[: d // HDIM, 2 * NSTATE :].astype(f32)

    gains = lax.fori_loop(0, planes * ranks, lay, jnp.zeros((d // HDIM, LANES), f32))
    moved = pltpu.roll(gains, HDIM, 1)
    low = iota((1, LANES), 1) < HDIM
    gain = [jnp.where(low, moved[2 * j : 2 * j + 1], gains[2 * j + 1 : 2 * j + 2]) for j in range(d // LANES)]

    def norm(i, _):
        per = tile // strip
        part = lax.div(i, per)
        at = pl.ds(pl.multiple_of((i % per) * strip, strip), strip)
        x = tok.at[lax.div(part, 2), part % 2][at, :].astype(f32)
        scale = lax.rsqrt(jnp.sum(x * x, axis=1, keepdims=True) * (1.0 / d) + epsilon)
        to = pl.ds(pl.multiple_of(i * strip, strip), strip)
        for j in range(d // LANES):
            cut = slice(j * LANES, (j + 1) * LANES)
            normed[to, cut] = (x[:, cut] * scale * gain[j]).astype(bf16)
        return 0

    lax.fori_loop(0, ranks * 2 * tile // strip, norm, 0)


def stored(i, flipped, proj, flip_out, proj_out, store):
    at = pl.ds(pl.multiple_of(i * 256, 256), 256)
    return (
        pltpu.make_async_copy(proj.at[at, :], proj_out.at[at, :], store.at[0, i]),
        pltpu.make_async_copy(flipped.at[:, at], flip_out.at[:, at], store.at[1, i]),
    )


def project(w, normed, flipped, proj, raw, w_full, flip_out, proj_out, store):
    planes, ranks, rows, width = w.shape
    total, d = normed.shape
    main = width + 2 * NSTATE

    def lay(i, _):
        at = pl.ds(pl.multiple_of(i * rows, 16), rows)
        w_full[at, :width] = w[lax.div(i, ranks), i % ranks]
        return 0

    lax.fori_loop(0, planes * ranks, lay, 0)

    def multiply(i, _):
        at = pl.ds(pl.multiple_of(i * 256, 256), 256)
        for start in range(0, main, 512):
            cut = slice(start, min(start + 512, main))
            proj[at, cut] = dot(normed[at, :], w_full[:, cut], NN).astype(bf16)
        for k in range(2):
            to = pl.ds(pl.multiple_of(i * 256 + k * LANES, LANES), LANES)
            for j in range(d // LANES):
                tokens = normed[to, j * LANES : (j + 1) * LANES].astype(f32)
                flipped[j * LANES : (j + 1) * LANES, to] = tokens.T.astype(bf16)
        steps = dot(normed[at, :], w_full[:, main:], NN).astype(bf16).astype(f32)
        for k in range(2):
            to = pl.ds(pl.multiple_of(i * 256 + k * LANES, LANES), LANES)
            raw[:, to] = steps[k * LANES : (k + 1) * LANES].T[: raw.shape[0]]
        for copy in stored(i, flipped, proj, flip_out, proj_out, store):
            copy.start()
        return 0

    lax.fori_loop(0, total // 256, multiply, 0)


def gather_kernel(
    fused, tok_in, cot_in, w_in, wout_in, common_in,
    cot, wout, common, *rest,
):
    if fused:
        raw, flip_out, proj_out, full_out, tok, w, normed, flipped, proj, w_full, store, *rest = rest
    else:
        tok, w, *rest = rest
    (stage, tok_s, tok_r, cot_s, cot_r, com_s, com_r, wz_s, wz_r, oz_s, oz_r, cz_s, cz_r,
    a2a_s, a2a_r, mix_s, mix_r, local) = rest
    ranks, planes = tok.shape[0], w.shape[0]
    me, dp = lax.axis_index("seq"), lax.axis_index("dp")
    bits = bits_of(ranks)
    greet(ranks, planes)
    half = planes // 2
    tokens = Spread(tok, tok_s, tok_r, tok_in)
    cots = Spread(cot, cot_s, cot_r, cot_in)
    commons = Spread(common, com_s, com_r)
    w_line = Line(lambda d: w.at[d], planes, wz_s, wz_r)
    o_line = Line(lambda d: stage.at[d], planes, oz_s, oz_r)
    c_line = Line(lambda d: common.at[me, lax.div(d, half), d % half], planes, cz_s, cz_r)

    def exchange(mask):
        peer = flip_mask(me, mask, bits)
        return remote(w_in.at[peer], w.at[dp, me], a2a_s.at[mask], a2a_r.at[mask], (dp, peer))

    def arrived(mask):
        ref = w.at[dp, flip_mask(me, mask, bits)]
        return pltpu.make_async_copy(ref, ref, a2a_r.at[mask])

    for mask in range(1, ranks):
        exchange(mask).start()
    places = [
        pltpu.make_async_copy(w_in.at[me], w.at[dp, me], local.at[0]),
        pltpu.make_async_copy(common_in, common.at[me, lax.div(dp, half), dp % half], local.at[1]),
        pltpu.make_async_copy(wout_in, stage.at[dp], local.at[2]),
        pltpu.make_async_copy(tok_in, tok.at[me], local.at[3]),
        pltpu.make_async_copy(cot_in, cot.at[me], local.at[4]),
    ]
    for place in places:
        place.start()
    for h in range(2):
        tokens.start(h, 0)
    for place in places:
        place.wait()
    c_line.start(1)
    for hop in range(1, planes):
        c_line.forward(hop)
    for mask in range(1, ranks):
        arrived(mask).wait()
    w_line.start(1)
    o_line.start(1)
    tokens.forward(0)
    for h in range(2):
        commons.start(h, 0)
    for h in range(2):
        cots.start(h, 0)
    w_line.forward(1)
    o_line.forward(1)
    for group in range(1, tokens.groups - 1):
        tokens.forward(group)
    for group in range(commons.groups - 1):
        commons.forward(group)
    for hop in range(2, planes - 1):
        w_line.forward(hop)
    tokens.forward(tokens.groups - 1)
    commons.forward(commons.groups - 1)
    if fused:
        norm_tokens(tok, common, normed, w.shape[2], w_full)
    cots.forward(0)
    for hop in range(2, planes - 1):
        o_line.forward(hop)
    w_line.forward(planes - 1)
    o_line.forward(planes - 1)

    def moved(d):
        index = d * ranks + me
        return lax.div(index, planes), index % planes

    for d in range(planes):
        to, place = moved(d)

        @pl.when(to == me)
        def _():
            pltpu.make_async_copy(stage.at[d], wout.at[place], mix_r.at[place]).start()

        @pl.when(to != me)
        def _():
            remote(stage.at[d], wout.at[place], mix_s.at[d], mix_r.at[place], (dp, to)).start()

    if fused:
        project(w, normed, flipped, proj, raw, w_full, flip_out, proj_out, store)
        full = pltpu.make_async_copy(w_full, full_out, local.at[0])
        full.start()
    for group in range(1, cots.groups):
        cots.forward(group)
    for place in range(planes):
        pltpu.make_async_copy(wout.at[place], wout.at[place], mix_r.at[place]).wait()
    for d in range(planes):
        to, place = moved(d)

        @pl.when(to != me)
        def _():
            remote(stage.at[d], wout.at[place], mix_s.at[d], mix_r.at[place], (dp, to)).wait_send()

    for mask in range(1, ranks):
        exchange(mask).wait_send()
    for ring in (tokens, cots, commons, w_line, o_line, c_line):
        ring.finish()
    if fused:
        full.wait()
        for i in range(store.shape[1]):
            for copy in stored(i, flipped, proj, flip_out, proj_out, store):
                copy.wait()


def gather_all(ranks, planes, tok, cot, w, w_out, common):
    length, d = tok.shape
    halves = (2, length // 2, d)
    total = ranks * length
    rows, cols = w.shape[1:]
    fused = rows % 16 == 0 and rows * HDIM >= 2 * d and length % 256 == 0 and cols % 384 == 0
    dma = pltpu.SemaphoreType.DMA
    vmem = pl.BlockSpec(memory_space=pltpu.VMEM)
    ring, line = 2 * ranks, 2 * planes
    anywhere = pl.BlockSpec(memory_space=pl.ANY)
    buffers = [((ranks,) + halves, bf16), ((planes,) + w.shape, bf16)]
    out = [
        ((ranks,) + halves, bf16), ((planes,) + w_out.shape, bf16), ((ranks, 2, planes // 2) + common.shape, bf16)
    ]
    places = [vmem, vmem, vmem]
    stores = []
    if fused:
        own = [((d, total), bf16), ((total, cols + 2 * NSTATE), bf16), ((d, cols + common.shape[1]), bf16)]
        out += [((HDIM, total), f32)] + own
        places += [vmem, anywhere, anywhere, anywhere]
        stores = [pltpu.VMEM(*s) for s in buffers + [((total, d), bf16)] + own] + [dma((2, total // 256))]
    else:
        out += buffers
        places += [vmem, vmem]
    cot_all, out_all, common_all, *rest = pl.pallas_call(
        partial(gather_kernel, fused),
        in_specs=[anywhere] * 5,
        out_specs=places,
        out_shape=[jax.ShapeDtypeStruct(*s) for s in out],
        scratch_shapes=stores
        + [pltpu.VMEM((planes,) + w_out.shape, bf16)]
        + [dma((ring,))] * 6
        + [dma((line,))] * 6
        + [dma((ranks,)), dma((ranks,)), dma((planes,)), dma((planes,)), dma((5,))],
        compiler_params=pltpu.CompilerParams(
            collective_id=0, has_side_effects=True, vmem_limit_bytes=67043328
        ),
        name="gather_all",
    )(tok.reshape(halves), cot.reshape(halves), w, w_out, common)
    common_all = common_all.reshape((ranks, planes) + common.shape).transpose(1, 0, 2, 3)
    cot_all, out_all = cot_all.reshape(total, d), out_all.reshape(planes * w_out.shape[0], d)
    if fused:
        return (cot_all, out_all, common_all, True) + tuple(rest)
    tok_all, w_all = rest
    return cot_all, out_all, common_all, False, tok_all.reshape(total, d), w_all.reshape(-1, cols)


def plane_sum_kernel(x_in, total, land, send, recv):
    ranks = land.shape[0]
    me, dp = lax.axis_index("seq"), lax.axis_index("dp")
    bits = bits_of(ranks)
    barrier = pltpu.get_barrier_semaphore()
    for mask in range(1, ranks):
        pl.semaphore_signal(barrier, inc=1, device_id=(dp, flip_mask(me, mask, bits)), device_id_type=MESH)
    pl.semaphore_wait(barrier, ranks - 1)

    def copy(mask):
        return remote(x_in, land.at[mask], send.at[mask], recv.at[mask], (dp, flip_mask(me, mask, bits)))

    for mask in range(1, ranks):
        copy(mask).start()
    value = x_in[...]
    for mask in range(1, ranks):
        copy(mask).wait_recv()
        value = value + land[mask]
    total[...] = value
    for mask in range(1, ranks):
        copy(mask).wait_send()


def plane_sum(ranks, x):
    vmem = pl.BlockSpec(memory_space=pltpu.VMEM)
    return pl.pallas_call(
        plane_sum_kernel,
        in_specs=[vmem],
        out_specs=vmem,
        out_shape=jax.ShapeDtypeStruct(x.shape, f32),
        scratch_shapes=[pltpu.VMEM((ranks,) + x.shape, f32)] + [pltpu.SemaphoreType.DMA((ranks,))] * 2,
        compiler_params=pltpu.CompilerParams(collective_id=2, has_side_effects=True),
        name="plane_sum",
    )(x)


def add_into(dst, pieces, rows):
    count = dst.shape[-2]
    rows = 16 if count % 16 == 0 else count

    def body(i, _):
        at = pl.ds(pl.multiple_of(i * rows, rows), rows)
        total = pieces[0][at, :].astype(f32)
        for piece in pieces[1:]:
            total = total + piece[at, :].astype(f32)
        dst[at, :] = total.astype(dst.dtype)
        return 0

    lax.fori_loop(0, count // rows, body, 0)


def flat_views(ref):
    if len(ref.shape) == 2:
        return [ref]
    return [view for k in range(ref.shape[0]) for view in flat_views(ref.at[k])]


def add_all(dst, pieces, rows):
    for views in zip(flat_views(dst), *(flat_views(p) for p in pieces)):
        add_into(views[0], views[1:], rows)


class Collect:
    def __init__(self, acc, land, send, recv, rows):
        self.size = acc.shape[0]
        self.bits = bits_of(self.size)
        self.orders = both_orders(self.size)
        self.acc, self.land, self.send, self.recv, self.rows = acc, land, send, recv, rows
        self.me, self.dp = lax.axis_index("seq"), lax.axis_index("dp")

    def copy(self, half, mask, bit):
        slot = half * (self.size - 1) + (mask | bit) - 1
        owner = flip_mask(self.me, mask | bit, self.bits)
        return remote(
            self.acc.at[owner, half], self.land.at[slot], self.send.at[slot], self.recv.at[slot],
            (self.dp, flip(self.me, bit)),
        )

    def subsets(self, bits):
        got = [0]
        for bit in bits:
            got = got + [m | bit for m in got]
        return got

    def arrivals(self, half, mask, after):
        pieces = []
        for bit in self.orders[half][after:]:
            slot = half * (self.size - 1) + (mask | bit) - 1
            pltpu.make_async_copy(self.land.at[slot], self.land.at[slot], self.recv.at[slot]).wait()
            pieces.append(self.land.at[slot])
        return pieces

    def push(self, k):
        for half in range(2):
            order = self.orders[half]
            for mask in self.subsets(order[:k]):
                full = mask | order[k]
                pieces = self.arrivals(half, full, k + 1)
                if pieces:
                    ref = self.acc.at[flip_mask(self.me, full, self.bits), half]
                    add_all(ref, [ref] + pieces, self.rows)
                self.copy(half, mask, order[k]).start()

    def total(self, dst):
        for half in range(2):
            pieces = self.arrivals(half, 0, 0)
            add_all(dst.at[half], [self.acc.at[self.me, half]] + pieces, self.rows)

    def finish(self):
        for half in range(2):
            order = self.orders[half]
            for k in range(len(order)):
                for mask in self.subsets(order[:k]):
                    self.copy(half, mask, order[k]).wait_send()


class Fold:
    def __init__(self, at, land, size, send, recv, rows):
        self.at, self.land, self.size, self.send, self.recv, self.rows = at, land, size, send, recv, rows
        self.me, self.seq = lax.axis_index("dp"), lax.axis_index("seq")

    def copy(self, way, block):
        slot = (self.size if way > 0 else 0) + block
        return remote(
            self.at(block), self.land.at[slot], self.send.at[slot], self.recv.at[slot], (self.me + way, self.seq)
        )

    def landed(self, way, block):
        slot = (self.size if way > 0 else 0) + block
        ref = self.land.at[slot]
        pltpu.make_async_copy(ref, ref, self.recv.at[slot]).wait()
        return ref

    def sends(self, way, block):
        return block > self.me if way > 0 else block < self.me

    def push(self, t):
        last = self.size - 1
        for way, block in ((1, last + self.me - t), (-1, t - last + self.me)):
            @pl.when((block >= 0) & (block <= last))
            def _():
                behind = self.me - way

                @pl.when((behind >= 0) & (behind < self.size))
                def _():
                    add_all(self.at(block), [self.at(block), self.landed(way, block)], self.rows)

                self.copy(way, block).start()

    def total(self, dst):
        me = self.me
        add_all(dst, [self.at(me)], self.rows)
        for way in (1, -1):
            behind = me - way

            @pl.when((behind >= 0) & (behind < self.size))
            def _():
                add_all(dst, [dst, self.landed(way, me)], self.rows)

    def finish(self):
        for t in range(self.size):
            for way in (1, -1):
                @pl.when(self.sends(way, t))
                def _():
                    self.copy(way, t).wait_send()


def reduce_kernel(fused, s_in, *refs):
    if fused:
        flip_in, dproj_in, wfull_in, *refs = refs
    else:
        dn_in, w_in, c_in, *refs = refs
    (dn_sum, w_sum, c_sum, s_sum, dn_acc, w_acc, c_acc, s_acc, own,
     dn_land, w_land, c_land, s_land, cz_land, sz_land,
     dn_s, dn_r, cr_s, cr_r, sr_s, sr_r, wz_s, wz_r, cz_s, cz_r, sz_s, sz_r, a2a_s, a2a_r, local, *refs) = refs
    ranks, planes = dn_acc.shape[0], w_acc.shape[0]
    me, dp = lax.axis_index("seq"), lax.axis_index("dp")
    bits = bits_of(ranks)
    half = planes // 2
    top = len(bits) - 1
    rows, cols = w_acc.shape[2:]
    tokens = dn_acc.shape[2]
    if fused:
        flipped, dproj, w_full = refs
        pairs = [(flip_in, flipped), (dproj_in, dproj), (s_in, s_acc), (wfull_in, w_full)]
    else:
        pairs = [(w_in, w_acc), (c_in, c_acc), (s_in, s_acc), (dn_in, dn_acc)]
    loads = [pltpu.make_async_copy(src, dst, local.at[k]) for k, (src, dst) in enumerate(pairs)]
    for load in loads:
        load.start()
    greet(ranks, planes)
    dns = Collect(dn_acc, dn_land, dn_s, dn_r, 16)
    cs = Collect(c_acc, c_land, cr_s, cr_r, c_acc.shape[-2])
    ss = Collect(s_acc, s_land, sr_s, sr_r, 8)

    def own_c(d):
        return c_acc.at[me, lax.div(d, half), d % half]

    def own_s(d):
        return s_acc.at[me, lax.div(d, half), d % half]

    w_fold = Fold(lambda d: w_acc.at[d], w_land, planes, wz_s, wz_r, rows)
    c_fold = Fold(own_c, cz_land, planes, cz_s, cz_r, c_acc.shape[-2])
    s_fold = Fold(own_s, sz_land, planes, sz_s, sz_r, 8)

    def weight_rows(plane):
        left = pl.ds(plane * ranks * rows, ranks * rows)
        for start in range(0, dproj.shape[1], 384):
            cut = slice(start, start + 384)
            block = dot(flipped[left, :], dproj[:, cut], NN).astype(bf16)
            for rank in range(ranks):
                piece = block[rank * rows : (rank + 1) * rows]
                if start < cols:
                    w_acc[plane, rank, :, cut] = piece
                else:
                    c_acc[rank, plane // half, plane % half, :, start - cols : start - cols + 384] = piece

    def token_half(far):
        mine = me % 2

        def body(i, _):
            rank = 2 * i + (1 - mine if far else mine)
            at = pl.ds(pl.multiple_of(2 * rank * tokens, 16), 2 * tokens)
            for start in range(0, w_full.shape[0], 512):
                cut = slice(start, start + 512)
                block = dot(dproj[at, :], w_full[cut, :], NT).astype(bf16)
                for h in range(2):
                    dn_acc[rank, h, :, cut] = block[h * tokens : (h + 1) * tokens]
            return 0

        lax.fori_loop(0, ranks // 2, body, 0)

    order = []
    for t in range(half):
        order.append((planes - 1 - t, t))
    if fused:
        for load in loads:
            load.wait()
        for plane in order[0]:
            weight_rows(plane)
        w_fold.push(0)
        token_half(True)
        dns.push(top)
        ss.push(top)
        for pair in order[1:]:
            for plane in pair:
                weight_rows(plane)
        cs.push(top)
        token_half(False)
    else:
        for load in loads:
            load.wait()
        w_fold.push(0)
        dns.push(top)
        cs.push(top)
        ss.push(top)
    for k in reversed(range(1, top)):
        for ring in (dns, ss, cs):
            ring.push(k)
    w_fold.push(1)
    for ring in (dns, ss, cs):
        ring.push(0)
    for t in range(2, planes - 1):
        w_fold.push(t)
    dns.total(dn_sum)
    for h in range(2):
        for ring in (ss, cs):
            pieces = ring.arrivals(h, 0, 0)
            ref = ring.acc.at[me, h]
            add_all(ref, [ref] + pieces, ring.rows)
    w_fold.total(own)

    def exchange(mask):
        peer = flip_mask(me, mask, bits)
        return remote(own.at[peer], w_sum.at[me], a2a_s.at[mask], a2a_r.at[mask], (dp, peer))

    for mask in range(1, ranks):
        exchange(mask).start()
    keep = pltpu.make_async_copy(own.at[me], w_sum.at[me], local.at[0])
    keep.start()
    for t in range(planes - 1):
        c_fold.push(t)
        s_fold.push(t)
    c_fold.total(c_sum)
    s_fold.total(s_sum)
    keep.wait()
    for mask in range(1, ranks):
        ref = w_sum.at[flip_mask(me, mask, bits)]
        pltpu.make_async_copy(ref, ref, a2a_r.at[mask]).wait()
    for mask in range(1, ranks):
        exchange(mask).wait_send()
    for ring in (dns, cs, ss, w_fold, c_fold, s_fold):
        ring.finish()


def reduce_all(fused, ranks, planes, rows, cols, small, *operands):
    if fused:
        flipped, dproj, w_full = operands
        d, length = flipped.shape[0], dproj.shape[0] // ranks
        wide = w_full.shape[1] - cols
    else:
        dn, w, common = operands
        d, length, wide = dn.shape[-1], 2 * dn.shape[2], common.shape[-1]
    part = (2, length // 2, d)
    wshape = (planes, ranks, rows, cols)
    cshape = (ranks, 2, planes // 2, rows, wide)
    dma = pltpu.SemaphoreType.DMA
    vmem = pl.BlockSpec(memory_space=pltpu.VMEM)
    ring, line = 2 * (ranks - 1), 2 * planes
    results = pl.pallas_call(
        partial(reduce_kernel, fused),
        in_specs=[pl.BlockSpec(memory_space=pl.ANY)] * 4,
        out_specs=[vmem] * 4,
        out_shape=[
            jax.ShapeDtypeStruct(part, f32),
            jax.ShapeDtypeStruct((ranks, rows, cols), bf16),
            jax.ShapeDtypeStruct((rows, wide), f32),
            jax.ShapeDtypeStruct(small.shape[3:], f32),
        ],
        scratch_shapes=[
            pltpu.VMEM((ranks,) + part, bf16),
            pltpu.VMEM(wshape, bf16),
            pltpu.VMEM(cshape, bf16),
            pltpu.VMEM(small.shape, f32),
            pltpu.VMEM(wshape[1:], bf16),
            pltpu.VMEM((ring,) + part[1:], bf16),
            pltpu.VMEM((line,) + wshape[1:], bf16),
            pltpu.VMEM((ring,) + cshape[2:], bf16),
            pltpu.VMEM((ring,) + small.shape[2:], f32),
            pltpu.VMEM((line,) + cshape[3:], bf16),
            pltpu.VMEM((line,) + small.shape[3:], f32),
        ]
        + [dma((ring,))] * 6
        + [dma((line,))] * 6
        + [dma((ranks,)), dma((ranks,)), dma((4,))]
        + ([pltpu.VMEM(a.shape, bf16) for a in operands] if fused else []),
        compiler_params=pltpu.CompilerParams(
            collective_id=1, has_side_effects=True, vmem_limit_bytes=67043328
        ),
        name="reduce_all",
    )(small, *operands)
    dn_sum, w_sum, c_sum, s_sum = results
    return dn_sum.reshape(length, d), w_sum, c_sum, s_sum


def dot(a, b, dims, precision=None):
    return lax.dot_general(
        a, b, (dims, ((), ())), preferred_element_type=f32, precision=precision
    )


NN, NT, TN = ((1,), (0,)), ((1,), (1,)), ((0,), (0,))


def sigmoid(a):
    return 0.5 * jnp.tanh(0.5 * a) + 0.5


def iota(shape, axis):
    return lax.broadcasted_iota(jnp.int32, shape, axis)


def parts(a):
    high = a.astype(bf16)
    return high, (a - high.astype(f32)).astype(bf16)


def fine(a, b, dims):
    left = jnp.concatenate([a[0], a[0], a[1]], axis=dims[0][0])
    right = jnp.concatenate([b[0], b[1], b[0]], axis=dims[1][0])
    return dot(left, right, dims)


def steps_of(raw, bias):
    shifted = raw + bias
    return jnp.maximum(shifted, 0.0) + jnp.log1p(jnp.exp(-jnp.abs(shifted)))


def convolve(pad, conv_ref, tile, count):
    total = conv_ref[CONVK : CONVK + 1, tile]
    for k in range(CONVK):
        total = total + pad[EDGE - CONVK + 1 + k : EDGE - CONVK + 1 + k + count, tile] * conv_ref[k : k + 1, tile]
    return total


class Chunk:
    def __init__(self, step, rate):
        n = SUB
        upper = jnp.where(iota((n, n), 0) <= iota((n, n), 1), 1.0, 0.0)
        self.step = step
        self.rows = dot(step * -rate, upper, NN, highest)
        self.cols = self.rows.T
        self.step_cols = step.T

    def col(self, h):
        return jnp.broadcast_to(self.cols[:, h : h + 1], (SUB, SUB))

    def decay(self, h, col, hide):
        return jnp.exp(col - self.rows[h : h + 1, :] + hide)

    def step_col(self, h):
        return jnp.broadcast_to(self.step_cols[:, h : h + 1], (SUB, SUB))


def fwd_kernel(
    proj_ref, raw_ref, cot_ref, wout_ref, conv_ref, lane_ref, head_ref,
    y_ref, dg_ref, out_ref, state_ref, sum_ref, gated,
    pad, act, carry,
):
    block = proj_ref.shape[0]
    din = y_ref.shape[1]
    conv = conv_ref.shape[1]

    @pl.when(pl.program_id(0) == 0)
    def _():
        carry[...] = jnp.zeros_like(carry)
        pad[0:EDGE, :] = jnp.zeros((EDGE, conv), f32)

    @pl.when(pl.program_id(0) > 0)
    def _():
        pad[0:EDGE, :] = pad[block : block + EDGE, :]

    for j in range(conv // LANES):
        tile = slice(j * LANES, (j + 1) * LANES)
        pad[EDGE:, tile] = proj_ref[:, din + j * LANES : din + (j + 1) * LANES].astype(f32)
        filtered = convolve(pad, conv_ref, tile, block)
        act[:, tile] = filtered * sigmoid(filtered)
    dg_ref[...] = dot(cot_ref[...], wout_ref[...], NT)

    low = iota((SUB, LANES), 1) < HDIM
    hide = jnp.where(iota((SUB, SUB), 0) >= iota((SUB, SUB), 1), 0.0, -1e30)
    for i in range(block // SUB):
        rows = slice(i * SUB, (i + 1) * SUB)
        b, c = parts(act[rows, din : din + NSTATE]), parts(act[rows, din + NSTATE :])
        chunk = Chunk(steps_of(raw_ref[:, rows], head_ref[1]), head_ref[0])
        scores = fine(c, b, NT)
        sq = jnp.zeros((SUB, LANES), f32)
        cross = jnp.zeros((SUB, LANES), f32)
        for j in range(din // LANES):
            tile = slice(j * LANES, (j + 1) * LANES)
            x = act[rows, tile]
            col0, col1 = chunk.col(2 * j), chunk.col(2 * j + 1)
            m0 = chunk.decay(2 * j, col0, hide) * scores
            m1 = chunk.decay(2 * j + 1, col1, hide) * scores
            cexp = jnp.where(low, col0, col1)
            xs = x * jnp.where(low, chunk.step_col(2 * j), chunk.step_col(2 * j + 1))
            zero = jnp.zeros_like(xs)
            split = jnp.concatenate([jnp.where(low, xs, zero), jnp.where(low, zero, xs)], axis=0)
            before = carry[:, tile]
            state_ref[i, :, tile] = before
            y = fine(parts(jnp.concatenate([m0, m1], axis=1)), parts(split), NN)
            y = y + fine(c, parts(before), NN) * jnp.exp(cexp)
            y_ref[rows, tile] = y
            last = cexp[SUB - 1 :, :]
            carry[:, tile] = before * jnp.exp(last) + fine(b, parts(xs * jnp.exp(last - cexp)), TN)
            z = proj_ref[rows, tile].astype(f32)
            v = (y + lane_ref[0:1, tile] * x) * (z * sigmoid(z))
            scaled = v * lane_ref[1:2, tile]
            gated[rows, tile] = scaled.astype(bf16)
            sq = sq + v * v
            cross = cross + scaled * dg_ref[rows, tile]
        ones = jnp.ones((4, LANES), f32)
        sum_ref[0:4, rows] = dot(ones, sq, NT, highest)
        sum_ref[4:8, rows] = dot(ones, cross, NT, highest)
    out_ref[...] = dot(gated[...], wout_ref[...], NN).astype(bf16)


def bwd_kernel(
    total_din,
    proj_ref, rim_ref, raw_ref, y_ref, dg_ref, sum_ref, state_ref, conv_ref, lane_ref, head_ref, spot_ref,
    out_in, o_in,
    dproj_ref, dconv_ref, dlane_ref, dhead_ref, out_sum, o_sum,
    pad, act, slope, dpad, carry, edge, dact,
    *links,
):
    side_reduce(out_in, o_in, out_sum, o_sum, *links)

    block = proj_ref.shape[0]
    din = y_ref.shape[1]
    conv = conv_ref.shape[1]
    step_id = pl.program_id(0)
    first = step_id == pl.num_programs(0) - 1

    @pl.when(step_id == 0)
    def _():
        carry[...] = jnp.zeros_like(carry)
        edge[...] = jnp.zeros_like(edge)
        dpad[0:EDGE, :] = jnp.zeros((EDGE, conv), f32)
        dconv_ref[...] = jnp.zeros_like(dconv_ref)
        dlane_ref[...] = jnp.zeros_like(dlane_ref)
        dhead_ref[...] = jnp.zeros_like(dhead_ref)

    dpad[block : block + EDGE, :] = dpad[0:EDGE, :]
    keep = jnp.where(first, 0.0, 1.0)
    for j in range(conv // LANES):
        tile = slice(j * LANES, (j + 1) * LANES)
        src = slice(din + j * LANES, din + (j + 1) * LANES)
        pad[0:EDGE, tile] = rim_ref[rim_ref.shape[0] - EDGE :, src].astype(f32) * keep
        pad[EDGE:, tile] = proj_ref[:, src].astype(f32)
        filtered = convolve(pad, conv_ref, tile, block)
        s = sigmoid(filtered)
        act[:, tile] = filtered * s
        slope[:, tile] = s * (1.0 + filtered * (1.0 - s))

    low = iota((SUB, LANES), 1) < HDIM
    hide = jnp.where(iota((SUB, SUB), 0) >= iota((SUB, SUB), 1), 0.0, -1e30)
    lower = jnp.where(iota((SUB, SUB), 0) >= iota((SUB, SUB), 1), 1.0, 0.0)
    heads = raw_ref.shape[0]
    dgain = [jnp.zeros((1, LANES), f32) for _ in range(din // LANES)]
    dskip = [jnp.zeros((1, LANES), f32) for _ in range(din // LANES)]
    for i in reversed(range(block // SUB)):
        rows = slice(i * SUB, (i + 1) * SUB)
        b_parts, c_parts = parts(act[rows, din : din + NSTATE]), parts(act[rows, din + NSTATE :])
        chunk = Chunk(steps_of(raw_ref[:, rows], head_ref[1]), head_ref[0])
        scores = fine(c_parts, b_parts, NT)
        sums = sum_ref[:, rows].T
        scale = lax.rsqrt(jnp.broadcast_to(sums[:, 0:1], (SUB, LANES)) * (1.0 / total_din) + epsilon)
        mean = jnp.broadcast_to(sums[:, 4:5], (SUB, LANES)) * (1.0 / total_din) * (scale * scale * scale)
        dscores = jnp.zeros((SUB, SUB), f32)
        d_b = jnp.zeros((SUB, NSTATE), f32)
        d_c = jnp.zeros((SUB, NSTATE), f32)
        d_cum = jnp.zeros((heads, SUB), f32)
        d_step = jnp.zeros((heads, SUB), f32)
        reach = jnp.zeros((heads, 8), f32)
        for j in range(din // LANES):
            tile = slice(j * LANES, (j + 1) * LANES)
            x = act[rows, tile]
            y = y_ref[rows, tile]
            skip, gain = lane_ref[0:1, tile], lane_ref[1:2, tile]
            z = proj_ref[rows, tile].astype(f32)
            sz = sigmoid(z)
            mixed = y + skip * x
            silu = z * sz
            v = mixed * silu
            dg = dg_ref[rows, tile]
            vs = v * scale
            dgain[j] = dgain[j] + jnp.sum(dg * vs, axis=0, keepdims=True)
            dv = scale * (gain * dg) - v * mean
            dy = dv * silu
            dproj_ref[rows, tile] = (dv * mixed * (sz * (1.0 + z * (1.0 - sz)))).astype(bf16)
            dskip[j] = dskip[j] + jnp.sum(dy * x, axis=0, keepdims=True)

            col0, col1 = chunk.col(2 * j), chunk.col(2 * j + 1)
            l0, l1 = chunk.decay(2 * j, col0, hide), chunk.decay(2 * j + 1, col1, hide)
            m = parts(jnp.concatenate([l0 * scores, l1 * scores], axis=0))
            cexp = jnp.where(low, col0, col1)
            step = jnp.where(low, chunk.step_col(2 * j), chunk.step_col(2 * j + 1))
            last = cexp[SUB - 1 :, :]
            grow, tail = jnp.exp(cexp), jnp.exp(last - cexp)
            xs = x * step
            zero = jnp.zeros_like(dy)
            dsplit = parts(jnp.concatenate([jnp.where(low, dy, zero), jnp.where(low, zero, dy)], axis=0))
            xs_parts = parts(xs)
            dm = fine(dsplit, xs_parts, NT)
            dscores = dscores + dm[:SUB] * l0 + dm[SUB:] * l1
            dend = carry[:, tile]
            dend_parts = parts(dend)
            before = state_ref[i, :, tile]
            dxs = fine(m, dsplit, TN) + fine(b_parts, dend_parts, NN) * tail
            grown = parts(dy * grow)
            d_c = d_c + fine(grown, parts(before), NT)
            d_b = d_b + fine(parts(xs * tail), dend_parts, NT)
            dprev = dend * jnp.exp(last) + fine(c_parts, grown, TN)
            carry[:, tile] = dprev
            pick = jnp.where(lax.shift_right_logical(iota((heads, LANES), 1), 6) + 2 * j == iota((heads, LANES), 0), 1.0, 0.0)
            balance = dy * y - xs * dxs
            d_cum = d_cum + dot(pick, balance, NT, highest)
            d_step = d_step + dot(pick, x * dxs, NT, highest)
            crossing = jnp.sum(dprev * before, axis=0, keepdims=True)
            reach = reach + dot(pick, jnp.broadcast_to(crossing, (8, LANES)), NT, highest)
            dact[rows, tile] = dxs * step + skip * dy
        ds_parts = parts(dscores)
        dact[rows, din : din + NSTATE] = d_b + fine(ds_parts, c_parts, TN)
        dact[rows, din + NSTATE :] = d_c + fine(ds_parts, b_parts, NN)
        d_log = dot(d_cum, lower, NN, highest) + edge[...]
        edge[...] = jnp.broadcast_to(reach[:, 0:1], edge.shape)
        raw = raw_ref[:, rows] + head_ref[1]
        draw = (d_step - head_ref[0] * d_log) * sigmoid(raw)
        dproj_ref[rows, din + conv :] = dot(draw.astype(bf16), spot_ref[...], TN).astype(bf16)
        dhead_ref[0] += -chunk.step * d_log
        dhead_ref[1] += draw
    for j in range(din // LANES):
        tile = slice(j * LANES, (j + 1) * LANES)
        dlane_ref[0:1, tile] += dskip[j]
        dlane_ref[1:2, tile] += dgain[j]
    for j in range(conv // LANES):
        tile = slice(j * LANES, (j + 1) * LANES)
        df = dact[:, tile] * slope[:, tile]
        dpad[0:block, tile] = df
        dconv_ref[CONVK : CONVK + 1, tile] += jnp.sum(df, axis=0, keepdims=True)
        back = jnp.zeros((block, LANES), f32)
        for k in range(CONVK):
            shift = CONVK - 1 - k
            dconv_ref[k : k + 1, tile] += jnp.sum(
                df * pad[EDGE - shift : EDGE - shift + block, tile], axis=0, keepdims=True
            )
            back = back + conv_ref[k : k + 1, tile] * dpad[shift : shift + block, tile]
        dproj_ref[:, din + j * LANES : din + (j + 1) * LANES] = back.astype(bf16)


def rows_spec(block, width):
    return pl.BlockSpec((block, width), lambda t: (t, 0))


def whole(shape):
    return pl.BlockSpec(shape, lambda t: (0,) * len(shape))


def mixer_forward(proj, raw, cot, w_out, conv, lanes, heads):
    length, width = proj.shape
    din, d = w_out.shape
    cc = conv.shape[1]
    block = min(TOKENS, length)
    n = block // SUB
    cols = pl.BlockSpec((8, block), lambda t: (0, t))
    return pl.pallas_call(
        fwd_kernel,
        grid=(length // block,),
        in_specs=[
            rows_spec(block, width), cols, rows_spec(block, d), whole(w_out.shape),
            whole(conv.shape), whole(lanes.shape), whole(heads.shape),
        ],
        out_specs=[
            rows_spec(block, din), rows_spec(block, din), rows_spec(block, d),
            pl.BlockSpec((n, NSTATE, din), lambda t: (t, 0, 0)), cols, rows_spec(block, din),
        ],
        out_shape=[
            jax.ShapeDtypeStruct((length, din), f32),
            jax.ShapeDtypeStruct((length, din), f32),
            jax.ShapeDtypeStruct((length, d), bf16),
            jax.ShapeDtypeStruct((length // SUB, NSTATE, din), f32),
            jax.ShapeDtypeStruct((8, length), f32),
            jax.ShapeDtypeStruct((length, din), bf16),
        ],
        scratch_shapes=[
            pltpu.VMEM((block + EDGE, cc), f32),
            pltpu.VMEM((block, cc), f32),
            pltpu.VMEM((NSTATE, din), f32),
        ],
        name="mix_forward",
    )(proj, raw, cot, w_out, conv, lanes, heads)


def side_reduce(out_in, o_in, out_sum, o_sum, acc, land, stage, o_land, out_s, out_r, oz_s, oz_r, mix_s, mix_r, local):
    ranks, planes = acc.shape[0], stage.shape[0]
    me, dp = lax.axis_index("seq"), lax.axis_index("dp")
    outs = Collect(acc, land, out_s, out_r, 16)
    fold = Fold(lambda d: stage.at[d], o_land, planes, oz_s, oz_r, stage.shape[1])
    top = len(bits_of(ranks)) - 1
    load = pltpu.make_async_copy(out_in, acc, local.at[0])

    def move(k, act):
        index = me * planes + k
        plane, to = lax.div(index, ranks), index % ranks

        @pl.when(to != me)
        def _():
            copy = remote(o_in.at[k], stage.at[plane], mix_s.at[k], mix_r.at[plane], (dp, to))
            copy.start() if act else copy.wait_send()

        if act:
            @pl.when(to == me)
            def _():
                pltpu.make_async_copy(o_in.at[k], stage.at[plane], mix_r.at[plane]).start()

    def begin():
        load.start()
        greet(ranks, planes)
        for k in range(planes):
            move(k, True)
        load.wait()
        outs.push(top)

    def settle():
        for d in range(planes):
            pltpu.make_async_copy(stage.at[d], stage.at[d], mix_r.at[d]).wait()
        fold.push(0)

    def end():
        outs.total(out_sum)
        fold.total(o_sum)
        for k in range(planes):
            move(k, False)
        outs.finish()
        fold.finish()

    pushes = {4 * i + 1: partial(outs.push, top - 1 - i) for i in range(top)}
    folds = [settle] + [partial(fold.push, t) for t in range(1, planes - 1)]
    spare = [t for t in range(3, 64) if t not in pushes]
    stages = {0: begin, **pushes, **dict(zip(spare, folds))}
    last = pl.num_programs(0) - 1
    for k, run in sorted(stages.items()):
        pl.when(pl.program_id(0) == k)(run)
    pl.when(pl.program_id(0) == last)(end)


def mixer_backward(ranks, planes, total_din, proj, raw, y, dg, sums, states, conv, lanes, heads, spot, out_part, d_w_out):
    length, width = proj.shape
    din, d = y.shape[1], out_part.shape[1]
    cc = conv.shape[1]
    block = min(TOKENS, length)
    n = block // SUB
    last = length // block - 1
    rim = 16
    assert last > max(4 * len(bits_of(ranks)) - 7, planes + 1 + (planes > 3))
    part = (2, length // ranks // 2, d)
    ring, line = 2 * (ranks - 1), 2 * planes
    dma = pltpu.SemaphoreType.DMA

    def back(block, width):
        return pl.BlockSpec((block, width), lambda t: (last - t, 0))

    cols = pl.BlockSpec((8, block), lambda t: (0, last - t))
    anywhere = pl.BlockSpec(memory_space=pl.ANY)
    *results, out_sum, o_sum = pl.pallas_call(
        partial(bwd_kernel, total_din),
        grid=(length // block,),
        in_specs=[
            back(block, width),
            pl.BlockSpec((rim, width), lambda t: (jnp.maximum((last - t) * (block // rim) - 1, 0), 0)),
            cols, back(block, din), back(block, din), cols,
            pl.BlockSpec((n, NSTATE, din), lambda t: (last - t, 0, 0)),
            whole(conv.shape), whole(lanes.shape), whole(heads.shape), whole(spot.shape), anywhere, anywhere,
        ],
        out_specs=[
            back(block, width + LANES), whole((8, cc)), whole((8, din)), whole((2, 8, SUB)),
            whole(part), whole(d_w_out.shape[1:]),
        ],
        out_shape=[
            jax.ShapeDtypeStruct((length, width + LANES), bf16),
            jax.ShapeDtypeStruct((8, cc), f32),
            jax.ShapeDtypeStruct((8, din), f32),
            jax.ShapeDtypeStruct((2, 8, SUB), f32),
            jax.ShapeDtypeStruct(part, f32),
            jax.ShapeDtypeStruct(d_w_out.shape[1:], f32),
        ],
        scratch_shapes=[
            pltpu.VMEM((block + EDGE, cc), f32),
            pltpu.VMEM((block, cc), f32),
            pltpu.VMEM((block, cc), f32),
            pltpu.VMEM((block + EDGE, cc), f32),
            pltpu.VMEM((NSTATE, din), f32),
            pltpu.VMEM((8, SUB), f32),
            pltpu.VMEM((block, cc), f32),
            pltpu.VMEM((ranks,) + part, bf16),
            pltpu.VMEM((ring,) + part[1:], bf16),
            pltpu.VMEM(d_w_out.shape, bf16),
            pltpu.VMEM((line,) + d_w_out.shape[1:], bf16),
            dma((ring,)), dma((ring,)), dma((line,)), dma((line,)), dma((planes,)), dma((planes,)), dma((1,)),
        ],
        compiler_params=pltpu.CompilerParams(
            collective_id=3, has_side_effects=True, vmem_limit_bytes=67043328
        ),
        name="mix_backward",
    )(
        proj, proj, raw, y, dg, sums, states, conv, lanes, heads, spot,
        out_part.reshape((ranks,) + part), d_w_out,
    )
    return results + [out_sum.reshape(length // ranks, d), o_sum]


def rms_scale(values, gain):
    mean_sq = jnp.mean(values * values, axis=-1, keepdims=True)
    return values * lax.rsqrt(mean_sq + epsilon) * gain


def widen(array, size, axis):
    pads = [(0, 0)] * array.ndim
    pads[axis] = (0, size - array.shape[axis])
    return jnp.pad(array, pads)


def per_device(
    tokens,
    cotangent,
    in_weight,
    out_weight,
    conv_weight,
    conv_bias,
    norm_gain,
    gate_gain,
    decay_rate,
    dt_bias,
    d_skip,
):
    ranks = lax.axis_size("seq")
    me = lax.axis_index("seq")
    both = ("dp", "seq")
    heads = decay_rate.shape[0] // ranks
    din = heads * HDIM
    padded = -(-din // LANES) * LANES
    din_all = din * ranks
    rows, width = in_weight.shape
    conv_all = din_all + 2 * NSTATE
    main = 2 * padded + 2 * NSTATE

    def mine(array, size, axis=0):
        return lax.dynamic_slice_in_dim(array, me * size, size, axis)

    planes = lax.axis_size("dp")
    x_own = tokens[0].astype(f32)
    send = jnp.concatenate(
        [
            widen(in_weight[:, :din_all].reshape(rows, ranks, din), padded, 2),
            widen(in_weight[:, din_all : 2 * din_all].reshape(rows, ranks, din), padded, 2),
        ],
        axis=2,
    ).transpose(1, 0, 2)
    d = in_weight.shape[0] * ranks * planes
    rank_id = lax.axis_index("dp") * ranks + me
    small = [norm_gain, gate_gain, conv_weight.reshape(-1), conv_bias]
    sizes = [a.shape[0] for a in small]
    room = rows * HDIM - d
    if room >= sum(sizes):
        placed = lax.dynamic_update_slice_in_dim(jnp.zeros((d,), bf16), norm_gain, rank_id * rows, 0)
        packed = jnp.concatenate([placed, widen(jnp.concatenate(small), room, 0)])
    else:
        packed = widen(jnp.concatenate(small), rows * HDIM, 0)
    common = jnp.concatenate(
        [
            in_weight[:, 2 * din_all : 2 * din_all + 2 * NSTATE],
            widen(in_weight[:, din_all + conv_all :], HDIM, 1),
            packed.reshape(rows, HDIM),
        ],
        axis=1,
    )
    cot, w_out, common, fused, *rest = gather_all(
        ranks, planes, tokens[0], cotangent[0], send, out_weight, common
    )
    w_out = widen(w_out, padded, 0)
    packed = common[..., 2 * NSTATE + HDIM :].reshape(ranks * planes, rows * HDIM).astype(f32)
    if room >= sum(sizes):
        packed = packed[:, d:]
    gain_norm, gain_gate, conv_w, conv_b = (
        packed[:, sum(sizes[:k]) : sum(sizes[: k + 1])].reshape(-1) for k in range(4)
    )
    conv_w = conv_w.reshape(-1, CONVK)
    taps = jnp.concatenate([conv_w.T, conv_b[None], jnp.zeros((8 - CONVK - 1, conv_all), f32)], axis=0)
    conv = jnp.concatenate([widen(mine(taps, din, 1), padded, 1), taps[:, din_all:]], axis=1)
    if fused:
        raw, flipped, proj, w_full = rest
    else:
        tok, w_all = rest
        w_full = jnp.concatenate([w_all, common.reshape(-1, common.shape[-1])], axis=1)
        normed = rms_scale(tok.astype(f32), gain_norm).astype(bf16)
        proj = dot(normed, w_full[:, :main], NN).astype(bf16)
        raw = dot(w_full[:, main : main + HDIM].T, normed, NT).astype(bf16).astype(f32)
    raw = widen(mine(raw, heads), 8, 0)
    rate, bias, skip = (mine(a, heads) for a in (decay_rate, dt_bias, d_skip))
    lanes = jnp.stack([jnp.repeat(skip, HDIM), mine(gain_gate, din)])
    lanes = widen(widen(lanes, padded, 1), 8, 0)
    head_rows = jnp.broadcast_to(widen(jnp.stack([rate, bias]), 8, 1)[:, :, None], (2, 8, SUB))

    y, dg, out_part, states, sums, gated = mixer_forward(proj, raw, cot, w_out, conv, lanes, head_rows)
    sums = plane_sum(ranks, sums[::4].reshape(8, -1)).reshape(2, -1)
    inverse = lax.rsqrt(sums[0] / din_all + epsilon)[:, None]
    d_w_out = dot((gated * inverse).astype(bf16), cot, TN)[:din].astype(bf16)
    spot = (jnp.arange(LANES)[None] == me * heads + jnp.arange(8)[:, None]) & (jnp.arange(8)[:, None] < heads)
    d_proj, d_conv, d_lane, d_head, out_sum, grad_out = mixer_backward(
        ranks, planes, din_all, proj, raw, y, dg, jnp.repeat(sums, 4, axis=0), states, conv, lanes, head_rows,
        spot.astype(bf16), out_part, d_w_out.reshape(planes, -1, d),
    )

    def by_owner(array):
        split = array.reshape((2, planes // 2, ranks) + array.shape[1:])
        return split.transpose((2, 0, 1) + tuple(range(3, split.ndim)))

    def place(own, size):
        return lax.dynamic_update_slice_in_dim(
            jnp.zeros((size * ranks,) + own.shape[1:], f32), own, me * size, 0
        )

    d_cw, d_cb = d_conv[:CONVK].T, d_conv[CONVK]
    full_cw = jnp.concatenate([place(d_cw[:din], din), d_cw[padded:]], axis=0)
    full_cb = jnp.concatenate([place(d_cb[:din], din), d_cb[padded:]], axis=0)
    d_skp = jnp.sum(d_lane[0, :din].reshape(heads, HDIM), axis=1)
    d_rate, d_bias = jnp.sum(d_head, axis=2)[:, :heads]
    devices = planes * ranks
    head_part = jnp.concatenate([place(a, heads) for a in (d_rate, d_bias, d_skp)])
    fields = [
        a.reshape(devices, -1) for a in (full_cw, full_cb, place(d_lane[1, :din], din))
    ] + [jnp.broadcast_to(head_part, (devices,) + head_part.shape)]
    ends = [0]
    for a in fields:
        ends.append(ends[-1] + a.shape[1])
    small = widen(jnp.concatenate(fields, axis=1), 8 * LANES, 1).reshape(devices, 8, LANES)
    if fused:
        operands = flipped, d_proj, w_full
    else:
        d_w = dot(normed, d_proj, TN).astype(bf16)
        part = dot(d_proj, w_full, NT).astype(bf16)
        operands = (
            part.reshape(ranks, 2, -1, d),
            d_w[:, : 2 * padded].reshape(planes, ranks, rows, -1),
            by_owner(d_w[:, 2 * padded :].reshape(planes * ranks, rows, -1)),
        )
    d_normed, w_sum, bc_sum, small_sum = reduce_all(
        fused, ranks, planes, rows, 2 * padded, by_owner(small), *operands
    )
    block_out = (x_own + mine(inverse, x_own.shape[0]) * out_sum).astype(bf16)
    gain = gain_norm * d_normed
    inv = lax.rsqrt(jnp.mean(x_own * x_own, axis=1, keepdims=True) + epsilon)
    d_xn = inv * (gain - x_own * (inv * inv * jnp.mean(gain * x_own, axis=1, keepdims=True)))
    grad_x = cotangent[0].astype(f32) + d_xn
    spread = w_sum.astype(f32).transpose(1, 0, 2)
    grad_in = jnp.concatenate(
        [
            spread[:, :, :din].reshape(rows, din_all),
            spread[:, :, padded : padded + din].reshape(rows, din_all),
            bc_sum[:, : 2 * NSTATE + heads * ranks],
        ],
        axis=1,
    )
    g_gain = jnp.sum(grad_in * in_weight.astype(f32), axis=1) / norm_gain.astype(f32)
    small_sum = small_sum.reshape(-1)
    g_cw, g_cb, g_gate, head_sums = (small_sum[a:b] for a, b in zip(ends[:-1], ends[1:]))
    g_cw = g_cw.reshape(-1, CONVK)
    head_sums = head_sums.reshape(3, -1)
    return (
        block_out[None],
        grad_x[None],
        grad_in,
        grad_out,
        g_cw,
        g_cb,
        g_gain,
        g_gate,
        head_sums[0],
        head_sums[1],
        head_sums[2],
    )


def solution(mesh):
    rows = P(("dp", "seq"), None)
    flat = P(("dp", "seq"))
    act = P("dp", "seq", None)
    return jax.shard_map(
        per_device,
        mesh=mesh,
        in_specs=(act, act, rows, rows, rows, flat, flat, flat, P(), P(), P()),
        out_specs=(act, act, rows, rows, rows, flat, flat, flat, P(), P(), P()),
        check_vma=False,
    )
```

```python
from functools import partial

import jax
import jax.numpy as jnp
from jax import lax
from jax.experimental import pallas as pl
from jax.experimental.pallas import tpu as pltpu
from jax.sharding import PartitionSpec as P

HDIM = 64
NSTATE = 128
CONVK = 4
LANES = 128
SUB = 128
TOKENS = 256
EDGE = 8

epsilon = 1e-05
highest = lax.Precision.HIGHEST
bf16 = jnp.bfloat16
f32 = jnp.float32


MESH = pl.DeviceIdType.MESH


def flip(index, bit):
    return index + bit * (1 - 2 * (lax.div(index, bit) % 2))


def flip_mask(index, mask, bits):
    for bit in bits:
        if mask & bit:
            index = flip(index, bit)
    return index


def bits_of(size):
    return [1 << k for k in range(size.bit_length() - 1)]


def both_orders(size):
    bits = bits_of(size)
    slow = bits[1:]
    return [slow + bits[:1], slow[::-1] + bits[:1]]


def remote(src, dst, send, recv, to):
    return pltpu.make_async_remote_copy(
        src_ref=src, dst_ref=dst, send_sem=send, recv_sem=recv, device_id=to, device_id_type=MESH
    )


class Spread:
    def __init__(self, buf, send, recv, own=None):
        self.size = buf.shape[0]
        self.bits = bits_of(self.size)
        self.orders = both_orders(self.size)
        self.buf, self.send, self.recv = buf, send, recv
        self.me, self.dp = lax.axis_index("seq"), lax.axis_index("dp")
        self.own = own

    def masks(self, half):
        order = self.orders[half]
        got = [0]
        for bit in order:
            got = got + [m | bit for m in got]
        return got

    def copy(self, half, mask, bit):
        origin = flip_mask(self.me, mask, self.bits)
        dst = self.buf.at[origin, half]
        src = self.own.at[half] if (mask == 0 and self.own is not None) else dst
        slot = half * self.size + (mask | bit)
        return remote(src, dst, self.send.at[slot], self.recv.at[slot], (self.dp, flip(self.me, bit)))

    def start(self, half, mask):
        order = self.orders[half]
        after = max((order.index(b) for b in self.bits if mask & b), default=-1) + 1
        for bit in order[after:]:
            self.copy(half, mask, bit).start()

    def arrive(self, half, mask):
        order = self.orders[half]
        top = order[max(order.index(b) for b in self.bits if mask & b)]
        self.copy(half, mask & ~top, top).wait_recv()

    def forward(self, group):
        for k in range(1 << group, 2 << group):
            for half in range(2):
                mask = self.masks(half)[k]
                self.arrive(half, mask)
                self.start(half, mask)

    def finish(self):
        for half in range(2):
            for mask in range(1, self.size):
                order = self.orders[half]
                top = order[max(order.index(b) for b in self.bits if mask & b)]
                self.copy(half, mask & ~top, top).wait_send()

    @property
    def groups(self):
        return len(self.bits)


class Line:
    def __init__(self, at, size, send, recv):
        self.at, self.size, self.send, self.recv = at, size, send, recv
        self.me, self.seq = lax.axis_index("dp"), lax.axis_index("seq")

    def copy(self, way, hop):
        block = self.me - way * (hop - 1)
        slot = (self.size if way > 0 else 0) + hop
        ref = self.at(block)
        return remote(ref, ref, self.send.at[slot], self.recv.at[slot], (self.me + way, self.seq))

    def sends(self, way, hop):
        block = self.me - way * (hop - 1)
        to = self.me + way
        return (block >= 0) & (block < self.size) & (to >= 0) & (to < self.size)

    def start(self, hop):
        for way in (1, -1):
            @pl.when(self.sends(way, hop))
            def _():
                self.copy(way, hop).start()

    def arrive(self, hop):
        for way in (1, -1):
            source = self.me - way * hop
            @pl.when((source >= 0) & (source < self.size))
            def _():
                ref = self.at(source)
                slot = (self.size if way > 0 else 0) + hop
                pltpu.make_async_copy(ref, ref, self.recv.at[slot]).wait()

    def forward(self, hop):
        self.arrive(hop)
        if hop + 1 < self.size:
            self.start(hop + 1)

    def finish(self):
        for hop in range(1, self.size):
            for way in (1, -1):
                @pl.when(self.sends(way, hop))
                def _():
                    self.copy(way, hop).wait_send()


def greet(ranks, planes):
    me, dp = lax.axis_index("seq"), lax.axis_index("dp")
    barrier = pltpu.get_barrier_semaphore()
    for mask in range(1, ranks):
        pl.semaphore_signal(
            barrier, inc=1, device_id=(dp, flip_mask(me, mask, bits_of(ranks))), device_id_type=MESH
        )
    for way in (1, -1):
        @pl.when((dp + way >= 0) & (dp + way < planes))
        def _():
            pl.semaphore_signal(barrier, inc=1, device_id=(dp + way, me), device_id_type=MESH)
    near = jnp.where(dp > 0, 1, 0) + jnp.where(dp < planes - 1, 1, 0)
    pl.semaphore_wait(barrier, ranks - 1 + near)


def norm_tokens(tok, common, normed, rows, w_full):
    ranks, planes = tok.shape[0], 2 * common.shape[2]
    width = w_full.shape[1] - common.shape[-1]
    strip, tile = 32, tok.shape[2]
    d = tok.shape[3]
    half = planes // 2

    def lay(i, gains):
        at = pl.ds(pl.multiple_of(i * rows, 16), rows)
        plane, rank = lax.div(i, ranks), i % ranks
        shared = common[rank, lax.div(plane, half), plane % half]
        w_full[at, width:] = shared
        return gains + shared[: d // HDIM, 2 * NSTATE :].astype(f32)

    gains = lax.fori_loop(0, planes * ranks, lay, jnp.zeros((d // HDIM, LANES), f32))
    moved = pltpu.roll(gains, HDIM, 1)
    low = iota((1, LANES), 1) < HDIM
    gain = [jnp.where(low, moved[2 * j : 2 * j + 1], gains[2 * j + 1 : 2 * j + 2]) for j in range(d // LANES)]

    def norm(i, _):
        per = tile // strip
        part = lax.div(i, per)
        at = pl.ds(pl.multiple_of((i % per) * strip, strip), strip)
        x = tok.at[lax.div(part, 2), part % 2][at, :].astype(f32)
        scale = lax.rsqrt(jnp.sum(x * x, axis=1, keepdims=True) * (1.0 / d) + epsilon)
        to = pl.ds(pl.multiple_of(i * strip, strip), strip)
        for j in range(d // LANES):
            cut = slice(j * LANES, (j + 1) * LANES)
            normed[to, cut] = (x[:, cut] * scale * gain[j]).astype(bf16)
        return 0

    lax.fori_loop(0, ranks * 2 * tile // strip, norm, 0)


def stored(i, flipped, proj, flip_out, proj_out, store):
    at = pl.ds(pl.multiple_of(i * 256, 256), 256)
    return (
        pltpu.make_async_copy(proj.at[at, :], proj_out.at[at, :], store.at[0, i]),
        pltpu.make_async_copy(flipped.at[:, at], flip_out.at[:, at], store.at[1, i]),
    )


def project(w, normed, flipped, proj, raw, w_full, flip_out, proj_out, store):
    planes, ranks, rows, width = w.shape
    total, d = normed.shape
    main = width + 2 * NSTATE

    def lay(i, _):
        at = pl.ds(pl.multiple_of(i * rows, 16), rows)
        w_full[at, :width] = w[lax.div(i, ranks), i % ranks]
        return 0

    lax.fori_loop(0, planes * ranks, lay, 0)

    def multiply(i, _):
        at = pl.ds(pl.multiple_of(i * 256, 256), 256)
        for start in range(0, main, 512):
            cut = slice(start, min(start + 512, main))
            proj[at, cut] = dot(normed[at, :], w_full[:, cut], NN).astype(bf16)
        for k in range(2):
            to = pl.ds(pl.multiple_of(i * 256 + k * LANES, LANES), LANES)
            for j in range(d // LANES):
                tokens = normed[to, j * LANES : (j + 1) * LANES].astype(f32)
                flipped[j * LANES : (j + 1) * LANES, to] = tokens.T.astype(bf16)
        steps = dot(normed[at, :], w_full[:, main:], NN).astype(bf16).astype(f32)
        for k in range(2):
            to = pl.ds(pl.multiple_of(i * 256 + k * LANES, LANES), LANES)
            raw[:, to] = steps[k * LANES : (k + 1) * LANES].T[: raw.shape[0]]
        for copy in stored(i, flipped, proj, flip_out, proj_out, store):
            copy.start()
        return 0

    lax.fori_loop(0, total // 256, multiply, 0)


def gather_kernel(
    fused, tok_in, cot_in, w_in, wout_in, common_in,
    cot, wout, common, *rest,
):
    if fused:
        raw, flip_out, proj_out, full_out, tok, w, normed, flipped, proj, w_full, store, *rest = rest
    else:
        tok, w, *rest = rest
    (stage, tok_s, tok_r, cot_s, cot_r, com_s, com_r, wz_s, wz_r, oz_s, oz_r, cz_s, cz_r,
    a2a_s, a2a_r, mix_s, mix_r, local) = rest
    ranks, planes = tok.shape[0], w.shape[0]
    me, dp = lax.axis_index("seq"), lax.axis_index("dp")
    bits = bits_of(ranks)
    greet(ranks, planes)
    half = planes // 2
    tokens = Spread(tok, tok_s, tok_r, tok_in)
    cots = Spread(cot, cot_s, cot_r, cot_in)
    commons = Spread(common, com_s, com_r)
    w_line = Line(lambda d: w.at[d], planes, wz_s, wz_r)
    o_line = Line(lambda d: stage.at[d], planes, oz_s, oz_r)
    c_line = Line(lambda d: common.at[me, lax.div(d, half), d % half], planes, cz_s, cz_r)

    def exchange(mask):
        peer = flip_mask(me, mask, bits)
        return remote(w_in.at[peer], w.at[dp, me], a2a_s.at[mask], a2a_r.at[mask], (dp, peer))

    def arrived(mask):
        ref = w.at[dp, flip_mask(me, mask, bits)]
        return pltpu.make_async_copy(ref, ref, a2a_r.at[mask])

    for mask in range(1, ranks):
        exchange(mask).start()
    places = [
        pltpu.make_async_copy(w_in.at[me], w.at[dp, me], local.at[0]),
        pltpu.make_async_copy(common_in, common.at[me, lax.div(dp, half), dp % half], local.at[1]),
        pltpu.make_async_copy(wout_in, stage.at[dp], local.at[2]),
        pltpu.make_async_copy(tok_in, tok.at[me], local.at[3]),
        pltpu.make_async_copy(cot_in, cot.at[me], local.at[4]),
    ]
    for place in places:
        place.start()
    for h in range(2):
        tokens.start(h, 0)
    for place in places:
        place.wait()
    c_line.start(1)
    for hop in range(1, planes):
        c_line.forward(hop)
    for mask in range(1, ranks):
        arrived(mask).wait()
    w_line.start(1)
    o_line.start(1)
    tokens.forward(0)
    for h in range(2):
        commons.start(h, 0)
    for h in range(2):
        cots.start(h, 0)
    w_line.forward(1)
    o_line.forward(1)
    for group in range(1, tokens.groups - 1):
        tokens.forward(group)
    for hop in range(2, planes - 1):
        o_line.forward(hop)
    for group in range(commons.groups - 1):
        commons.forward(group)
    for hop in range(2, planes - 1):
        w_line.forward(hop)
    tokens.forward(tokens.groups - 1)
    commons.forward(commons.groups - 1)
    if fused:
        norm_tokens(tok, common, normed, w.shape[2], w_full)
    cots.forward(0)
    o_line.forward(planes - 1)

    def moved(d):
        index = d * ranks + me
        return lax.div(index, planes), index % planes

    for d in range(planes):
        to, place = moved(d)

        @pl.when(to == me)
        def _():
            pltpu.make_async_copy(stage.at[d], wout.at[place], mix_r.at[place]).start()

        @pl.when(to != me)
        def _():
            remote(stage.at[d], wout.at[place], mix_s.at[d], mix_r.at[place], (dp, to)).start()

    w_line.forward(planes - 1)
    if fused:
        project(w, normed, flipped, proj, raw, w_full, flip_out, proj_out, store)
        full = pltpu.make_async_copy(w_full, full_out, local.at[0])
        full.start()
    for group in range(1, cots.groups):
        cots.forward(group)
    for place in range(planes):
        pltpu.make_async_copy(wout.at[place], wout.at[place], mix_r.at[place]).wait()
    for d in range(planes):
        to, place = moved(d)

        @pl.when(to != me)
        def _():
            remote(stage.at[d], wout.at[place], mix_s.at[d], mix_r.at[place], (dp, to)).wait_send()

    for mask in range(1, ranks):
        exchange(mask).wait_send()
    for ring in (tokens, cots, commons, w_line, o_line, c_line):
        ring.finish()
    if fused:
        full.wait()
        for i in range(store.shape[1]):
            for copy in stored(i, flipped, proj, flip_out, proj_out, store):
                copy.wait()


def gather_all(ranks, planes, tok, cot, w, w_out, common):
    length, d = tok.shape
    halves = (2, length // 2, d)
    total = ranks * length
    rows, cols = w.shape[1:]
    fused = rows % 16 == 0 and rows * HDIM >= 2 * d and length % 256 == 0 and cols % 768 == 0
    dma = pltpu.SemaphoreType.DMA
    vmem = pl.BlockSpec(memory_space=pltpu.VMEM)
    ring, line = 2 * ranks, 2 * planes
    anywhere = pl.BlockSpec(memory_space=pl.ANY)
    buffers = [((ranks,) + halves, bf16), ((planes,) + w.shape, bf16)]
    out = [
        ((ranks,) + halves, bf16), ((planes,) + w_out.shape, bf16), ((ranks, 2, planes // 2) + common.shape, bf16)
    ]
    places = [vmem, vmem, vmem]
    stores = []
    if fused:
        own = [((d, total), bf16), ((total, cols + 2 * NSTATE), bf16), ((d, cols + common.shape[1]), bf16)]
        out += [((HDIM, total), f32)] + own
        places += [vmem, anywhere, anywhere, anywhere]
        stores = [pltpu.VMEM(*s) for s in buffers + [((total, d), bf16)] + own] + [dma((2, total // 256))]
    else:
        out += buffers
        places += [vmem, vmem]
    cot_all, out_all, common_all, *rest = pl.pallas_call(
        partial(gather_kernel, fused),
        in_specs=[anywhere] * 5,
        out_specs=places,
        out_shape=[jax.ShapeDtypeStruct(*s) for s in out],
        scratch_shapes=stores
        + [pltpu.VMEM((planes,) + w_out.shape, bf16)]
        + [dma((ring,))] * 6
        + [dma((line,))] * 6
        + [dma((ranks,)), dma((ranks,)), dma((planes,)), dma((planes,)), dma((5,))],
        compiler_params=pltpu.CompilerParams(
            collective_id=0, has_side_effects=True, vmem_limit_bytes=67043328
        ),
        name="gather_all",
    )(tok.reshape(halves), cot.reshape(halves), w, w_out, common)
    common_all = common_all.reshape((ranks, planes) + common.shape).transpose(1, 0, 2, 3)
    cot_all, out_all = cot_all.reshape(total, d), out_all.reshape(planes * w_out.shape[0], d)
    if fused:
        return (cot_all, out_all, common_all, True) + tuple(rest)
    tok_all, w_all = rest
    return cot_all, out_all, common_all, False, tok_all.reshape(total, d), w_all.reshape(-1, cols)


def plane_sum_kernel(x_in, total, land, send, recv):
    ranks = land.shape[0]
    me, dp = lax.axis_index("seq"), lax.axis_index("dp")
    bits = bits_of(ranks)
    barrier = pltpu.get_barrier_semaphore()
    for mask in range(1, ranks):
        pl.semaphore_signal(barrier, inc=1, device_id=(dp, flip_mask(me, mask, bits)), device_id_type=MESH)
    pl.semaphore_wait(barrier, ranks - 1)

    def copy(mask):
        return remote(x_in, land.at[mask], send.at[mask], recv.at[mask], (dp, flip_mask(me, mask, bits)))

    for mask in range(1, ranks):
        copy(mask).start()
    value = x_in[...]
    for mask in range(1, ranks):
        copy(mask).wait_recv()
        value = value + land[mask]
    total[...] = value
    for mask in range(1, ranks):
        copy(mask).wait_send()


def plane_sum(ranks, x):
    vmem = pl.BlockSpec(memory_space=pltpu.VMEM)
    return pl.pallas_call(
        plane_sum_kernel,
        in_specs=[vmem],
        out_specs=vmem,
        out_shape=jax.ShapeDtypeStruct(x.shape, f32),
        scratch_shapes=[pltpu.VMEM((ranks,) + x.shape, f32)] + [pltpu.SemaphoreType.DMA((ranks,))] * 2,
        compiler_params=pltpu.CompilerParams(collective_id=2, has_side_effects=True),
        name="plane_sum",
    )(x)


def add_into(dst, pieces, rows):
    count = dst.shape[-2]
    rows = 16 if count % 16 == 0 else count

    def body(i, _):
        at = pl.ds(pl.multiple_of(i * rows, rows), rows)
        total = pieces[0][at, :].astype(f32)
        for piece in pieces[1:]:
            total = total + piece[at, :].astype(f32)
        dst[at, :] = total.astype(dst.dtype)
        return 0

    lax.fori_loop(0, count // rows, body, 0)


def flat_views(ref):
    if len(ref.shape) == 2:
        return [ref]
    return [view for k in range(ref.shape[0]) for view in flat_views(ref.at[k])]


def add_all(dst, pieces, rows):
    for views in zip(flat_views(dst), *(flat_views(p) for p in pieces)):
        add_into(views[0], views[1:], rows)


class Collect:
    def __init__(self, acc, land, send, recv, rows):
        self.size = acc.shape[0]
        self.bits = bits_of(self.size)
        self.orders = both_orders(self.size)
        self.acc, self.land, self.send, self.recv, self.rows = acc, land, send, recv, rows
        self.me, self.dp = lax.axis_index("seq"), lax.axis_index("dp")

    def copy(self, half, mask, bit):
        slot = half * (self.size - 1) + (mask | bit) - 1
        owner = flip_mask(self.me, mask | bit, self.bits)
        return remote(
            self.acc.at[owner, half], self.land.at[slot], self.send.at[slot], self.recv.at[slot],
            (self.dp, flip(self.me, bit)),
        )

    def subsets(self, bits):
        got = [0]
        for bit in bits:
            got = got + [m | bit for m in got]
        return got

    def arrivals(self, half, mask, after):
        pieces = []
        for bit in self.orders[half][after:]:
            slot = half * (self.size - 1) + (mask | bit) - 1
            pltpu.make_async_copy(self.land.at[slot], self.land.at[slot], self.recv.at[slot]).wait()
            pieces.append(self.land.at[slot])
        return pieces

    def push(self, k):
        for half in range(2):
            order = self.orders[half]
            for mask in self.subsets(order[:k]):
                full = mask | order[k]
                pieces = self.arrivals(half, full, k + 1)
                if pieces:
                    ref = self.acc.at[flip_mask(self.me, full, self.bits), half]
                    add_all(ref, [ref] + pieces, self.rows)
                self.copy(half, mask, order[k]).start()

    def total(self, dst):
        for half in range(2):
            pieces = self.arrivals(half, 0, 0)
            add_all(dst.at[half], [self.acc.at[self.me, half]] + pieces, self.rows)

    def finish(self):
        for half in range(2):
            order = self.orders[half]
            for k in range(len(order)):
                for mask in self.subsets(order[:k]):
                    self.copy(half, mask, order[k]).wait_send()


class Fold:
    def __init__(self, at, land, size, send, recv, rows):
        self.at, self.land, self.size, self.send, self.recv, self.rows = at, land, size, send, recv, rows
        self.me, self.seq = lax.axis_index("dp"), lax.axis_index("seq")

    def copy(self, way, block):
        slot = (self.size if way > 0 else 0) + block
        return remote(
            self.at(block), self.land.at[slot], self.send.at[slot], self.recv.at[slot], (self.me + way, self.seq)
        )

    def landed(self, way, block):
        slot = (self.size if way > 0 else 0) + block
        ref = self.land.at[slot]
        pltpu.make_async_copy(ref, ref, self.recv.at[slot]).wait()
        return ref

    def sends(self, way, block):
        return block > self.me if way > 0 else block < self.me

    def push(self, t):
        last = self.size - 1
        for way, block in ((1, last + self.me - t), (-1, t - last + self.me)):
            @pl.when((block >= 0) & (block <= last))
            def _():
                behind = self.me - way

                @pl.when((behind >= 0) & (behind < self.size))
                def _():
                    add_all(self.at(block), [self.at(block), self.landed(way, block)], self.rows)

                self.copy(way, block).start()

    def total(self, dst):
        me = self.me
        add_all(dst, [self.at(me)], self.rows)
        for way in (1, -1):
            behind = me - way

            @pl.when((behind >= 0) & (behind < self.size))
            def _():
                add_all(dst, [dst, self.landed(way, me)], self.rows)

    def finish(self):
        for t in range(self.size):
            for way in (1, -1):
                @pl.when(self.sends(way, t))
                def _():
                    self.copy(way, t).wait_send()


def input_grad(dn, tok, cot, gain):
    count, d = dn.shape[1:]

    for h in range(dn.shape[0]):
        def body(i, _):
            at = pl.ds(pl.multiple_of(i * 16, 16), 16)
            x = tok[h, at, :].astype(f32)
            g = gain[...] * dn[h, at, :]
            inv = lax.rsqrt(jnp.sum(x * x, axis=1, keepdims=True) * (1.0 / d) + epsilon)
            along = jnp.sum(g * x, axis=1, keepdims=True) * (1.0 / d)
            dn[h, at, :] = cot[h, at, :].astype(f32) + inv * (g - x * (inv * inv * along))
            return 0

        lax.fori_loop(0, count // 16, body, 0)


def reduce_kernel(fused, s_in, tok_own, cot_own, gain_in, *refs):
    if fused:
        flip_in, dproj_in, wfull_in, *refs = refs
    else:
        dn_in, w_in, c_in, *refs = refs
    if fused:
        dn_sum, g_in, s_sum, *refs = refs
    else:
        dn_sum, w_sum, c_sum, s_sum, *refs = refs
    (dn_acc, w_acc, c_acc, s_acc, own,
     dn_land, w_land, c_land, s_land, cz_land, sz_land,
     dn_s, dn_r, cr_s, cr_r, sr_s, sr_r, wz_s, wz_r, cz_s, cz_r, sz_s, sz_r, a2a_s, a2a_r, local, *refs) = refs
    ranks, planes = dn_acc.shape[0], w_acc.shape[0]
    me, dp = lax.axis_index("seq"), lax.axis_index("dp")
    bits = bits_of(ranks)
    half = planes // 2
    top = len(bits) - 1
    rows, cols = w_acc.shape[2:]
    tokens = dn_acc.shape[2]
    if fused:
        flipped, dproj, w_full, w_sum, c_sum = refs
        pairs = [(flip_in, flipped), (dproj_in, dproj), (s_in, s_acc), (wfull_in, w_full)]
    else:
        pairs = [(w_in, w_acc), (c_in, c_acc), (s_in, s_acc), (dn_in, dn_acc)]
    loads = [pltpu.make_async_copy(src, dst, local.at[k]) for k, (src, dst) in enumerate(pairs)]
    for load in loads:
        load.start()
    greet(ranks, planes)
    dns = Collect(dn_acc, dn_land, dn_s, dn_r, 16)
    cs = Collect(c_acc, c_land, cr_s, cr_r, c_acc.shape[-2])
    ss = Collect(s_acc, s_land, sr_s, sr_r, 8)

    def own_c(d):
        return c_acc.at[me, lax.div(d, half), d % half]

    def own_s(d):
        return s_acc.at[me, lax.div(d, half), d % half]

    w_fold = Fold(lambda d: w_acc.at[d], w_land, planes, wz_s, wz_r, rows)
    c_fold = Fold(own_c, cz_land, planes, cz_s, cz_r, c_acc.shape[-2])
    s_fold = Fold(own_s, sz_land, planes, sz_s, sz_r, 8)

    def weight_rows(plane):
        left = pl.ds(plane * ranks * rows, ranks * rows)
        for start in range(0, dproj.shape[1], 384):
            cut = slice(start, start + 384)
            block = dot(flipped[left, :], dproj[:, cut], NN).astype(bf16)
            for rank in range(ranks):
                piece = block[rank * rows : (rank + 1) * rows]
                if start < cols:
                    w_acc[plane, rank, :, cut] = piece
                else:
                    c_acc[rank, plane // half, plane % half, :, start - cols : start - cols + 384] = piece

    def token_half(far):
        mine = me % 2

        def body(i, _):
            rank = 2 * i + (1 - mine if far else mine)
            at = pl.ds(pl.multiple_of(2 * rank * tokens, 16), 2 * tokens)
            for start in range(0, w_full.shape[0], 512):
                cut = slice(start, start + 512)
                block = dot(dproj[at, :], w_full[cut, :], NT).astype(bf16)
                for h in range(2):
                    dn_acc[rank, h, :, cut] = block[h * tokens : (h + 1) * tokens]
            return 0

        lax.fori_loop(0, ranks // 2, body, 0)

    order = []
    for t in range(half):
        order.append((planes - 1 - t, t))
    if fused:
        for load in loads:
            load.wait()
        for plane in order[0]:
            weight_rows(plane)
        w_fold.push(0)
        token_half(True)
        dns.push(top)
        ss.push(top)
        for pair in order[1:]:
            for plane in pair:
                weight_rows(plane)
        cs.push(top)
        token_half(False)
    else:
        for load in loads:
            load.wait()
        w_fold.push(0)
        dns.push(top)
        cs.push(top)
        ss.push(top)
    for k in reversed(range(1, top)):
        for ring in (dns, ss, cs):
            ring.push(k)
    w_fold.push(1)
    for ring in (dns, ss, cs):
        ring.push(0)
    for t in range(2, planes - 1):
        w_fold.push(t)
    dns.total(dn_sum)
    input_grad(dn_sum, tok_own, cot_own, gain_in)
    for h in range(2):
        for ring in (ss, cs):
            pieces = ring.arrivals(h, 0, 0)
            ref = ring.acc.at[me, h]
            add_all(ref, [ref] + pieces, ring.rows)
    w_fold.total(own)

    def exchange(mask):
        peer = flip_mask(me, mask, bits)
        return remote(own.at[peer], w_sum.at[me], a2a_s.at[mask], a2a_r.at[mask], (dp, peer))

    for mask in range(1, ranks):
        exchange(mask).start()
    keep = pltpu.make_async_copy(own.at[me], w_sum.at[me], local.at[0])
    keep.start()
    for t in range(planes - 1):
        c_fold.push(t)
        s_fold.push(t)
    c_fold.total(c_sum)
    s_fold.total(s_sum)
    keep.wait()
    for mask in range(1, ranks):
        ref = w_sum.at[flip_mask(me, mask, bits)]
        pltpu.make_async_copy(ref, ref, a2a_r.at[mask]).wait()
    for mask in range(1, ranks):
        exchange(mask).wait_send()
    if fused:
        din = cols // 2
        for rank in range(ranks):
            for part in range(2):
                start = (part * ranks + rank) * din
                g_in[:, start : start + din] = w_sum[rank, :, part * din : (part + 1) * din].astype(f32)
        g_in[:, ranks * cols :] = c_sum[:, : g_in.shape[1] - ranks * cols]
    for ring in (dns, cs, ss, w_fold, c_fold, s_fold):
        ring.finish()


def reduce_all(fused, ranks, planes, rows, cols, width, small, tok, cot, gain, *operands):
    if fused:
        flipped, dproj, w_full = operands
        d, length = flipped.shape[0], dproj.shape[0] // ranks
        wide = w_full.shape[1] - cols
    else:
        dn, w, common = operands
        d, length, wide = dn.shape[-1], 2 * dn.shape[2], common.shape[-1]
    part = (2, length // 2, d)
    wshape = (planes, ranks, rows, cols)
    cshape = (ranks, 2, planes // 2, rows, wide)
    dma = pltpu.SemaphoreType.DMA
    vmem = pl.BlockSpec(memory_space=pltpu.VMEM)
    ring, line = 2 * (ranks - 1), 2 * planes
    sums = [((ranks, rows, cols), bf16), ((rows, wide), f32)]
    dn_sum, *weights, s_sum = pl.pallas_call(
        partial(reduce_kernel, fused),
        in_specs=[pl.BlockSpec(memory_space=pl.ANY)] + [vmem] * 3 + [pl.BlockSpec(memory_space=pl.ANY)] * 3,
        out_specs=[vmem] * (3 if fused else 4),
        out_shape=[jax.ShapeDtypeStruct(part, f32)]
        + [jax.ShapeDtypeStruct(*s) for s in ([((rows, width), f32)] if fused else sums)]
        + [jax.ShapeDtypeStruct(small.shape[3:], f32)],
        scratch_shapes=[
            pltpu.VMEM((ranks,) + part, bf16),
            pltpu.VMEM(wshape, bf16),
            pltpu.VMEM(cshape, bf16),
            pltpu.VMEM(small.shape, f32),
            pltpu.VMEM(wshape[1:], bf16),
            pltpu.VMEM((ring,) + part[1:], bf16),
            pltpu.VMEM((line,) + wshape[1:], bf16),
            pltpu.VMEM((ring,) + cshape[2:], bf16),
            pltpu.VMEM((ring,) + small.shape[2:], f32),
            pltpu.VMEM((line,) + cshape[3:], bf16),
            pltpu.VMEM((line,) + small.shape[3:], f32),
        ]
        + [dma((ring,))] * 6
        + [dma((line,))] * 6
        + [dma((ranks,)), dma((ranks,)), dma((4,))]
        + ([pltpu.VMEM(a.shape, bf16) for a in operands] + [pltpu.VMEM(*s) for s in sums] if fused else []),
        compiler_params=pltpu.CompilerParams(
            collective_id=1, has_side_effects=True, vmem_limit_bytes=67043328
        ),
        name="reduce_all",
    )(small, tok.reshape(part), cot.reshape(part), gain, *operands)
    return [dn_sum.reshape(length, d), s_sum] + weights


def dot(a, b, dims, precision=None):
    return lax.dot_general(
        a, b, (dims, ((), ())), preferred_element_type=f32, precision=precision
    )


NN, NT, TN = ((1,), (0,)), ((1,), (1,)), ((0,), (0,))


def sigmoid(a):
    return 0.5 * jnp.tanh(0.5 * a) + 0.5


def iota(shape, axis):
    return lax.broadcasted_iota(jnp.int32, shape, axis)


def parts(a):
    high = a.astype(bf16)
    return high, (a - high.astype(f32)).astype(bf16)


def fine(a, b, dims):
    left = jnp.concatenate([a[0], a[0], a[1]], axis=dims[0][0])
    right = jnp.concatenate([b[0], b[1], b[0]], axis=dims[1][0])
    return dot(left, right, dims)


def steps_of(raw, bias):
    shifted = raw + bias
    return jnp.maximum(shifted, 0.0) + jnp.log1p(jnp.exp(-jnp.abs(shifted)))


def convolve(pad, conv_ref, tile, count):
    total = conv_ref[CONVK : CONVK + 1, tile]
    for k in range(CONVK):
        total = total + pad[EDGE - CONVK + 1 + k : EDGE - CONVK + 1 + k + count, tile] * conv_ref[k : k + 1, tile]
    return total


class Chunk:
    def __init__(self, step, rate):
        n = SUB
        upper = jnp.where(iota((n, n), 0) <= iota((n, n), 1), 1.0, 0.0)
        self.step = step
        self.rows = dot(step * -rate, upper, NN, highest)
        self.cols = self.rows.T
        self.step_cols = step.T

    def col(self, h):
        return jnp.broadcast_to(self.cols[:, h : h + 1], (SUB, SUB))

    def decay(self, h, col, hide):
        return jnp.exp(col - self.rows[h : h + 1, :] + hide)

    def step_col(self, h):
        return jnp.broadcast_to(self.step_cols[:, h : h + 1], (SUB, SUB))


def fwd_kernel(
    proj_ref, raw_ref, cot_ref, wout_ref, conv_ref, lane_ref, head_ref,
    y_ref, dg_ref, out_ref, state_ref, sum_ref, gated,
    pad, act, carry,
):
    block = proj_ref.shape[0]
    din = y_ref.shape[1]
    conv = conv_ref.shape[1]

    @pl.when(pl.program_id(0) == 0)
    def _():
        carry[...] = jnp.zeros_like(carry)
        pad[0:EDGE, :] = jnp.zeros((EDGE, conv), f32)

    @pl.when(pl.program_id(0) > 0)
    def _():
        pad[0:EDGE, :] = pad[block : block + EDGE, :]

    for j in range(conv // LANES):
        tile = slice(j * LANES, (j + 1) * LANES)
        pad[EDGE:, tile] = proj_ref[:, din + j * LANES : din + (j + 1) * LANES].astype(f32)
        filtered = convolve(pad, conv_ref, tile, block)
        act[:, tile] = filtered * sigmoid(filtered)
    dg_ref[...] = dot(cot_ref[...], wout_ref[...], NT)

    low = iota((SUB, LANES), 1) < HDIM
    hide = jnp.where(iota((SUB, SUB), 0) >= iota((SUB, SUB), 1), 0.0, -1e30)
    for i in range(block // SUB):
        rows = slice(i * SUB, (i + 1) * SUB)
        b, c = parts(act[rows, din : din + NSTATE]), parts(act[rows, din + NSTATE :])
        chunk = Chunk(steps_of(raw_ref[:, rows], head_ref[1]), head_ref[0])
        scores = fine(c, b, NT)
        sq = jnp.zeros((SUB, LANES), f32)
        cross = jnp.zeros((SUB, LANES), f32)
        for j in range(din // LANES):
            tile = slice(j * LANES, (j + 1) * LANES)
            x = act[rows, tile]
            col0, col1 = chunk.col(2 * j), chunk.col(2 * j + 1)
            m0 = chunk.decay(2 * j, col0, hide) * scores
            m1 = chunk.decay(2 * j + 1, col1, hide) * scores
            cexp = jnp.where(low, col0, col1)
            xs = x * jnp.where(low, chunk.step_col(2 * j), chunk.step_col(2 * j + 1))
            zero = jnp.zeros_like(xs)
            split = jnp.concatenate([jnp.where(low, xs, zero), jnp.where(low, zero, xs)], axis=0)
            before = carry[:, tile]
            state_ref[i, :, tile] = before
            y = fine(parts(jnp.concatenate([m0, m1], axis=1)), parts(split), NN)
            y = y + fine(c, parts(before), NN) * jnp.exp(cexp)
            y_ref[rows, tile] = y
            last = cexp[SUB - 1 :, :]
            carry[:, tile] = before * jnp.exp(last) + fine(b, parts(xs * jnp.exp(last - cexp)), TN)
            z = proj_ref[rows, tile].astype(f32)
            v = (y + lane_ref[0:1, tile] * x) * (z * sigmoid(z))
            scaled = v * lane_ref[1:2, tile]
            gated[rows, tile] = scaled.astype(bf16)
            sq = sq + v * v
            cross = cross + scaled * dg_ref[rows, tile]
        ones = jnp.ones((4, LANES), f32)
        sum_ref[0:4, rows] = dot(ones, sq, NT, highest)
        sum_ref[4:8, rows] = dot(ones, cross, NT, highest)
    out_ref[...] = dot(gated[...], wout_ref[...], NN).astype(bf16)


def bwd_kernel(
    total_din, live,
    proj_ref, rim_ref, raw_ref, y_ref, dg_ref, sum_ref, state_ref, conv_ref, lane_ref, head_ref,
    out_in, o_in,
    dproj_ref, dconv_ref, dlane_ref, dhead_ref, out_sum, o_sum,
    pad, act, slope, dpad, carry, edge, dact,
    *links,
):
    side_reduce(out_in, o_in, out_sum, o_sum, *links)

    block = proj_ref.shape[0]
    din = y_ref.shape[1]
    conv = conv_ref.shape[1]
    step_id = pl.program_id(0)
    first = step_id == pl.num_programs(0) - 1

    @pl.when(step_id == 0)
    def _():
        carry[...] = jnp.zeros_like(carry)
        edge[...] = jnp.zeros_like(edge)
        dpad[0:EDGE, :] = jnp.zeros((EDGE, conv), f32)
        dconv_ref[...] = jnp.zeros_like(dconv_ref)
        dlane_ref[...] = jnp.zeros_like(dlane_ref)
        dhead_ref[...] = jnp.zeros_like(dhead_ref)

    dpad[block : block + EDGE, :] = dpad[0:EDGE, :]
    keep = jnp.where(first, 0.0, 1.0)
    for j in range(conv // LANES):
        tile = slice(j * LANES, (j + 1) * LANES)
        src = slice(din + j * LANES, din + (j + 1) * LANES)
        pad[0:EDGE, tile] = rim_ref[rim_ref.shape[0] - EDGE :, src].astype(f32) * keep
        pad[EDGE:, tile] = proj_ref[:, src].astype(f32)
        filtered = convolve(pad, conv_ref, tile, block)
        s = sigmoid(filtered)
        act[:, tile] = filtered * s
        slope[:, tile] = s * (1.0 + filtered * (1.0 - s))

    low = iota((SUB, LANES), 1) < HDIM
    hide = jnp.where(iota((SUB, SUB), 0) >= iota((SUB, SUB), 1), 0.0, -1e30)
    lower = jnp.where(iota((SUB, SUB), 0) >= iota((SUB, SUB), 1), 1.0, 0.0)
    heads = raw_ref.shape[0]
    row, lane = iota((heads, LANES), 0), iota((heads, LANES), 1)
    spot = jnp.where((row < live) & (lane == row + lax.axis_index("seq") * live), 1.0, 0.0).astype(bf16)
    dgain = [jnp.zeros((1, LANES), f32) for _ in range(din // LANES)]
    dskip = [jnp.zeros((1, LANES), f32) for _ in range(din // LANES)]
    for i in reversed(range(block // SUB)):
        rows = slice(i * SUB, (i + 1) * SUB)
        b_parts, c_parts = parts(act[rows, din : din + NSTATE]), parts(act[rows, din + NSTATE :])
        chunk = Chunk(steps_of(raw_ref[:, rows], head_ref[1]), head_ref[0])
        scores = fine(c_parts, b_parts, NT)
        sums = sum_ref[:, rows].T
        scale = lax.rsqrt(jnp.broadcast_to(sums[:, 0:1], (SUB, LANES)) * (1.0 / total_din) + epsilon)
        mean = jnp.broadcast_to(sums[:, 4:5], (SUB, LANES)) * (1.0 / total_din) * (scale * scale * scale)
        dscores = jnp.zeros((SUB, SUB), f32)
        d_b = jnp.zeros((SUB, NSTATE), f32)
        d_c = jnp.zeros((SUB, NSTATE), f32)
        d_cum = jnp.zeros((heads, SUB), f32)
        d_step = jnp.zeros((heads, SUB), f32)
        reach = jnp.zeros((heads, 8), f32)
        for j in range(din // LANES):
            tile = slice(j * LANES, (j + 1) * LANES)
            x = act[rows, tile]
            y = y_ref[rows, tile]
            skip, gain = lane_ref[0:1, tile], lane_ref[1:2, tile]
            z = proj_ref[rows, tile].astype(f32)
            sz = sigmoid(z)
            mixed = y + skip * x
            silu = z * sz
            v = mixed * silu
            dg = dg_ref[rows, tile]
            vs = v * scale
            dgain[j] = dgain[j] + jnp.sum(dg * vs, axis=0, keepdims=True)
            dv = scale * (gain * dg) - v * mean
            dy = dv * silu
            dproj_ref[rows, tile] = (dv * mixed * (sz * (1.0 + z * (1.0 - sz)))).astype(bf16)
            dskip[j] = dskip[j] + jnp.sum(dy * x, axis=0, keepdims=True)

            col0, col1 = chunk.col(2 * j), chunk.col(2 * j + 1)
            l0, l1 = chunk.decay(2 * j, col0, hide), chunk.decay(2 * j + 1, col1, hide)
            m = parts(jnp.concatenate([l0 * scores, l1 * scores], axis=0))
            cexp = jnp.where(low, col0, col1)
            step = jnp.where(low, chunk.step_col(2 * j), chunk.step_col(2 * j + 1))
            last = cexp[SUB - 1 :, :]
            grow, tail = jnp.exp(cexp), jnp.exp(last - cexp)
            xs = x * step
            zero = jnp.zeros_like(dy)
            dsplit = parts(jnp.concatenate([jnp.where(low, dy, zero), jnp.where(low, zero, dy)], axis=0))
            xs_parts = parts(xs)
            dm = fine(dsplit, xs_parts, NT)
            dscores = dscores + dm[:SUB] * l0 + dm[SUB:] * l1
            dend = carry[:, tile]
            dend_parts = parts(dend)
            before = state_ref[i, :, tile]
            dxs = fine(m, dsplit, TN) + fine(b_parts, dend_parts, NN) * tail
            grown = parts(dy * grow)
            d_c = d_c + fine(grown, parts(before), NT)
            d_b = d_b + fine(parts(xs * tail), dend_parts, NT)
            dprev = dend * jnp.exp(last) + fine(c_parts, grown, TN)
            carry[:, tile] = dprev
            pick = jnp.where(lax.shift_right_logical(iota((heads, LANES), 1), 6) + 2 * j == iota((heads, LANES), 0), 1.0, 0.0)
            balance = dy * y - xs * dxs
            d_cum = d_cum + dot(pick, balance, NT, highest)
            d_step = d_step + dot(pick, x * dxs, NT, highest)
            crossing = jnp.sum(dprev * before, axis=0, keepdims=True)
            reach = reach + dot(pick, jnp.broadcast_to(crossing, (8, LANES)), NT, highest)
            dact[rows, tile] = dxs * step + skip * dy
        ds_parts = parts(dscores)
        dact[rows, din : din + NSTATE] = d_b + fine(ds_parts, c_parts, TN)
        dact[rows, din + NSTATE :] = d_c + fine(ds_parts, b_parts, NN)
        d_log = dot(d_cum, lower, NN, highest) + edge[...]
        edge[...] = jnp.broadcast_to(reach[:, 0:1], edge.shape)
        raw = raw_ref[:, rows] + head_ref[1]
        draw = (d_step - head_ref[0] * d_log) * sigmoid(raw)
        dproj_ref[rows, din + conv :] = dot(draw.astype(bf16), spot, TN).astype(bf16)
        dhead_ref[0] += -chunk.step * d_log
        dhead_ref[1] += draw
    for j in range(din // LANES):
        tile = slice(j * LANES, (j + 1) * LANES)
        dlane_ref[0:1, tile] += dskip[j]
        dlane_ref[1:2, tile] += dgain[j]
    for j in range(conv // LANES):
        tile = slice(j * LANES, (j + 1) * LANES)
        df = dact[:, tile] * slope[:, tile]
        dpad[0:block, tile] = df
        dconv_ref[CONVK : CONVK + 1, tile] += jnp.sum(df, axis=0, keepdims=True)
        back = jnp.zeros((block, LANES), f32)
        for k in range(CONVK):
            shift = CONVK - 1 - k
            dconv_ref[k : k + 1, tile] += jnp.sum(
                df * pad[EDGE - shift : EDGE - shift + block, tile], axis=0, keepdims=True
            )
            back = back + conv_ref[k : k + 1, tile] * dpad[shift : shift + block, tile]
        dproj_ref[:, din + j * LANES : din + (j + 1) * LANES] = back.astype(bf16)


def rows_spec(block, width):
    return pl.BlockSpec((block, width), lambda t: (t, 0))


def whole(shape):
    return pl.BlockSpec(shape, lambda t: (0,) * len(shape))


def mixer_forward(proj, raw, cot, w_out, conv, lanes, heads):
    length, width = proj.shape
    din, d = w_out.shape
    cc = conv.shape[1]
    block = min(TOKENS, length)
    n = block // SUB
    cols = pl.BlockSpec((8, block), lambda t: (0, t))
    return pl.pallas_call(
        fwd_kernel,
        grid=(length // block,),
        in_specs=[
            rows_spec(block, width), cols, rows_spec(block, d), whole(w_out.shape),
            whole(conv.shape), whole(lanes.shape), whole(heads.shape),
        ],
        out_specs=[
            rows_spec(block, din), rows_spec(block, din), rows_spec(block, d),
            pl.BlockSpec((n, NSTATE, din), lambda t: (t, 0, 0)), cols, rows_spec(block, din),
        ],
        out_shape=[
            jax.ShapeDtypeStruct((length, din), f32),
            jax.ShapeDtypeStruct((length, din), f32),
            jax.ShapeDtypeStruct((length, d), bf16),
            jax.ShapeDtypeStruct((length // SUB, NSTATE, din), f32),
            jax.ShapeDtypeStruct((8, length), f32),
            jax.ShapeDtypeStruct((length, din), bf16),
        ],
        scratch_shapes=[
            pltpu.VMEM((block + EDGE, cc), f32),
            pltpu.VMEM((block, cc), f32),
            pltpu.VMEM((NSTATE, din), f32),
        ],
        name="mix_forward",
    )(proj, raw, cot, w_out, conv, lanes, heads)


def side_reduce(out_in, o_in, out_sum, o_sum, acc, land, stage, o_land, out_s, out_r, oz_s, oz_r, mix_s, mix_r, local):
    ranks, planes = acc.shape[0], stage.shape[0]
    me, dp = lax.axis_index("seq"), lax.axis_index("dp")
    outs = Collect(acc, land, out_s, out_r, 16)
    fold = Fold(lambda d: stage.at[d], o_land, planes, oz_s, oz_r, stage.shape[1])
    top = len(bits_of(ranks)) - 1
    load = pltpu.make_async_copy(out_in, acc, local.at[0])

    def move(k, act):
        index = me * planes + k
        plane, to = lax.div(index, ranks), index % ranks

        @pl.when(to != me)
        def _():
            copy = remote(o_in.at[k], stage.at[plane], mix_s.at[k], mix_r.at[plane], (dp, to))
            copy.start() if act else copy.wait_send()

        if act:
            @pl.when(to == me)
            def _():
                pltpu.make_async_copy(o_in.at[k], stage.at[plane], mix_r.at[plane]).start()

    def begin():
        load.start()
        greet(ranks, planes)
        for k in range(planes):
            move(k, True)
        load.wait()
        outs.push(top)

    def settle():
        for d in range(planes):
            pltpu.make_async_copy(stage.at[d], stage.at[d], mix_r.at[d]).wait()
        fold.push(0)

    def end():
        outs.total(out_sum)
        fold.total(o_sum)
        for k in range(planes):
            move(k, False)
        outs.finish()
        fold.finish()

    pushes = {4 * i + 1: partial(outs.push, top - 1 - i) for i in range(top)}
    folds = [settle] + [partial(fold.push, t) for t in range(1, planes - 1)]
    spare = [t for t in range(3, 64) if t not in pushes]
    stages = {0: begin, **pushes, **dict(zip(spare, folds))}
    last = pl.num_programs(0) - 1
    for k, run in sorted(stages.items()):
        pl.when(pl.program_id(0) == k)(run)
    pl.when(pl.program_id(0) == last)(end)


def mixer_backward(ranks, planes, total_din, proj, raw, y, dg, sums, states, conv, lanes, heads, live, out_part, d_w_out):
    length, width = proj.shape
    din, d = y.shape[1], out_part.shape[1]
    cc = conv.shape[1]
    block = min(TOKENS, length)
    n = block // SUB
    last = length // block - 1
    rim = 16
    assert last > max(4 * len(bits_of(ranks)) - 7, planes + 1 + (planes > 3))
    part = (2, length // ranks // 2, d)
    ring, line = 2 * (ranks - 1), 2 * planes
    dma = pltpu.SemaphoreType.DMA

    def back(block, width):
        return pl.BlockSpec((block, width), lambda t: (last - t, 0))

    cols = pl.BlockSpec((8, block), lambda t: (0, last - t))
    anywhere = pl.BlockSpec(memory_space=pl.ANY)
    *results, out_sum, o_sum = pl.pallas_call(
        partial(bwd_kernel, total_din, live),
        grid=(length // block,),
        in_specs=[
            back(block, width),
            pl.BlockSpec((rim, width), lambda t: (jnp.maximum((last - t) * (block // rim) - 1, 0), 0)),
            cols, back(block, din), back(block, din), cols,
            pl.BlockSpec((n, NSTATE, din), lambda t: (last - t, 0, 0)),
            whole(conv.shape), whole(lanes.shape), whole(heads.shape), anywhere, anywhere,
        ],
        out_specs=[
            back(block, width + LANES), whole((8, cc)), whole((8, din)), whole((2, 8, SUB)),
            whole(part), whole(d_w_out.shape[1:]),
        ],
        out_shape=[
            jax.ShapeDtypeStruct((length, width + LANES), bf16),
            jax.ShapeDtypeStruct((8, cc), f32),
            jax.ShapeDtypeStruct((8, din), f32),
            jax.ShapeDtypeStruct((2, 8, SUB), f32),
            jax.ShapeDtypeStruct(part, f32),
            jax.ShapeDtypeStruct(d_w_out.shape[1:], f32),
        ],
        scratch_shapes=[
            pltpu.VMEM((block + EDGE, cc), f32),
            pltpu.VMEM((block, cc), f32),
            pltpu.VMEM((block, cc), f32),
            pltpu.VMEM((block + EDGE, cc), f32),
            pltpu.VMEM((NSTATE, din), f32),
            pltpu.VMEM((8, SUB), f32),
            pltpu.VMEM((block, cc), f32),
            pltpu.VMEM((ranks,) + part, bf16),
            pltpu.VMEM((ring,) + part[1:], bf16),
            pltpu.VMEM(d_w_out.shape, bf16),
            pltpu.VMEM((line,) + d_w_out.shape[1:], bf16),
            dma((ring,)), dma((ring,)), dma((line,)), dma((line,)), dma((planes,)), dma((planes,)), dma((1,)),
        ],
        compiler_params=pltpu.CompilerParams(
            collective_id=3, has_side_effects=True, vmem_limit_bytes=67043328
        ),
        name="mix_backward",
    )(
        proj, proj, raw, y, dg, sums, states, conv, lanes, heads,
        out_part.reshape((ranks,) + part), d_w_out,
    )
    return results + [out_sum.reshape(length // ranks, d), o_sum]


def rms_scale(values, gain):
    mean_sq = jnp.mean(values * values, axis=-1, keepdims=True)
    return values * lax.rsqrt(mean_sq + epsilon) * gain


def widen(array, size, axis):
    pads = [(0, 0)] * array.ndim
    pads[axis] = (0, size - array.shape[axis])
    return jnp.pad(array, pads)


def per_device(
    tokens,
    cotangent,
    in_weight,
    out_weight,
    conv_weight,
    conv_bias,
    norm_gain,
    gate_gain,
    decay_rate,
    dt_bias,
    d_skip,
):
    ranks = lax.axis_size("seq")
    me = lax.axis_index("seq")
    both = ("dp", "seq")
    heads = decay_rate.shape[0] // ranks
    din = heads * HDIM
    padded = -(-din // LANES) * LANES
    din_all = din * ranks
    rows, width = in_weight.shape
    conv_all = din_all + 2 * NSTATE
    main = 2 * padded + 2 * NSTATE

    def mine(array, size, axis=0):
        return lax.dynamic_slice_in_dim(array, me * size, size, axis)

    planes = lax.axis_size("dp")
    x_own = tokens[0].astype(f32)
    send = jnp.concatenate(
        [
            widen(in_weight[:, :din_all].reshape(rows, ranks, din), padded, 2),
            widen(in_weight[:, din_all : 2 * din_all].reshape(rows, ranks, din), padded, 2),
        ],
        axis=2,
    ).transpose(1, 0, 2)
    d = in_weight.shape[0] * ranks * planes
    rank_id = lax.axis_index("dp") * ranks + me
    small = [norm_gain, gate_gain, conv_weight.reshape(-1), conv_bias]
    sizes = [a.shape[0] for a in small]
    room = rows * HDIM - d
    if room >= sum(sizes):
        placed = lax.dynamic_update_slice_in_dim(jnp.zeros((d,), bf16), norm_gain, rank_id * rows, 0)
        packed = jnp.concatenate([placed, widen(jnp.concatenate(small), room, 0)])
    else:
        packed = widen(jnp.concatenate(small), rows * HDIM, 0)
    common = jnp.concatenate(
        [
            in_weight[:, 2 * din_all : 2 * din_all + 2 * NSTATE],
            widen(in_weight[:, din_all + conv_all :], HDIM, 1),
            packed.reshape(rows, HDIM),
        ],
        axis=1,
    )
    cot, w_out, common, fused, *rest = gather_all(
        ranks, planes, tokens[0], cotangent[0], send, out_weight, common
    )
    w_out = widen(w_out, padded, 0)
    packed = common[..., 2 * NSTATE + HDIM :].reshape(ranks * planes, rows * HDIM).astype(f32)
    if room >= sum(sizes):
        packed = packed[:, d:]
    gain_norm, gain_gate, conv_w, conv_b = (
        packed[:, sum(sizes[:k]) : sum(sizes[: k + 1])].reshape(-1) for k in range(4)
    )
    conv_w = conv_w.reshape(-1, CONVK)
    taps = jnp.concatenate([conv_w.T, conv_b[None], jnp.zeros((8 - CONVK - 1, conv_all), f32)], axis=0)
    conv = jnp.concatenate([widen(mine(taps, din, 1), padded, 1), taps[:, din_all:]], axis=1)
    if fused:
        raw, flipped, proj, w_full = rest
    else:
        tok, w_all = rest
        w_full = jnp.concatenate([w_all, common.reshape(-1, common.shape[-1])], axis=1)
        normed = rms_scale(tok.astype(f32), gain_norm).astype(bf16)
        proj = dot(normed, w_full[:, :main], NN).astype(bf16)
        raw = dot(w_full[:, main : main + HDIM].T, normed, NT).astype(bf16).astype(f32)
    raw = widen(mine(raw, heads), 8, 0)
    rate, bias, skip = (mine(a, heads) for a in (decay_rate, dt_bias, d_skip))
    lanes = jnp.stack([jnp.repeat(skip, HDIM), mine(gain_gate, din)])
    lanes = widen(widen(lanes, padded, 1), 8, 0)
    head_rows = jnp.broadcast_to(widen(jnp.stack([rate, bias]), 8, 1)[:, :, None], (2, 8, SUB))

    y, dg, out_part, states, sums, gated = mixer_forward(proj, raw, cot, w_out, conv, lanes, head_rows)
    sums = plane_sum(ranks, sums[::4].reshape(8, -1)).reshape(2, -1)
    inverse = lax.rsqrt(sums[0] / din_all + epsilon)[:, None]
    d_w_out = dot((gated * inverse).astype(bf16), cot, TN)[:din].astype(bf16)
    d_proj, d_conv, d_lane, d_head, out_sum, grad_out = mixer_backward(
        ranks, planes, din_all, proj, raw, y, dg, jnp.repeat(sums, 4, axis=0), states, conv, lanes, head_rows,
        heads, out_part, d_w_out.reshape(planes, -1, d),
    )

    def by_owner(array):
        split = array.reshape((2, planes // 2, ranks) + array.shape[1:])
        return split.transpose((2, 0, 1) + tuple(range(3, split.ndim)))

    def place(own, size):
        return lax.dynamic_update_slice_in_dim(
            jnp.zeros((size * ranks,) + own.shape[1:], f32), own, me * size, 0
        )

    d_cw, d_cb = d_conv[:CONVK].T, d_conv[CONVK]
    full_cw = jnp.concatenate([place(d_cw[:din], din), d_cw[padded:]], axis=0)
    full_cb = jnp.concatenate([place(d_cb[:din], din), d_cb[padded:]], axis=0)
    d_skp = jnp.sum(d_lane[0, :din].reshape(heads, HDIM), axis=1)
    d_rate, d_bias = jnp.sum(d_head, axis=2)[:, :heads]
    devices = planes * ranks
    head_part = jnp.concatenate([place(a, heads) for a in (d_rate, d_bias, d_skp)])
    fields = [
        a.reshape(devices, -1) for a in (full_cw, full_cb, place(d_lane[1, :din], din))
    ] + [jnp.broadcast_to(head_part, (devices,) + head_part.shape)]
    ends = [0]
    for a in fields:
        ends.append(ends[-1] + a.shape[1])
    small = widen(jnp.concatenate(fields, axis=1), 8 * LANES, 1).reshape(devices, 8, LANES)
    if fused:
        operands = flipped, d_proj, w_full
    else:
        d_w = dot(normed, d_proj, TN).astype(bf16)
        part = dot(d_proj, w_full, NT).astype(bf16)
        operands = (
            part.reshape(ranks, 2, -1, d),
            d_w[:, : 2 * padded].reshape(planes, ranks, rows, -1),
            by_owner(d_w[:, 2 * padded :].reshape(planes * ranks, rows, -1)),
        )
    grad_x, small_sum, *sums_in = reduce_all(
        fused, ranks, planes, rows, 2 * padded, width, by_owner(small), tokens[0], cotangent[0],
        gain_norm[None], *operands,
    )
    block_out = (x_own + mine(inverse, x_own.shape[0]) * out_sum).astype(bf16)
    if fused:
        (grad_in,) = sums_in
    else:
        w_sum, bc_sum = sums_in
        spread = w_sum.astype(f32).transpose(1, 0, 2)
        grad_in = jnp.concatenate(
            [
                spread[:, :, :din].reshape(rows, din_all),
                spread[:, :, padded : padded + din].reshape(rows, din_all),
                bc_sum[:, : 2 * NSTATE + heads * ranks],
            ],
            axis=1,
        )
    g_gain = jnp.sum(grad_in * in_weight.astype(f32), axis=1) / norm_gain.astype(f32)
    small_sum = small_sum.reshape(-1)
    g_cw, g_cb, g_gate, head_sums = (small_sum[a:b] for a, b in zip(ends[:-1], ends[1:]))
    g_cw = g_cw.reshape(-1, CONVK)
    head_sums = head_sums.reshape(3, -1)
    return (
        block_out[None],
        grad_x[None],
        grad_in,
        grad_out,
        g_cw,
        g_cb,
        g_gain,
        g_gate,
        head_sums[0],
        head_sums[1],
        head_sums[2],
    )


def solution(mesh):
    rows = P(("dp", "seq"), None)
    flat = P(("dp", "seq"))
    act = P("dp", "seq", None)
    return jax.shard_map(
        per_device,
        mesh=mesh,
        in_specs=(act, act, rows, rows, rows, flat, flat, flat, P(), P(), P()),
        out_specs=(act, act, rows, rows, rows, flat, flat, flat, P(), P(), P()),
        check_vma=False,
    )
```

```python
from functools import partial

import jax
import jax.numpy as jnp
from jax import lax
from jax.experimental import pallas as pl
from jax.experimental.pallas import tpu as pltpu
from jax.sharding import PartitionSpec as P

HDIM = 64
NSTATE = 128
CONVK = 4
LANES = 128
SUB = 128
TOKENS = 256
EDGE = 8

epsilon = 1e-05
highest = lax.Precision.HIGHEST
bf16 = jnp.bfloat16
f32 = jnp.float32


MESH = pl.DeviceIdType.MESH


def flip(index, bit):
    return index + bit * (1 - 2 * (lax.div(index, bit) % 2))


def flip_mask(index, mask, bits):
    for bit in bits:
        if mask & bit:
            index = flip(index, bit)
    return index


def bits_of(size):
    return [1 << k for k in range(size.bit_length() - 1)]


def both_orders(size):
    bits = bits_of(size)
    slow = bits[1:]
    return [slow + bits[:1], slow[::-1] + bits[:1]]


def remote(src, dst, send, recv, to):
    return pltpu.make_async_remote_copy(
        src_ref=src, dst_ref=dst, send_sem=send, recv_sem=recv, device_id=to, device_id_type=MESH
    )


class Spread:
    def __init__(self, buf, send, recv, own=None):
        self.size = buf.shape[0]
        self.bits = bits_of(self.size)
        self.orders = both_orders(self.size)
        self.buf, self.send, self.recv = buf, send, recv
        self.me, self.dp = lax.axis_index("seq"), lax.axis_index("dp")
        self.own = own

    def masks(self, half):
        order = self.orders[half]
        got = [0]
        for bit in order:
            got = got + [m | bit for m in got]
        return got

    def copy(self, half, mask, bit):
        origin = flip_mask(self.me, mask, self.bits)
        dst = self.buf.at[origin, half]
        src = self.own.at[half] if (mask == 0 and self.own is not None) else dst
        slot = half * self.size + (mask | bit)
        return remote(src, dst, self.send.at[slot], self.recv.at[slot], (self.dp, flip(self.me, bit)))

    def start(self, half, mask):
        order = self.orders[half]
        after = max((order.index(b) for b in self.bits if mask & b), default=-1) + 1
        for bit in order[after:]:
            self.copy(half, mask, bit).start()

    def arrive(self, half, mask):
        order = self.orders[half]
        top = order[max(order.index(b) for b in self.bits if mask & b)]
        self.copy(half, mask & ~top, top).wait_recv()

    def forward(self, group):
        for k in range(1 << group, 2 << group):
            for half in range(2):
                mask = self.masks(half)[k]
                self.arrive(half, mask)
                self.start(half, mask)

    def finish(self):
        for half in range(2):
            for mask in range(1, self.size):
                order = self.orders[half]
                top = order[max(order.index(b) for b in self.bits if mask & b)]
                self.copy(half, mask & ~top, top).wait_send()

    @property
    def groups(self):
        return len(self.bits)


class Line:
    def __init__(self, at, size, send, recv):
        self.at, self.size, self.send, self.recv = at, size, send, recv
        self.me, self.seq = lax.axis_index("dp"), lax.axis_index("seq")

    def copy(self, way, hop):
        block = self.me - way * (hop - 1)
        slot = (self.size if way > 0 else 0) + hop
        ref = self.at(block)
        return remote(ref, ref, self.send.at[slot], self.recv.at[slot], (self.me + way, self.seq))

    def sends(self, way, hop):
        block = self.me - way * (hop - 1)
        to = self.me + way
        return (block >= 0) & (block < self.size) & (to >= 0) & (to < self.size)

    def start(self, hop):
        for way in (1, -1):
            @pl.when(self.sends(way, hop))
            def _():
                self.copy(way, hop).start()

    def arrive(self, hop):
        for way in (1, -1):
            source = self.me - way * hop
            @pl.when((source >= 0) & (source < self.size))
            def _():
                ref = self.at(source)
                slot = (self.size if way > 0 else 0) + hop
                pltpu.make_async_copy(ref, ref, self.recv.at[slot]).wait()

    def forward(self, hop):
        self.arrive(hop)
        if hop + 1 < self.size:
            self.start(hop + 1)

    def finish(self):
        for hop in range(1, self.size):
            for way in (1, -1):
                @pl.when(self.sends(way, hop))
                def _():
                    self.copy(way, hop).wait_send()


def greet(ranks, planes):
    me, dp = lax.axis_index("seq"), lax.axis_index("dp")
    barrier = pltpu.get_barrier_semaphore()
    for mask in range(1, ranks):
        pl.semaphore_signal(
            barrier, inc=1, device_id=(dp, flip_mask(me, mask, bits_of(ranks))), device_id_type=MESH
        )
    for way in (1, -1):
        @pl.when((dp + way >= 0) & (dp + way < planes))
        def _():
            pl.semaphore_signal(barrier, inc=1, device_id=(dp + way, me), device_id_type=MESH)
    near = jnp.where(dp > 0, 1, 0) + jnp.where(dp < planes - 1, 1, 0)
    pl.semaphore_wait(barrier, ranks - 1 + near)


def norm_tokens(tok, common, normed, rows, w_full):
    ranks, planes = tok.shape[0], 2 * common.shape[2]
    width = w_full.shape[1] - common.shape[-1]
    strip, tile = 32, tok.shape[2]
    d = tok.shape[3]
    half = planes // 2

    def lay(i, gains):
        at = pl.ds(pl.multiple_of(i * rows, 16), rows)
        plane, rank = lax.div(i, ranks), i % ranks
        shared = common[rank, lax.div(plane, half), plane % half]
        w_full[at, width:] = shared
        return gains + shared[: d // HDIM, 2 * NSTATE :].astype(f32)

    gains = lax.fori_loop(0, planes * ranks, lay, jnp.zeros((d // HDIM, LANES), f32))
    moved = pltpu.roll(gains, HDIM, 1)
    low = iota((1, LANES), 1) < HDIM
    gain = [jnp.where(low, moved[2 * j : 2 * j + 1], gains[2 * j + 1 : 2 * j + 2]) for j in range(d // LANES)]

    def norm(i, _):
        per = tile // strip
        part = lax.div(i, per)
        at = pl.ds(pl.multiple_of((i % per) * strip, strip), strip)
        x = tok.at[lax.div(part, 2), part % 2][at, :].astype(f32)
        scale = lax.rsqrt(jnp.sum(x * x, axis=1, keepdims=True) * (1.0 / d) + epsilon)
        to = pl.ds(pl.multiple_of(i * strip, strip), strip)
        for j in range(d // LANES):
            cut = slice(j * LANES, (j + 1) * LANES)
            normed[to, cut] = (x[:, cut] * scale * gain[j]).astype(bf16)
        return 0

    lax.fori_loop(0, ranks * 2 * tile // strip, norm, 0)


def stored(i, flipped, proj, flip_out, proj_out, store):
    at = pl.ds(pl.multiple_of(i * 256, 256), 256)
    return (
        pltpu.make_async_copy(proj.at[at, :], proj_out.at[at, :], store.at[0, i]),
        pltpu.make_async_copy(flipped.at[:, at], flip_out.at[:, at], store.at[1, i]),
    )


def project(w, normed, flipped, proj, raw, w_full, flip_out, proj_out, store):
    planes, ranks, rows, width = w.shape
    total, d = normed.shape
    main = width + 2 * NSTATE

    def lay(i, _):
        at = pl.ds(pl.multiple_of(i * rows, 16), rows)
        w_full[at, :width] = w[lax.div(i, ranks), i % ranks]
        return 0

    lax.fori_loop(0, planes * ranks, lay, 0)

    def multiply(i, _):
        at = pl.ds(pl.multiple_of(i * 256, 256), 256)
        for start in range(0, main, 512):
            cut = slice(start, min(start + 512, main))
            proj[at, cut] = dot(normed[at, :], w_full[:, cut], NN).astype(bf16)
        for k in range(2):
            to = pl.ds(pl.multiple_of(i * 256 + k * LANES, LANES), LANES)
            for j in range(d // LANES):
                tokens = normed[to, j * LANES : (j + 1) * LANES].astype(f32)
                flipped[j * LANES : (j + 1) * LANES, to] = tokens.T.astype(bf16)
        steps = dot(normed[at, :], w_full[:, main:], NN).astype(bf16).astype(f32)
        for k in range(2):
            to = pl.ds(pl.multiple_of(i * 256 + k * LANES, LANES), LANES)
            raw[:, to] = steps[k * LANES : (k + 1) * LANES].T[: raw.shape[0]]
        for copy in stored(i, flipped, proj, flip_out, proj_out, store):
            copy.start()
        return 0

    lax.fori_loop(0, total // 256, multiply, 0)


def gather_kernel(
    fused, tok_in, cot_in, w_in, wout_in, common_in,
    cot, wout, common, *rest,
):
    if fused:
        raw, flip_out, proj_out, full_out, tok, w, normed, flipped, proj, w_full, store, *rest = rest
    else:
        tok, w, *rest = rest
    (stage, tok_s, tok_r, cot_s, cot_r, com_s, com_r, wz_s, wz_r, oz_s, oz_r, cz_s, cz_r,
    a2a_s, a2a_r, mix_s, mix_r, local) = rest
    ranks, planes = tok.shape[0], w.shape[0]
    me, dp = lax.axis_index("seq"), lax.axis_index("dp")
    bits = bits_of(ranks)
    greet(ranks, planes)
    half = planes // 2
    tokens = Spread(tok, tok_s, tok_r, tok_in)
    cots = Spread(cot, cot_s, cot_r, cot_in)
    commons = Spread(common, com_s, com_r)
    w_line = Line(lambda d: w.at[d], planes, wz_s, wz_r)
    o_line = Line(lambda d: stage.at[d], planes, oz_s, oz_r)
    c_line = Line(lambda d: common.at[me, lax.div(d, half), d % half], planes, cz_s, cz_r)

    def exchange(mask):
        peer = flip_mask(me, mask, bits)
        return remote(w_in.at[peer], w.at[dp, me], a2a_s.at[mask], a2a_r.at[mask], (dp, peer))

    def arrived(mask):
        ref = w.at[dp, flip_mask(me, mask, bits)]
        return pltpu.make_async_copy(ref, ref, a2a_r.at[mask])

    for mask in range(1, ranks):
        exchange(mask).start()
    places = [
        pltpu.make_async_copy(w_in.at[me], w.at[dp, me], local.at[0]),
        pltpu.make_async_copy(common_in, common.at[me, lax.div(dp, half), dp % half], local.at[1]),
        pltpu.make_async_copy(wout_in, stage.at[dp], local.at[2]),
        pltpu.make_async_copy(tok_in, tok.at[me], local.at[3]),
        pltpu.make_async_copy(cot_in, cot.at[me], local.at[4]),
    ]
    for place in places:
        place.start()
    for h in range(2):
        tokens.start(h, 0)
    for place in places:
        place.wait()
    c_line.start(1)
    for hop in range(1, planes):
        c_line.forward(hop)
    for mask in range(1, ranks):
        arrived(mask).wait()
    w_line.start(1)
    o_line.start(1)
    tokens.forward(0)
    for h in range(2):
        commons.start(h, 0)
    for h in range(2):
        cots.start(h, 0)
    w_line.forward(1)
    o_line.forward(1)
    for group in range(1, tokens.groups - 1):
        tokens.forward(group)
    for hop in range(2, planes - 1):
        o_line.forward(hop)
    for group in range(commons.groups - 1):
        commons.forward(group)
    for hop in range(2, planes - 1):
        w_line.forward(hop)
    tokens.forward(tokens.groups - 1)
    commons.forward(commons.groups - 1)
    if fused:
        norm_tokens(tok, common, normed, w.shape[2], w_full)
    cots.forward(0)
    o_line.forward(planes - 1)

    def moved(d):
        index = d * ranks + me
        return lax.div(index, planes), index % planes

    for d in range(planes):
        to, place = moved(d)

        @pl.when(to == me)
        def _():
            pltpu.make_async_copy(stage.at[d], wout.at[place], mix_r.at[place]).start()

        @pl.when(to != me)
        def _():
            remote(stage.at[d], wout.at[place], mix_s.at[d], mix_r.at[place], (dp, to)).start()

    w_line.forward(planes - 1)
    if fused:
        project(w, normed, flipped, proj, raw, w_full, flip_out, proj_out, store)
        full = pltpu.make_async_copy(w_full, full_out, local.at[0])
        full.start()
    for group in range(1, cots.groups):
        cots.forward(group)
    for place in range(planes):
        pltpu.make_async_copy(wout.at[place], wout.at[place], mix_r.at[place]).wait()
    for d in range(planes):
        to, place = moved(d)

        @pl.when(to != me)
        def _():
            remote(stage.at[d], wout.at[place], mix_s.at[d], mix_r.at[place], (dp, to)).wait_send()

    for mask in range(1, ranks):
        exchange(mask).wait_send()
    for ring in (tokens, cots, commons, w_line, o_line, c_line):
        ring.finish()
    if fused:
        full.wait()
        for i in range(store.shape[1]):
            for copy in stored(i, flipped, proj, flip_out, proj_out, store):
                copy.wait()


def gather_all(ranks, planes, tok, cot, w, w_out, common):
    length, d = tok.shape
    halves = (2, length // 2, d)
    total = ranks * length
    rows, cols = w.shape[1:]
    fused = rows % 16 == 0 and rows * HDIM >= 2 * d and length % 256 == 0 and cols % 768 == 0
    dma = pltpu.SemaphoreType.DMA
    vmem = pl.BlockSpec(memory_space=pltpu.VMEM)
    ring, line = 2 * ranks, 2 * planes
    anywhere = pl.BlockSpec(memory_space=pl.ANY)
    buffers = [((ranks,) + halves, bf16), ((planes,) + w.shape, bf16)]
    out = [
        ((ranks,) + halves, bf16), ((planes,) + w_out.shape, bf16), ((ranks, 2, planes // 2) + common.shape, bf16)
    ]
    places = [vmem, vmem, vmem]
    stores = []
    if fused:
        own = [((d, total), bf16), ((total, cols + 2 * NSTATE), bf16), ((d, cols + common.shape[1]), bf16)]
        out += [((HDIM, total), f32)] + own
        places += [vmem, anywhere, anywhere, anywhere]
        stores = [pltpu.VMEM(*s) for s in buffers + [((total, d), bf16)] + own] + [dma((2, total // 256))]
    else:
        out += buffers
        places += [vmem, vmem]
    cot_all, out_all, common_all, *rest = pl.pallas_call(
        partial(gather_kernel, fused),
        in_specs=[anywhere] * 5,
        out_specs=places,
        out_shape=[jax.ShapeDtypeStruct(*s) for s in out],
        scratch_shapes=stores
        + [pltpu.VMEM((planes,) + w_out.shape, bf16)]
        + [dma((ring,))] * 6
        + [dma((line,))] * 6
        + [dma((ranks,)), dma((ranks,)), dma((planes,)), dma((planes,)), dma((5,))],
        compiler_params=pltpu.CompilerParams(
            collective_id=0, has_side_effects=True, vmem_limit_bytes=67043328
        ),
        name="gather_all",
    )(tok.reshape(halves), cot.reshape(halves), w, w_out, common)
    common_all = common_all.reshape((ranks, planes) + common.shape).transpose(1, 0, 2, 3)
    cot_all, out_all = cot_all.reshape(total, d), out_all.reshape(planes * w_out.shape[0], d)
    if fused:
        return (cot_all, out_all, common_all, True) + tuple(rest)
    tok_all, w_all = rest
    return cot_all, out_all, common_all, False, tok_all.reshape(total, d), w_all.reshape(-1, cols)


def plane_sum_kernel(x_in, total, land, send, recv):
    ranks = land.shape[0]
    me, dp = lax.axis_index("seq"), lax.axis_index("dp")
    bits = bits_of(ranks)
    barrier = pltpu.get_barrier_semaphore()
    for mask in range(1, ranks):
        pl.semaphore_signal(barrier, inc=1, device_id=(dp, flip_mask(me, mask, bits)), device_id_type=MESH)
    pl.semaphore_wait(barrier, ranks - 1)

    def copy(mask):
        return remote(x_in, land.at[mask], send.at[mask], recv.at[mask], (dp, flip_mask(me, mask, bits)))

    for mask in range(1, ranks):
        copy(mask).start()
    value = x_in[...]
    for mask in range(1, ranks):
        copy(mask).wait_recv()
        value = value + land[mask]
    total[...] = value
    for mask in range(1, ranks):
        copy(mask).wait_send()


def plane_sum(ranks, x):
    vmem = pl.BlockSpec(memory_space=pltpu.VMEM)
    return pl.pallas_call(
        plane_sum_kernel,
        in_specs=[vmem],
        out_specs=vmem,
        out_shape=jax.ShapeDtypeStruct(x.shape, f32),
        scratch_shapes=[pltpu.VMEM((ranks,) + x.shape, f32)] + [pltpu.SemaphoreType.DMA((ranks,))] * 2,
        compiler_params=pltpu.CompilerParams(collective_id=2, has_side_effects=True),
        name="plane_sum",
    )(x)


def add_into(dst, pieces, rows):
    count = dst.shape[-2]
    rows = 16 if count % 16 == 0 else count

    def body(i, _):
        at = pl.ds(pl.multiple_of(i * rows, rows), rows)
        total = pieces[0][at, :].astype(f32)
        for piece in pieces[1:]:
            total = total + piece[at, :].astype(f32)
        dst[at, :] = total.astype(dst.dtype)
        return 0

    lax.fori_loop(0, count // rows, body, 0)


def flat_views(ref):
    if len(ref.shape) == 2:
        return [ref]
    return [view for k in range(ref.shape[0]) for view in flat_views(ref.at[k])]


def add_all(dst, pieces, rows):
    for views in zip(flat_views(dst), *(flat_views(p) for p in pieces)):
        add_into(views[0], views[1:], rows)


class Collect:
    def __init__(self, acc, land, send, recv, rows):
        self.size = acc.shape[0]
        self.bits = bits_of(self.size)
        self.orders = both_orders(self.size)
        self.acc, self.land, self.send, self.recv, self.rows = acc, land, send, recv, rows
        self.me, self.dp = lax.axis_index("seq"), lax.axis_index("dp")

    def copy(self, half, mask, bit):
        slot = half * (self.size - 1) + (mask | bit) - 1
        owner = flip_mask(self.me, mask | bit, self.bits)
        return remote(
            self.acc.at[owner, half], self.land.at[slot], self.send.at[slot], self.recv.at[slot],
            (self.dp, flip(self.me, bit)),
        )

    def subsets(self, bits):
        got = [0]
        for bit in bits:
            got = got + [m | bit for m in got]
        return got

    def arrivals(self, half, mask, after):
        pieces = []
        for bit in self.orders[half][after:]:
            slot = half * (self.size - 1) + (mask | bit) - 1
            pltpu.make_async_copy(self.land.at[slot], self.land.at[slot], self.recv.at[slot]).wait()
            pieces.append(self.land.at[slot])
        return pieces

    def push(self, k):
        for half in range(2):
            order = self.orders[half]
            for mask in self.subsets(order[:k]):
                full = mask | order[k]
                pieces = self.arrivals(half, full, k + 1)
                if pieces:
                    ref = self.acc.at[flip_mask(self.me, full, self.bits), half]
                    add_all(ref, [ref] + pieces, self.rows)
                self.copy(half, mask, order[k]).start()

    def total(self, dst):
        for half in range(2):
            pieces = self.arrivals(half, 0, 0)
            add_all(dst.at[half], [self.acc.at[self.me, half]] + pieces, self.rows)

    def finish(self):
        for half in range(2):
            order = self.orders[half]
            for k in range(len(order)):
                for mask in self.subsets(order[:k]):
                    self.copy(half, mask, order[k]).wait_send()


class Fold:
    def __init__(self, at, land, size, send, recv, rows):
        self.at, self.land, self.size, self.send, self.recv, self.rows = at, land, size, send, recv, rows
        self.me, self.seq = lax.axis_index("dp"), lax.axis_index("seq")

    def copy(self, way, block):
        slot = (self.size if way > 0 else 0) + block
        return remote(
            self.at(block), self.land.at[slot], self.send.at[slot], self.recv.at[slot], (self.me + way, self.seq)
        )

    def landed(self, way, block):
        slot = (self.size if way > 0 else 0) + block
        ref = self.land.at[slot]
        pltpu.make_async_copy(ref, ref, self.recv.at[slot]).wait()
        return ref

    def sends(self, way, block):
        return block > self.me if way > 0 else block < self.me

    def push(self, t):
        last = self.size - 1
        for way, block in ((1, last + self.me - t), (-1, t - last + self.me)):
            @pl.when((block >= 0) & (block <= last))
            def _():
                behind = self.me - way

                @pl.when((behind >= 0) & (behind < self.size))
                def _():
                    add_all(self.at(block), [self.at(block), self.landed(way, block)], self.rows)

                self.copy(way, block).start()

    def total(self, dst):
        me = self.me
        add_all(dst, [self.at(me)], self.rows)
        for way in (1, -1):
            behind = me - way

            @pl.when((behind >= 0) & (behind < self.size))
            def _():
                add_all(dst, [dst, self.landed(way, me)], self.rows)

    def finish(self):
        for t in range(self.size):
            for way in (1, -1):
                @pl.when(self.sends(way, t))
                def _():
                    self.copy(way, t).wait_send()


def input_grad(dn, tok, cot, gain):
    count, d = dn.shape[1:]

    for h in range(dn.shape[0]):
        def body(i, _):
            at = pl.ds(pl.multiple_of(i * 16, 16), 16)
            x = tok[h, at, :].astype(f32)
            g = gain[...] * dn[h, at, :]
            inv = lax.rsqrt(jnp.sum(x * x, axis=1, keepdims=True) * (1.0 / d) + epsilon)
            along = jnp.sum(g * x, axis=1, keepdims=True) * (1.0 / d)
            dn[h, at, :] = cot[h, at, :].astype(f32) + inv * (g - x * (inv * inv * along))
            return 0

        lax.fori_loop(0, count // 16, body, 0)


def reduce_kernel(fused, s_in, tok_own, cot_own, gain_in, *refs):
    if fused:
        flip_in, dproj_in, wfull_in, *refs = refs
    else:
        dn_in, w_in, c_in, *refs = refs
    if fused:
        dn_sum, g_in, s_sum, *refs = refs
    else:
        dn_sum, w_sum, c_sum, s_sum, *refs = refs
    (dn_acc, w_acc, c_acc, s_acc, own,
     dn_land, w_land, c_land, s_land, cz_land, sz_land,
     dn_s, dn_r, cr_s, cr_r, sr_s, sr_r, wz_s, wz_r, cz_s, cz_r, sz_s, sz_r, a2a_s, a2a_r, local, *refs) = refs
    ranks, planes = dn_acc.shape[0], w_acc.shape[0]
    me, dp = lax.axis_index("seq"), lax.axis_index("dp")
    bits = bits_of(ranks)
    half = planes // 2
    top = len(bits) - 1
    rows, cols = w_acc.shape[2:]
    tokens = dn_acc.shape[2]
    if fused:
        flipped, dproj, w_full, w_sum, c_sum = refs
        pairs = [(flip_in, flipped), (dproj_in, dproj), (s_in, s_acc), (wfull_in, w_full)]
    else:
        pairs = [(w_in, w_acc), (c_in, c_acc), (s_in, s_acc), (dn_in, dn_acc)]
    loads = [pltpu.make_async_copy(src, dst, local.at[k]) for k, (src, dst) in enumerate(pairs)]
    for load in loads:
        load.start()
    greet(ranks, planes)
    dns = Collect(dn_acc, dn_land, dn_s, dn_r, 16)
    cs = Collect(c_acc, c_land, cr_s, cr_r, c_acc.shape[-2])
    ss = Collect(s_acc, s_land, sr_s, sr_r, 8)

    def own_c(d):
        return c_acc.at[me, lax.div(d, half), d % half]

    def own_s(d):
        return s_acc.at[me, lax.div(d, half), d % half]

    w_fold = Fold(lambda d: w_acc.at[d], w_land, planes, wz_s, wz_r, rows)
    c_fold = Fold(own_c, cz_land, planes, cz_s, cz_r, c_acc.shape[-2])
    s_fold = Fold(own_s, sz_land, planes, sz_s, sz_r, 8)

    def weight_rows(plane):
        left = pl.ds(plane * ranks * rows, ranks * rows)
        for start in range(0, dproj.shape[1], 384):
            cut = slice(start, start + 384)
            block = dot(flipped[left, :], dproj[:, cut], NN).astype(bf16)
            for rank in range(ranks):
                piece = block[rank * rows : (rank + 1) * rows]
                if start < cols:
                    w_acc[plane, rank, :, cut] = piece
                else:
                    c_acc[rank, plane // half, plane % half, :, start - cols : start - cols + 384] = piece

    def token_half(far):
        mine = me % 2

        def body(i, _):
            rank = 2 * i + (1 - mine if far else mine)
            at = pl.ds(pl.multiple_of(2 * rank * tokens, 16), 2 * tokens)
            for start in range(0, w_full.shape[0], 512):
                cut = slice(start, start + 512)
                block = dot(dproj[at, :], w_full[cut, :], NT).astype(bf16)
                for h in range(2):
                    dn_acc[rank, h, :, cut] = block[h * tokens : (h + 1) * tokens]
            return 0

        lax.fori_loop(0, ranks // 2, body, 0)

    order = []
    for t in range(half):
        order.append((planes - 1 - t, t))
    if fused:
        for load in loads:
            load.wait()
        for plane in order[0]:
            weight_rows(plane)
        w_fold.push(0)
        token_half(True)
        dns.push(top)
        ss.push(top)
        for pair in order[1:]:
            for plane in pair:
                weight_rows(plane)
        cs.push(top)
        token_half(False)
    else:
        for load in loads:
            load.wait()
        w_fold.push(0)
        dns.push(top)
        cs.push(top)
        ss.push(top)
    for k in reversed(range(1, top)):
        for ring in (dns, ss, cs):
            ring.push(k)
    w_fold.push(1)
    for ring in (dns, ss, cs):
        ring.push(0)
    for t in range(2, planes - 1):
        w_fold.push(t)
    dns.total(dn_sum)
    input_grad(dn_sum, tok_own, cot_own, gain_in)
    for h in range(2):
        for ring in (ss, cs):
            pieces = ring.arrivals(h, 0, 0)
            ref = ring.acc.at[me, h]
            add_all(ref, [ref] + pieces, ring.rows)
    w_fold.total(own)

    def exchange(mask):
        peer = flip_mask(me, mask, bits)
        return remote(own.at[peer], w_sum.at[me], a2a_s.at[mask], a2a_r.at[mask], (dp, peer))

    for mask in range(1, ranks):
        exchange(mask).start()
    keep = pltpu.make_async_copy(own.at[me], w_sum.at[me], local.at[0])
    keep.start()
    for t in range(planes - 1):
        c_fold.push(t)
        s_fold.push(t)
    c_fold.total(c_sum)
    s_fold.total(s_sum)
    keep.wait()
    for mask in range(1, ranks):
        ref = w_sum.at[flip_mask(me, mask, bits)]
        pltpu.make_async_copy(ref, ref, a2a_r.at[mask]).wait()
    for mask in range(1, ranks):
        exchange(mask).wait_send()
    if fused:
        din = cols // 2
        for rank in range(ranks):
            for part in range(2):
                start = (part * ranks + rank) * din
                g_in[:, start : start + din] = w_sum[rank, :, part * din : (part + 1) * din].astype(f32)
        g_in[:, ranks * cols :] = c_sum[:, : g_in.shape[1] - ranks * cols]
    for ring in (dns, cs, ss, w_fold, c_fold, s_fold):
        ring.finish()


def reduce_all(fused, ranks, planes, rows, cols, width, small, tok, cot, gain, *operands):
    if fused:
        flipped, dproj, w_full = operands
        d, length = flipped.shape[0], dproj.shape[0] // ranks
        wide = w_full.shape[1] - cols
    else:
        dn, w, common = operands
        d, length, wide = dn.shape[-1], 2 * dn.shape[2], common.shape[-1]
    part = (2, length // 2, d)
    wshape = (planes, ranks, rows, cols)
    cshape = (ranks, 2, planes // 2, rows, wide)
    dma = pltpu.SemaphoreType.DMA
    vmem = pl.BlockSpec(memory_space=pltpu.VMEM)
    ring, line = 2 * (ranks - 1), 2 * planes
    sums = [((ranks, rows, cols), bf16), ((rows, wide), f32)]
    dn_sum, *weights, s_sum = pl.pallas_call(
        partial(reduce_kernel, fused),
        in_specs=[pl.BlockSpec(memory_space=pl.ANY)] + [vmem] * 3 + [pl.BlockSpec(memory_space=pl.ANY)] * 3,
        out_specs=[vmem] * (3 if fused else 4),
        out_shape=[jax.ShapeDtypeStruct(part, f32)]
        + [jax.ShapeDtypeStruct(*s) for s in ([((rows, width), f32)] if fused else sums)]
        + [jax.ShapeDtypeStruct(small.shape[3:], f32)],
        scratch_shapes=[
            pltpu.VMEM((ranks,) + part, bf16),
            pltpu.VMEM(wshape, bf16),
            pltpu.VMEM(cshape, bf16),
            pltpu.VMEM(small.shape, f32),
            pltpu.VMEM(wshape[1:], bf16),
            pltpu.VMEM((ring,) + part[1:], bf16),
            pltpu.VMEM((line,) + wshape[1:], bf16),
            pltpu.VMEM((ring,) + cshape[2:], bf16),
            pltpu.VMEM((ring,) + small.shape[2:], f32),
            pltpu.VMEM((line,) + cshape[3:], bf16),
            pltpu.VMEM((line,) + small.shape[3:], f32),
        ]
        + [dma((ring,))] * 6
        + [dma((line,))] * 6
        + [dma((ranks,)), dma((ranks,)), dma((4,))]
        + ([pltpu.VMEM(a.shape, bf16) for a in operands] + [pltpu.VMEM(*s) for s in sums] if fused else []),
        compiler_params=pltpu.CompilerParams(
            collective_id=1, has_side_effects=True, vmem_limit_bytes=67043328
        ),
        name="reduce_all",
    )(small, tok.reshape(part), cot.reshape(part), gain, *operands)
    return [dn_sum.reshape(length, d), s_sum] + weights


def dot(a, b, dims, precision=None):
    return lax.dot_general(
        a, b, (dims, ((), ())), preferred_element_type=f32, precision=precision
    )


NN, NT, TN = ((1,), (0,)), ((1,), (1,)), ((0,), (0,))


def sigmoid(a):
    return 0.5 * jnp.tanh(0.5 * a) + 0.5


def iota(shape, axis):
    return lax.broadcasted_iota(jnp.int32, shape, axis)


def parts(a):
    high = a.astype(bf16)
    return high, (a - high.astype(f32)).astype(bf16)


def fine(a, b, dims):
    left = jnp.concatenate([a[0], a[0], a[1]], axis=dims[0][0])
    right = jnp.concatenate([b[0], b[1], b[0]], axis=dims[1][0])
    return dot(left, right, dims)


def steps_of(raw, bias):
    shifted = raw + bias
    return jnp.maximum(shifted, 0.0) + jnp.log1p(jnp.exp(-jnp.abs(shifted)))


def convolve(pad, conv_ref, tile, count):
    total = conv_ref[CONVK : CONVK + 1, tile]
    for k in range(CONVK):
        total = total + pad[EDGE - CONVK + 1 + k : EDGE - CONVK + 1 + k + count, tile] * conv_ref[k : k + 1, tile]
    return total


class Chunk:
    def __init__(self, step, rate):
        n = SUB
        upper = jnp.where(iota((n, n), 0) <= iota((n, n), 1), 1.0, 0.0)
        self.step = step
        self.rows = dot(step * -rate, upper, NN, highest)
        self.cols = self.rows.T
        self.step_cols = step.T

    def col(self, h):
        return jnp.broadcast_to(self.cols[:, h : h + 1], (SUB, SUB))

    def decay(self, h, col, hide):
        return jnp.exp(col - self.rows[h : h + 1, :] + hide)

    def step_col(self, h):
        return jnp.broadcast_to(self.step_cols[:, h : h + 1], (SUB, SUB))


def fwd_kernel(
    proj_ref, raw_ref, cot_ref, wout_ref, conv_ref, lane_ref, head_ref,
    y_ref, dg_ref, out_ref, state_ref, sum_ref, gated,
    pad, act, carry,
):
    block = proj_ref.shape[0]
    din = y_ref.shape[1]
    conv = conv_ref.shape[1]

    @pl.when(pl.program_id(0) == 0)
    def _():
        carry[...] = jnp.zeros_like(carry)
        pad[0:EDGE, :] = jnp.zeros((EDGE, conv), f32)

    @pl.when(pl.program_id(0) > 0)
    def _():
        pad[0:EDGE, :] = pad[block : block + EDGE, :]

    for j in range(conv // LANES):
        tile = slice(j * LANES, (j + 1) * LANES)
        pad[EDGE:, tile] = proj_ref[:, din + j * LANES : din + (j + 1) * LANES].astype(f32)
        filtered = convolve(pad, conv_ref, tile, block)
        act[:, tile] = filtered * sigmoid(filtered)
    dg_ref[...] = dot(cot_ref[...], wout_ref[...], NT)

    low = iota((SUB, LANES), 1) < HDIM
    hide = jnp.where(iota((SUB, SUB), 0) >= iota((SUB, SUB), 1), 0.0, -1e30)
    for i in range(block // SUB):
        rows = slice(i * SUB, (i + 1) * SUB)
        b, c = parts(act[rows, din : din + NSTATE]), parts(act[rows, din + NSTATE :])
        chunk = Chunk(steps_of(raw_ref[:, rows], head_ref[1]), head_ref[0])
        scores = fine(c, b, NT)
        sq = jnp.zeros((SUB, LANES), f32)
        cross = jnp.zeros((SUB, LANES), f32)
        for j in range(din // LANES):
            tile = slice(j * LANES, (j + 1) * LANES)
            x = act[rows, tile]
            col0, col1 = chunk.col(2 * j), chunk.col(2 * j + 1)
            m0 = chunk.decay(2 * j, col0, hide) * scores
            m1 = chunk.decay(2 * j + 1, col1, hide) * scores
            cexp = jnp.where(low, col0, col1)
            xs = x * jnp.where(low, chunk.step_col(2 * j), chunk.step_col(2 * j + 1))
            zero = jnp.zeros_like(xs)
            split = jnp.concatenate([jnp.where(low, xs, zero), jnp.where(low, zero, xs)], axis=0)
            before = carry[:, tile]
            state_ref[i, :, tile] = before
            y = fine(parts(jnp.concatenate([m0, m1], axis=1)), parts(split), NN)
            y = y + fine(c, parts(before), NN) * jnp.exp(cexp)
            y_ref[rows, tile] = y
            last = cexp[SUB - 1 :, :]
            carry[:, tile] = before * jnp.exp(last) + fine(b, parts(xs * jnp.exp(last - cexp)), TN)
            z = proj_ref[rows, tile].astype(f32)
            v = (y + lane_ref[0:1, tile] * x) * (z * sigmoid(z))
            scaled = v * lane_ref[1:2, tile]
            gated[rows, tile] = scaled.astype(bf16)
            sq = sq + v * v
            cross = cross + scaled * dg_ref[rows, tile]
        ones = jnp.ones((4, LANES), f32)
        sum_ref[0:4, rows] = dot(ones, sq, NT, highest)
        sum_ref[4:8, rows] = dot(ones, cross, NT, highest)
    out_ref[...] = dot(gated[...], wout_ref[...], NN).astype(bf16)


def bwd_kernel(
    total_din, live,
    proj_ref, rim_ref, raw_ref, y_ref, dg_ref, sum_ref, state_ref, conv_ref, lane_ref, head_ref,
    out_in, o_in,
    dproj_ref, dconv_ref, dlane_ref, dhead_ref, out_sum, o_sum,
    pad, act, slope, dpad, carry, edge, dact,
    *links,
):
    side_reduce(out_in, o_in, out_sum, o_sum, *links)

    block = proj_ref.shape[0]
    din = y_ref.shape[1]
    conv = conv_ref.shape[1]
    step_id = pl.program_id(0)
    first = step_id == pl.num_programs(0) - 1

    @pl.when(step_id == 0)
    def _():
        carry[...] = jnp.zeros_like(carry)
        edge[...] = jnp.zeros_like(edge)
        dpad[0:EDGE, :] = jnp.zeros((EDGE, conv), f32)
        dconv_ref[...] = jnp.zeros_like(dconv_ref)
        dlane_ref[...] = jnp.zeros_like(dlane_ref)
        dhead_ref[...] = jnp.zeros_like(dhead_ref)

    dpad[block : block + EDGE, :] = dpad[0:EDGE, :]
    keep = jnp.where(first, 0.0, 1.0)
    for j in range(conv // LANES):
        tile = slice(j * LANES, (j + 1) * LANES)
        src = slice(din + j * LANES, din + (j + 1) * LANES)
        pad[0:EDGE, tile] = rim_ref[rim_ref.shape[0] - EDGE :, src].astype(f32) * keep
        pad[EDGE:, tile] = proj_ref[:, src].astype(f32)
        filtered = convolve(pad, conv_ref, tile, block)
        s = sigmoid(filtered)
        act[:, tile] = filtered * s
        slope[:, tile] = s * (1.0 + filtered * (1.0 - s))

    low = iota((SUB, LANES), 1) < HDIM
    hide = jnp.where(iota((SUB, SUB), 0) >= iota((SUB, SUB), 1), 0.0, -1e30)
    lower = jnp.where(iota((SUB, SUB), 0) >= iota((SUB, SUB), 1), 1.0, 0.0)
    heads = raw_ref.shape[0]
    row, lane = iota((heads, LANES), 0), iota((heads, LANES), 1)
    spot = jnp.where((row < live) & (lane == row + lax.axis_index("seq") * live), 1.0, 0.0).astype(bf16)
    dgain = [jnp.zeros((1, LANES), f32) for _ in range(din // LANES)]
    dskip = [jnp.zeros((1, LANES), f32) for _ in range(din // LANES)]
    for i in reversed(range(block // SUB)):
        rows = slice(i * SUB, (i + 1) * SUB)
        b_parts, c_parts = parts(act[rows, din : din + NSTATE]), parts(act[rows, din + NSTATE :])
        chunk = Chunk(steps_of(raw_ref[:, rows], head_ref[1]), head_ref[0])
        scores = fine(c_parts, b_parts, NT)
        sums = sum_ref[:, rows].T
        scale = lax.rsqrt(jnp.broadcast_to(sums[:, 0:1], (SUB, LANES)) * (1.0 / total_din) + epsilon)
        mean = jnp.broadcast_to(sums[:, 4:5], (SUB, LANES)) * (1.0 / total_din) * (scale * scale * scale)
        dscores = jnp.zeros((SUB, SUB), f32)
        d_b = jnp.zeros((SUB, NSTATE), f32)
        d_c = jnp.zeros((SUB, NSTATE), f32)
        d_cum = jnp.zeros((heads, SUB), f32)
        d_step = jnp.zeros((heads, SUB), f32)
        reach = jnp.zeros((heads, 8), f32)
        for j in range(din // LANES):
            tile = slice(j * LANES, (j + 1) * LANES)
            x = act[rows, tile]
            y = y_ref[rows, tile]
            skip, gain = lane_ref[0:1, tile], lane_ref[1:2, tile]
            z = proj_ref[rows, tile].astype(f32)
            sz = sigmoid(z)
            mixed = y + skip * x
            silu = z * sz
            v = mixed * silu
            dg = dg_ref[rows, tile]
            vs = v * scale
            dgain[j] = dgain[j] + jnp.sum(dg * vs, axis=0, keepdims=True)
            dv = scale * (gain * dg) - v * mean
            dy = dv * silu
            dproj_ref[rows, tile] = (dv * mixed * (sz * (1.0 + z * (1.0 - sz)))).astype(bf16)
            dskip[j] = dskip[j] + jnp.sum(dy * x, axis=0, keepdims=True)

            col0, col1 = chunk.col(2 * j), chunk.col(2 * j + 1)
            l0, l1 = chunk.decay(2 * j, col0, hide), chunk.decay(2 * j + 1, col1, hide)
            m = parts(jnp.concatenate([l0 * scores, l1 * scores], axis=0))
            cexp = jnp.where(low, col0, col1)
            step = jnp.where(low, chunk.step_col(2 * j), chunk.step_col(2 * j + 1))
            last = cexp[SUB - 1 :, :]
            grow, tail = jnp.exp(cexp), jnp.exp(last - cexp)
            xs = x * step
            zero = jnp.zeros_like(dy)
            dsplit = parts(jnp.concatenate([jnp.where(low, dy, zero), jnp.where(low, zero, dy)], axis=0))
            xs_parts = parts(xs)
            dm = fine(dsplit, xs_parts, NT)
            dscores = dscores + dm[:SUB] * l0 + dm[SUB:] * l1
            dend = carry[:, tile]
            dend_parts = parts(dend)
            before = state_ref[i, :, tile]
            dxs = fine(m, dsplit, TN) + fine(b_parts, dend_parts, NN) * tail
            grown = parts(dy * grow)
            d_c = d_c + fine(grown, parts(before), NT)
            d_b = d_b + fine(parts(xs * tail), dend_parts, NT)
            dprev = dend * jnp.exp(last) + fine(c_parts, grown, TN)
            carry[:, tile] = dprev
            pick = jnp.where(lax.shift_right_logical(iota((heads, LANES), 1), 6) + 2 * j == iota((heads, LANES), 0), 1.0, 0.0)
            balance = dy * y - xs * dxs
            d_cum = d_cum + dot(pick, balance, NT, highest)
            d_step = d_step + dot(pick, x * dxs, NT, highest)
            crossing = jnp.sum(dprev * before, axis=0, keepdims=True)
            reach = reach + dot(pick, jnp.broadcast_to(crossing, (8, LANES)), NT, highest)
            dact[rows, tile] = dxs * step + skip * dy
        ds_parts = parts(dscores)
        dact[rows, din : din + NSTATE] = d_b + fine(ds_parts, c_parts, TN)
        dact[rows, din + NSTATE :] = d_c + fine(ds_parts, b_parts, NN)
        d_log = dot(d_cum, lower, NN, highest) + edge[...]
        edge[...] = jnp.broadcast_to(reach[:, 0:1], edge.shape)
        raw = raw_ref[:, rows] + head_ref[1]
        draw = (d_step - head_ref[0] * d_log) * sigmoid(raw)
        dproj_ref[rows, din + conv :] = dot(draw.astype(bf16), spot, TN).astype(bf16)
        dhead_ref[0] += -chunk.step * d_log
        dhead_ref[1] += draw
    for j in range(din // LANES):
        tile = slice(j * LANES, (j + 1) * LANES)
        dlane_ref[0:1, tile] += dskip[j]
        dlane_ref[1:2, tile] += dgain[j]
    for j in range(conv // LANES):
        tile = slice(j * LANES, (j + 1) * LANES)
        df = dact[:, tile] * slope[:, tile]
        dpad[0:block, tile] = df
        dconv_ref[CONVK : CONVK + 1, tile] += jnp.sum(df, axis=0, keepdims=True)
        back = jnp.zeros((block, LANES), f32)
        for k in range(CONVK):
            shift = CONVK - 1 - k
            dconv_ref[k : k + 1, tile] += jnp.sum(
                df * pad[EDGE - shift : EDGE - shift + block, tile], axis=0, keepdims=True
            )
            back = back + conv_ref[k : k + 1, tile] * dpad[shift : shift + block, tile]
        dproj_ref[:, din + j * LANES : din + (j + 1) * LANES] = back.astype(bf16)


def rows_spec(block, width):
    return pl.BlockSpec((block, width), lambda t: (t, 0))


def whole(shape):
    return pl.BlockSpec(shape, lambda t: (0,) * len(shape))


def mixer_forward(proj, raw, cot, w_out, conv, lanes, heads):
    length, width = proj.shape
    din, d = w_out.shape
    cc = conv.shape[1]
    block = min(2 * TOKENS, length)
    n = block // SUB
    cols = pl.BlockSpec((8, block), lambda t: (0, t))
    return pl.pallas_call(
        fwd_kernel,
        grid=(length // block,),
        in_specs=[
            rows_spec(block, width), cols, rows_spec(block, d), whole(w_out.shape),
            whole(conv.shape), whole(lanes.shape), whole(heads.shape),
        ],
        out_specs=[
            rows_spec(block, din), rows_spec(block, din), rows_spec(block, d),
            pl.BlockSpec((n, NSTATE, din), lambda t: (t, 0, 0)), cols, rows_spec(block, din),
        ],
        out_shape=[
            jax.ShapeDtypeStruct((length, din), f32),
            jax.ShapeDtypeStruct((length, din), f32),
            jax.ShapeDtypeStruct((length, d), bf16),
            jax.ShapeDtypeStruct((length // SUB, NSTATE, din), f32),
            jax.ShapeDtypeStruct((8, length), f32),
            jax.ShapeDtypeStruct((length, din), bf16),
        ],
        scratch_shapes=[
            pltpu.VMEM((block + EDGE, cc), f32),
            pltpu.VMEM((block, cc), f32),
            pltpu.VMEM((NSTATE, din), f32),
        ],
        name="mix_forward",
    )(proj, raw, cot, w_out, conv, lanes, heads)


def side_reduce(out_in, o_in, out_sum, o_sum, acc, land, stage, o_land, out_s, out_r, oz_s, oz_r, mix_s, mix_r, local):
    ranks, planes = acc.shape[0], stage.shape[0]
    me, dp = lax.axis_index("seq"), lax.axis_index("dp")
    outs = Collect(acc, land, out_s, out_r, 16)
    fold = Fold(lambda d: stage.at[d], o_land, planes, oz_s, oz_r, stage.shape[1])
    top = len(bits_of(ranks)) - 1
    load = pltpu.make_async_copy(out_in, acc, local.at[0])

    def move(k, act):
        index = me * planes + k
        plane, to = lax.div(index, ranks), index % ranks

        @pl.when(to != me)
        def _():
            copy = remote(o_in.at[k], stage.at[plane], mix_s.at[k], mix_r.at[plane], (dp, to))
            copy.start() if act else copy.wait_send()

        if act:
            @pl.when(to == me)
            def _():
                pltpu.make_async_copy(o_in.at[k], stage.at[plane], mix_r.at[plane]).start()

    def begin():
        load.start()
        greet(ranks, planes)
        for k in range(planes):
            move(k, True)
        load.wait()
        outs.push(top)

    def settle():
        for d in range(planes):
            pltpu.make_async_copy(stage.at[d], stage.at[d], mix_r.at[d]).wait()
        fold.push(0)

    def end():
        outs.total(out_sum)
        fold.total(o_sum)
        for k in range(planes):
            move(k, False)
        outs.finish()
        fold.finish()

    pushes = {4 * i + 1: partial(outs.push, top - 1 - i) for i in range(top)}
    folds = [settle] + [partial(fold.push, t) for t in range(1, planes - 1)]
    spare = [t for t in range(3, 64) if t not in pushes]
    stages = {0: begin, **pushes, **dict(zip(spare, folds))}
    last = pl.num_programs(0) - 1
    for k, run in sorted(stages.items()):
        pl.when(pl.program_id(0) == k)(run)
    pl.when(pl.program_id(0) == last)(end)


def mixer_backward(ranks, planes, total_din, proj, raw, y, dg, sums, states, conv, lanes, heads, live, out_part, d_w_out):
    length, width = proj.shape
    din, d = y.shape[1], out_part.shape[1]
    cc = conv.shape[1]
    block = min(TOKENS, length)
    n = block // SUB
    last = length // block - 1
    rim = 16
    assert last > max(4 * len(bits_of(ranks)) - 7, planes + 1 + (planes > 3))
    part = (2, length // ranks // 2, d)
    ring, line = 2 * (ranks - 1), 2 * planes
    dma = pltpu.SemaphoreType.DMA

    def back(block, width):
        return pl.BlockSpec((block, width), lambda t: (last - t, 0))

    cols = pl.BlockSpec((8, block), lambda t: (0, last - t))
    anywhere = pl.BlockSpec(memory_space=pl.ANY)
    *results, out_sum, o_sum = pl.pallas_call(
        partial(bwd_kernel, total_din, live),
        grid=(length // block,),
        in_specs=[
            back(block, width),
            pl.BlockSpec((rim, width), lambda t: (jnp.maximum((last - t) * (block // rim) - 1, 0), 0)),
            cols, back(block, din), back(block, din), cols,
            pl.BlockSpec((n, NSTATE, din), lambda t: (last - t, 0, 0)),
            whole(conv.shape), whole(lanes.shape), whole(heads.shape), anywhere, anywhere,
        ],
        out_specs=[
            back(block, width + LANES), whole((8, cc)), whole((8, din)), whole((2, 8, SUB)),
            whole(part), whole(d_w_out.shape[1:]),
        ],
        out_shape=[
            jax.ShapeDtypeStruct((length, width + LANES), bf16),
            jax.ShapeDtypeStruct((8, cc), f32),
            jax.ShapeDtypeStruct((8, din), f32),
            jax.ShapeDtypeStruct((2, 8, SUB), f32),
            jax.ShapeDtypeStruct(part, f32),
            jax.ShapeDtypeStruct(d_w_out.shape[1:], f32),
        ],
        scratch_shapes=[
            pltpu.VMEM((block + EDGE, cc), f32),
            pltpu.VMEM((block, cc), f32),
            pltpu.VMEM((block, cc), f32),
            pltpu.VMEM((block + EDGE, cc), f32),
            pltpu.VMEM((NSTATE, din), f32),
            pltpu.VMEM((8, SUB), f32),
            pltpu.VMEM((block, cc), f32),
            pltpu.VMEM((ranks,) + part, bf16),
            pltpu.VMEM((ring,) + part[1:], bf16),
            pltpu.VMEM(d_w_out.shape, bf16),
            pltpu.VMEM((line,) + d_w_out.shape[1:], bf16),
            dma((ring,)), dma((ring,)), dma((line,)), dma((line,)), dma((planes,)), dma((planes,)), dma((1,)),
        ],
        compiler_params=pltpu.CompilerParams(
            collective_id=3, has_side_effects=True, vmem_limit_bytes=67043328
        ),
        name="mix_backward",
    )(
        proj, proj, raw, y, dg, sums, states, conv, lanes, heads,
        out_part.reshape((ranks,) + part), d_w_out,
    )
    return results + [out_sum.reshape(length // ranks, d), o_sum]


def rms_scale(values, gain):
    mean_sq = jnp.mean(values * values, axis=-1, keepdims=True)
    return values * lax.rsqrt(mean_sq + epsilon) * gain


def widen(array, size, axis):
    pads = [(0, 0)] * array.ndim
    pads[axis] = (0, size - array.shape[axis])
    return jnp.pad(array, pads)


def per_device(
    tokens,
    cotangent,
    in_weight,
    out_weight,
    conv_weight,
    conv_bias,
    norm_gain,
    gate_gain,
    decay_rate,
    dt_bias,
    d_skip,
):
    ranks = lax.axis_size("seq")
    me = lax.axis_index("seq")
    both = ("dp", "seq")
    heads = decay_rate.shape[0] // ranks
    din = heads * HDIM
    padded = -(-din // LANES) * LANES
    din_all = din * ranks
    rows, width = in_weight.shape
    conv_all = din_all + 2 * NSTATE
    main = 2 * padded + 2 * NSTATE

    def mine(array, size, axis=0):
        return lax.dynamic_slice_in_dim(array, me * size, size, axis)

    planes = lax.axis_size("dp")
    x_own = tokens[0].astype(f32)
    send = jnp.concatenate(
        [
            widen(in_weight[:, :din_all].reshape(rows, ranks, din), padded, 2),
            widen(in_weight[:, din_all : 2 * din_all].reshape(rows, ranks, din), padded, 2),
        ],
        axis=2,
    ).transpose(1, 0, 2)
    d = in_weight.shape[0] * ranks * planes
    rank_id = lax.axis_index("dp") * ranks + me
    small = [norm_gain, gate_gain, conv_weight.reshape(-1), conv_bias]
    sizes = [a.shape[0] for a in small]
    room = rows * HDIM - d
    if room >= sum(sizes):
        placed = lax.dynamic_update_slice_in_dim(jnp.zeros((d,), bf16), norm_gain, rank_id * rows, 0)
        packed = jnp.concatenate([placed, widen(jnp.concatenate(small), room, 0)])
    else:
        packed = widen(jnp.concatenate(small), rows * HDIM, 0)
    common = jnp.concatenate(
        [
            in_weight[:, 2 * din_all : 2 * din_all + 2 * NSTATE],
            widen(in_weight[:, din_all + conv_all :], HDIM, 1),
            packed.reshape(rows, HDIM),
        ],
        axis=1,
    )
    cot, w_out, common, fused, *rest = gather_all(
        ranks, planes, tokens[0], cotangent[0], send, out_weight, common
    )
    w_out = widen(w_out, padded, 0)
    packed = common[..., 2 * NSTATE + HDIM :].reshape(ranks * planes, rows * HDIM).astype(f32)
    if room >= sum(sizes):
        packed = packed[:, d:]
    gain_norm, gain_gate, conv_w, conv_b = (
        packed[:, sum(sizes[:k]) : sum(sizes[: k + 1])].reshape(-1) for k in range(4)
    )
    conv_w = conv_w.reshape(-1, CONVK)
    taps = jnp.concatenate([conv_w.T, conv_b[None], jnp.zeros((8 - CONVK - 1, conv_all), f32)], axis=0)
    conv = jnp.concatenate([widen(mine(taps, din, 1), padded, 1), taps[:, din_all:]], axis=1)
    if fused:
        raw, flipped, proj, w_full = rest
    else:
        tok, w_all = rest
        w_full = jnp.concatenate([w_all, common.reshape(-1, common.shape[-1])], axis=1)
        normed = rms_scale(tok.astype(f32), gain_norm).astype(bf16)
        proj = dot(normed, w_full[:, :main], NN).astype(bf16)
        raw = dot(w_full[:, main : main + HDIM].T, normed, NT).astype(bf16).astype(f32)
    raw = widen(mine(raw, heads), 8, 0)
    rate, bias, skip = (mine(a, heads) for a in (decay_rate, dt_bias, d_skip))
    lanes = jnp.stack([jnp.repeat(skip, HDIM), mine(gain_gate, din)])
    lanes = widen(widen(lanes, padded, 1), 8, 0)
    head_rows = jnp.broadcast_to(widen(jnp.stack([rate, bias]), 8, 1)[:, :, None], (2, 8, SUB))

    y, dg, out_part, states, sums, gated = mixer_forward(proj, raw, cot, w_out, conv, lanes, head_rows)
    sums = plane_sum(ranks, sums[::4].reshape(8, -1)).reshape(2, -1)
    inverse = lax.rsqrt(sums[0] / din_all + epsilon)[:, None]
    d_w_out = dot((gated * inverse).astype(bf16), cot, TN)[:din].astype(bf16)
    d_proj, d_conv, d_lane, d_head, out_sum, grad_out = mixer_backward(
        ranks, planes, din_all, proj, raw, y, dg, jnp.repeat(sums, 4, axis=0), states, conv, lanes, head_rows,
        heads, out_part, d_w_out.reshape(planes, -1, d),
    )

    def by_owner(array):
        split = array.reshape((2, planes // 2, ranks) + array.shape[1:])
        return split.transpose((2, 0, 1) + tuple(range(3, split.ndim)))

    def place(own, size):
        return lax.dynamic_update_slice_in_dim(
            jnp.zeros((size * ranks,) + own.shape[1:], f32), own, me * size, 0
        )

    d_cw, d_cb = d_conv[:CONVK].T, d_conv[CONVK]
    full_cw = jnp.concatenate([place(d_cw[:din], din), d_cw[padded:]], axis=0)
    full_cb = jnp.concatenate([place(d_cb[:din], din), d_cb[padded:]], axis=0)
    d_skp = jnp.sum(d_lane[0, :din].reshape(heads, HDIM), axis=1)
    d_rate, d_bias = jnp.sum(d_head, axis=2)[:, :heads]
    devices = planes * ranks
    head_part = jnp.concatenate([place(a, heads) for a in (d_rate, d_bias, d_skp)])
    fields = [
        a.reshape(devices, -1) for a in (full_cw, full_cb, place(d_lane[1, :din], din))
    ] + [jnp.broadcast_to(head_part, (devices,) + head_part.shape)]
    ends = [0]
    for a in fields:
        ends.append(ends[-1] + a.shape[1])
    small = widen(jnp.concatenate(fields, axis=1), 8 * LANES, 1).reshape(devices, 8, LANES)
    if fused:
        operands = flipped, d_proj, w_full
    else:
        d_w = dot(normed, d_proj, TN).astype(bf16)
        part = dot(d_proj, w_full, NT).astype(bf16)
        operands = (
            part.reshape(ranks, 2, -1, d),
            d_w[:, : 2 * padded].reshape(planes, ranks, rows, -1),
            by_owner(d_w[:, 2 * padded :].reshape(planes * ranks, rows, -1)),
        )
    grad_x, small_sum, *sums_in = reduce_all(
        fused, ranks, planes, rows, 2 * padded, width, by_owner(small), tokens[0], cotangent[0],
        gain_norm[None], *operands,
    )
    block_out = (x_own + mine(inverse, x_own.shape[0]) * out_sum).astype(bf16)
    if fused:
        (grad_in,) = sums_in
    else:
        w_sum, bc_sum = sums_in
        spread = w_sum.astype(f32).transpose(1, 0, 2)
        grad_in = jnp.concatenate(
            [
                spread[:, :, :din].reshape(rows, din_all),
                spread[:, :, padded : padded + din].reshape(rows, din_all),
                bc_sum[:, : 2 * NSTATE + heads * ranks],
            ],
            axis=1,
        )
    g_gain = jnp.sum(grad_in * in_weight.astype(f32), axis=1) / norm_gain.astype(f32)
    small_sum = small_sum.reshape(-1)
    g_cw, g_cb, g_gate, head_sums = (small_sum[a:b] for a, b in zip(ends[:-1], ends[1:]))
    g_cw = g_cw.reshape(-1, CONVK)
    head_sums = head_sums.reshape(3, -1)
    return (
        block_out[None],
        grad_x[None],
        grad_in,
        grad_out,
        g_cw,
        g_cb,
        g_gain,
        g_gate,
        head_sums[0],
        head_sums[1],
        head_sums[2],
    )


def solution(mesh):
    rows = P(("dp", "seq"), None)
    flat = P(("dp", "seq"))
    act = P("dp", "seq", None)
    return jax.shard_map(
        per_device,
        mesh=mesh,
        in_specs=(act, act, rows, rows, rows, flat, flat, flat, P(), P(), P()),
        out_specs=(act, act, rows, rows, rows, flat, flat, flat, P(), P(), P()),
        check_vma=False,
    )
```
